256 devices in a mesh: section: 2 (over core), seq: 128 (over x, z, y).
Axes of the slice: x: 4, y: 4, z: 8, core: 2. Of those that a mesh axis runs over, the one named last changes fastest.
Arguments:
- acts: bfloat16 [2, 32768, 2048], P('section', 'seq'), may hold values from -6 to 6
- in_proj: bfloat16 [2, 2048, 4640], P('section', 'seq'), may hold values from -0.125 to 0.125
- out_proj: bfloat16 [2, 2048, 2048], P('section'), may hold values from -0.125 to 0.125
- conv_weight: float32 [2, 4, 2304], P('section'), may hold values from -3 to 3
- conv_bias: float32 [2, 2304], P('section'), may hold values from -3 to 3
- dt_bias: float32 [2, 32], P('section'), may hold values from -4 to -1
- decay_rate: float32 [2, 32], P('section'), may hold values from 0.0001 to 0.5
- skip_gain: float32 [2, 32], P('section'), may hold values from -4 to 4
- level_bias: float32 [2, 256], P('section'), may hold values from -4 to 4
- norm_gain: float32 [2, 2048], P('section'), may hold values from 0.5 to 1.5
- gate_gain: float32 [2, 2048], P('section'), may hold values from 0.5 to 1.5
Outputs:
- handoff: bfloat16 [2, 32768, 2048], P('section', 'seq')
The draws below stay inside these ranges and needn't reach their ends.
All inputs are finite; a program needn't handle non-finite values.
Results may differ from the reference program's by a relative error of at most 0.006.
Values may be sent and summed in bfloat16 or wider, within the bound.
A program may use at most 128 MiB of HBM per device.

```python
import math
import jax
import jax.numpy as jnp
from jax import lax

D = 2048
CONV = 4
HEADS = 32
LEVELS = 8
SECTIONS = 2
DI = 2048
CH = 2304
PROJ = 4640
SEQLEN = 32768
N_SEQ = 128


def block_levels(key, extent, shards, low, largest):
    loudness = 1.0
    for axis_at, parts in shards:
        steps = jax.random.uniform(jax.random.fold_in(jax.random.fold_in(key, 6), axis_at), (parts,), jnp.float32, low / len(shards), largest / len(shards))
        loudness = loudness * jnp.repeat(jnp.exp(steps), extent[axis_at] // parts).reshape((-1,) + (1,) * (len(extent) - 1 - axis_at))
    return loudness


def normal_values(key, extent, width, reach, pieces=(), kind=jnp.bfloat16):
    loudness = block_levels(key, extent, pieces, -0.22, 0.18) if pieces else 1.0
    values = jax.random.normal(key, extent, jnp.float32) * width * loudness
    return jnp.minimum(jnp.maximum(values, -reach), reach).astype(kind)


def setup_inputs(seed: int = 0) -> dict:
    streams_of = jax.random.split(jax.random.key(seed), 12)
    acts = normal_values(streams_of[0], (SECTIONS, SEQLEN, D), 1.0, 6.0, ((0, 2), (1, 128)))
    in_proj = normal_values(streams_of[1], (SECTIONS, D, PROJ), D ** -0.5, 0.125, ((0, 2), (1, 128)))
    out_proj = normal_values(streams_of[2], (SECTIONS, DI, D), DI ** -0.5, 0.125, ((0, 2),))
    conv_weight = normal_values(streams_of[3], (SECTIONS, CONV, CH), 0.6, 3.0, ((0, 2),), jnp.float32)
    conv_bias = normal_values(streams_of[4], (SECTIONS, CH), 0.5, 3.0, ((0, 2),), jnp.float32)
    dt_bias = jnp.clip(-4.0 + 3.0 * jax.random.uniform(streams_of[5], (SECTIONS, HEADS), jnp.float32) ** block_levels(streams_of[5], (SECTIONS, HEADS), ((0, 2),), -0.2, 0.2), -4.0, -1.0)
    decay_rate = jnp.clip(jnp.exp(math.log(0.5) - 8.517193 * jax.random.uniform(streams_of[6], (SECTIONS, HEADS), jnp.float32) ** block_levels(streams_of[6], (SECTIONS, HEADS), ((0, 2),), -0.2, 0.2)), 0.0001, 0.5)
    skip_gain = normal_values(streams_of[7], (SECTIONS, HEADS), 1.0, 4.0, ((0, 2),), jnp.float32)
    level_bias = normal_values(streams_of[8], (SECTIONS, HEADS * LEVELS), 1.0, 4.0, ((0, 2),), jnp.float32)
    norm_gain = jnp.clip(1.0 + 0.1 * jax.random.normal(streams_of[9], (SECTIONS, D), jnp.float32), 0.5, 1.5)
    gate_gain = jnp.clip(1.0 + 0.1 * jax.random.normal(streams_of[10], (SECTIONS, DI), jnp.float32), 0.5, 1.5)
    return dict(acts=acts, in_proj=in_proj, out_proj=out_proj, conv_weight=conv_weight, conv_bias=conv_bias, dt_bias=dt_bias, decay_rate=decay_rate, skip_gain=skip_gain, level_bias=level_bias, norm_gain=norm_gain, gate_gain=gate_gain)


EPS = 1e-05
best_precision = lax.Precision.HIGHEST

def block_core(operands):
    c_block, b_block, x_block, cum_block, dt_block, lam_block = operands
    length = c_block.shape[0]
    scores = jnp.dot(c_block, b_block.T, precision=best_precision, preferred_element_type=jnp.float32)
    row_ids = lax.broadcasted_iota(jnp.int32, (length, length), 0)
    col_ids = lax.broadcasted_iota(jnp.int32, (length, length), 1)
    causal = (col_ids <= row_ids)[:, :, None]
    differ = cum_block[:, None, :] - cum_block[None, :, :]
    decays = jnp.where(causal, jnp.exp(jnp.where(causal, differ, 0.0)), 0.0)
    weights = decays * scores[:, :, None] * dt_block[None, :, :] * lam_block[:, None, :]
    y_block = jnp.einsum('tsh,shp->thp', weights, x_block, precision=best_precision)
    tail = jnp.exp(cum_block[-1][None, :] - cum_block) * dt_block
    state = jnp.einsum('sn,shp->hnp', b_block, x_block * tail[:, :, None], precision=best_precision)
    return (y_block, state)

def mixer(acts, w_in, w_out, conv_w, conv_b, dt_b, rate, skip, lam_b, gain_in, gain_gate):
    hidden = acts.astype(jnp.float32)
    seqlen = hidden.shape[0]
    inner = gain_gate.shape[0]
    heads = dt_b.shape[0]
    head_size = inner // heads
    chans = conv_w.shape[1]
    state_size = (chans - inner) // 2
    kernel_len = conv_w.shape[0]
    normed_in = (hidden * lax.rsqrt(lax.optimization_barrier(jnp.mean(hidden * hidden, axis=1, keepdims=True)) + EPS) * gain_in).astype(jnp.bfloat16)
    projected = jnp.dot(normed_in, w_in, preferred_element_type=jnp.float32).astype(jnp.bfloat16)
    conv_in = jnp.concatenate([jnp.zeros((kernel_len - 1, chans), jnp.float32), projected[:, :chans].astype(jnp.float32)], axis=0)
    mixed = conv_b + jnp.zeros((seqlen, chans), jnp.float32)
    for offset in range(kernel_len):
        mixed = mixed + conv_w[offset] * conv_in[offset:offset + seqlen]
    mixed = jax.nn.silu(mixed)
    values = mixed[:, :inner].reshape(seqlen, heads, head_size)
    b_mat = mixed[:, inner:inner + state_size]
    c_mat = mixed[:, inner + state_size:]
    z_gate = projected[:, chans:chans + inner].astype(jnp.float32)
    steps = jax.nn.softplus(projected[:, chans + inner:chans + inner + heads].astype(jnp.float32) + dt_b)
    lam = jax.nn.softplus(projected[:, chans + inner + heads:].astype(jnp.float32) + lam_b).reshape(seqlen, heads, LEVELS)
    blocks = N_SEQ
    length = seqlen // blocks
    log_decay = (-steps * rate).reshape(blocks, length, heads)
    cum = jnp.cumsum(log_decay, axis=1)
    x_blocks = values.reshape(blocks, length, heads, head_size)
    b_blocks = b_mat.reshape(blocks, length, state_size)
    c_blocks = c_mat.reshape(blocks, length, state_size)
    dt_blocks = steps.reshape(blocks, length, heads)
    lam_blocks = lam.reshape(blocks, length, heads, LEVELS)
    y_all, states = lax.map(block_core, (c_blocks, b_blocks, x_blocks, cum, dt_blocks, lam_blocks[..., 0]))
    y_all = y_all + skip[None, None, :, None] * x_blocks
    endlog = cum[:, -1, :]
    inclusive = jnp.cumsum(endlog, axis=0)
    exclusive = inclusive - endlog
    for level in range(1, blocks.bit_length()):
        half = 2 ** (level - 1)
        groups = blocks // (2 * half)
        lower_states = states.reshape(groups, 2, half, heads, state_size, head_size)[:, 0]
        incl_groups = inclusive.reshape(groups, 2, half, heads)
        lower_end = incl_groups[:, 0, half - 1]
        weights = jnp.exp(lower_end[:, None, :] - incl_groups[:, 0])
        summed = jnp.einsum('gjh,gjhnp->ghnp', weights, lower_states, precision=best_precision)
        upper_excl = exclusive.reshape(groups, 2, half, heads)[:, 1]
        carry = jnp.exp(upper_excl - lower_end[:, None, :])
        c_upper = c_blocks.reshape(groups, 2, half, length, state_size)[:, 1]
        reads = jnp.einsum('gitn,ghnp->githp', c_upper, summed, precision=best_precision)
        cum_upper = cum.reshape(groups, 2, half, length, heads)[:, 1]
        lam_upper = lam_blocks.reshape(groups, 2, half, length, heads, LEVELS)[:, 1, :, :, :, level]
        scale = carry[:, :, None, :] * jnp.exp(cum_upper) * lam_upper
        shaped = y_all.reshape(groups, 2, half, length, heads, head_size)
        y_all = shaped.at[:, 1].add(reads * scale[..., None]).reshape(blocks, length, heads, head_size)
    y_flat = y_all.reshape(seqlen, inner)
    gated = y_flat * jax.nn.silu(z_gate)
    normed = (gated * lax.rsqrt(lax.optimization_barrier(jnp.mean(gated * gated, axis=1, keepdims=True)) + EPS) * gain_gate).astype(jnp.bfloat16)
    return (hidden + jnp.dot(normed, w_out, preferred_element_type=jnp.float32)).astype(jnp.bfloat16)

def reference(acts, in_proj, out_proj, conv_weight, conv_bias, dt_bias, decay_rate, skip_gain, level_bias, norm_gain, gate_gain):
    results = []
    for section_id in range(SECTIONS):
        results.append(mixer(acts[section_id], in_proj[section_id], out_proj[section_id], conv_weight[section_id], conv_bias[section_id], dt_bias[section_id], decay_rate[section_id], skip_gain[section_id], level_bias[section_id], norm_gain[section_id], gate_gain[section_id]))
    stacked = jnp.stack(results, axis=0)
    return jnp.roll(stacked, 1, axis=0)
```

```python
import functools
import jax
import jax.numpy as jnp
from jax import lax
from jax.experimental import pallas as pl
from jax.experimental.pallas import tpu as pltpu
from jax.sharding import PartitionSpec as P

EPS = 1e-05
MESH = pl.DeviceIdType.MESH
NX, NZ, NY = 4, 8, 4
GROUPS = NX * NZ
CA, CB = 512, 896
NP = CA + CB
ROWS = 256
F32, BF16 = jnp.float32, jnp.bfloat16


def seq_of(x, z, y):
    return (lax.rem(x + 4 * NX, NX) * NZ + lax.rem(z + 4 * NZ, NZ)) * NY + lax.rem(y + 4 * NY, NY)


def plan():
    msgs = {}
    ua, ub, un = 64 * CA * 2, 64 * CB * 2, 128 * 2048 * 2
    for d, links in ((1, {"y+": 1}), (3, {"y-": 1}), (2, {"y+": 1, "y-": 1})):
        msgs[("w", d)] = ("w", None, (0, 0, d), None, 16 * NP * 2, links)
    msgs[("P", 0)] = ("h0", 0, (0, 0, 1), None, un, {"y+": 1})
    msgs[("M", 1)] = ("h1", 0, (0, 0, -1), None, un, {"y-": 1})
    msgs[("P", 1)] = ("h1", 0, (0, 0, 1), None, un, {"y+": 1})
    msgs[("M", 0)] = ("h0", 0, (0, 0, -1), None, un, {"y-": 1})
    msgs[("P", 2)] = ("h0", -1, (0, 0, 1), ("P", 0), un, {"y+": 1})
    msgs[("M", 2)] = ("h1", 1, (0, 0, -1), ("M", 1), un, {"y-": 1})
    own = "own"
    for d, links in ((1, {"x+": 1}), (3, {"x-": 1}), (2, {"x+": 2})):
        msgs[("A1", d)] = ("a", (0, 0), (d, 0, 0), own, ua, links)
    for k in range(1, 5):
        if k < 5:
            dep = own if k == 1 else ("B1+", k - 1)
            msgs[("B1+", k)] = ("b", (0, -(k - 1)), (0, 1, 0), dep, ub, {"z+": 1})
        if k < 4:
            dep = own if k == 1 else ("B1-", k - 1)
            msgs[("B1-", k)] = ("b", (0, k - 1), (0, -1, 0), dep, ub, {"z-": 1})
    for k in range(1, 5):
        for d in range(4):
            up, down = (4, 3) if d < 2 else (3, 4)
            if k <= up:
                dep = (own if d == 0 else ("A1", d)) if k == 1 else ("A2+", d, k - 1)
                msgs[("A2+", d, k)] = ("a", (-d, -(k - 1)), (0, 1, 0), dep, ua, {"z+": 1})
            if k <= down:
                dep = (own if d == 0 else ("A1", d)) if k == 1 else ("A2-", d, k - 1)
                msgs[("A2-", d, k)] = ("a", (-d, k - 1), (0, -1, 0), dep, ua, {"z-": 1})
    offs = [0, -1, 1, -2, 2, -3, 3, -4]
    for n, o in enumerate(offs):
        dep = own if o == 0 else (("B1+", -o) if o < 0 else ("B1-", o))
        msgs[("B2+", o)] = ("b", (0, o), (1, 0, 0), dep, ub, {"x+": 1})
        msgs[("B2-", o)] = ("b", (0, o), (-1, 0, 0), dep, ub, {"x-": 1})
        if n in (1, 3, 5):
            msgs[("B2+2", o)] = ("b", (-1, o), (1, 0, 0), ("B2+", o), ub, {"x+": 1})
        else:
            msgs[("B2-2", o)] = ("b", (1, o), (-1, 0, 0), ("B2-", o), ub, {"x-": 1})
    return msgs


def schedule(msgs, rate=46.6e3, latency=1.9):
    free, arrive, order = {}, {}, []
    started = set()
    events = []

    def start(name, now):
        part, chunk, to, dep, size, links = msgs[name]
        begin = max([now] + [free.get(l, 0.0) for l in links])
        end = begin
        for l, n in links.items():
            free[l] = begin + size * n / rate
            end = max(end, free[l])
        arrive[name] = end + latency
        events.append((end + latency, len(started), name))
        started.add(name)

    for name, m in msgs.items():
        if m[3] is None:
            start(name, 0.0)
    got = set()
    while events:
        events.sort()
        now, _, name = events.pop(0)
        order.append(name)
        got.add(name)
        if all(("w", d) in got for d in (1, 2, 3)) and "own" not in got:
            got.add("own")
            order.append("own")
            for other, m in msgs.items():
                if m[3] == "own":
                    start(other, now)
        for other, m in msgs.items():
            if m[3] == name:
                start(other, now)
    return order, arrive


def gather_kernel(acts, wa_in, wb_in, gain, out, wa, wb, ablk, u, local_sems, send_sems, recv_sems):
    i = lax.axis_index("seq")
    y = lax.rem(i, NY)
    z = lax.rem(lax.div(i, NY), NZ)
    x = lax.div(i, NY * NZ)

    def there(dx, dz, dy):
        return {"seq": seq_of(x + dx, z + dz, y + dy)}

    barrier = pltpu.get_barrier_semaphore()
    near = ((1, 0, 0), (-1, 0, 0), (2, 0, 0), (0, 1, 0), (0, -1, 0), (0, 0, 1), (0, 0, -1), (0, 0, 2))
    for to in near:
        pl.semaphore_signal(barrier, inc=1, device_id=there(*to), device_id_type=MESH)

    msgs = plan()
    number = {name: n for n, name in enumerate(msgs)}
    order, _ = schedule(msgs)

    def block(rel):
        return lax.rem(y + rel + 2 * NY, NY)

    def rows_of(cx, cz):
        return pl.ds(pl.multiple_of(seq_of(x + cx, z + cz, 0) * 16, 64), 64)

    mine = pl.ds(pl.multiple_of(i * 16, 16), 16)
    local = [
        pltpu.make_async_copy(wa_in.at[y], wa.at[mine], local_sems.at[0]),
        pltpu.make_async_copy(wb_in.at[y], wb.at[mine], local_sems.at[1]),
    ]
    for copy in local:
        copy.start()
    pl.semaphore_wait(barrier, len(near))

    def remote(src, dst, n, to):
        return pltpu.make_async_remote_copy(
            src_ref=src, dst_ref=dst, send_sem=send_sems.at[n], recv_sem=recv_sems.at[n],
            device_id=there(*to), device_id_type=MESH)

    def copies(name, arriving):
        part, chunk, to, dep, _, _ = msgs[name]
        n = number[name]
        back = to if arriving else (0, 0, 0)
        if part == "w":
            d = to[2]
            if arriving:
                rows = pl.ds(pl.multiple_of(seq_of(x, z, y - d) * 16, 16), 16)
            else:
                rows = mine
            slot = lax.rem(y + d, NY)
            return [remote(wa_in.at[slot], wa.at[rows], n, to),
                    remote(wb_in.at[slot], wb.at[rows], len(msgs) + n, to)]
        if part in ("h0", "h1"):
            half = pl.ds(128 * int(part[1]), 128)
            dst = ablk.at[block(chunk - back[2]), half]
            src = acts.at[half] if chunk == 0 and not arriving else dst
            return [remote(src, dst, n, to)]
        ref = wa if part == "a" else wb
        rows = rows_of(chunk[0] - back[0], chunk[1] - back[1])
        return [remote(ref.at[rows], ref.at[rows], n, to)]

    def start(name):
        for copy in copies(name, False):
            copy.start()

    def normed(src, rel, half):
        def step(n, _):
            at = pl.multiple_of(half * 128 + n * 64, 64)
            h = src[pl.ds(at, 64), :].astype(F32)
            r = lax.rsqrt(jnp.mean(h * h, axis=1, keepdims=True) + EPS)
            to = pl.multiple_of(block(rel) * ROWS + at, 64)
            u[pl.ds(to, 64), :] = (h * r * gain[...]).astype(BF16)
            return 0

        lax.fori_loop(0, 2, step, 0)

    for name, m in msgs.items():
        if m[3] is None:
            start(name)
    normed(acts, 0, 0)
    normed(acts, 0, 1)
    halves = {("P", 0): (-1, 0), ("P", 1): (-1, 1), ("M", 1): (1, 1), ("M", 0): (1, 0), ("P", 2): (-2, 0), ("M", 2): (2, 1)}
    for name in order:
        if name == "own":
            for copy in local:
                copy.wait()
        else:
            for copy in copies(name, True):
                copy.wait_recv()
        for other, m in msgs.items():
            if m[3] == name:
                start(other)
        if name in halves:
            rel, half = halves[name]
            normed(ablk.at[block(rel)], rel, half)

    def product(n, _):
        rows = pl.ds(pl.multiple_of(n * 512, 512), 512)
        out[rows, :CA] = jnp.dot(u[rows, :], wa[...], preferred_element_type=F32).astype(BF16)
        out[rows, CA:] = jnp.dot(u[rows, :], wb[...], preferred_element_type=F32).astype(BF16)
        return 0

    lax.fori_loop(0, 2, product, 0)
    for name in msgs:
        for copy in copies(name, False):
            copy.wait_send()


def gather_project(acts, wa, wb, gain):
    count = len(plan())
    return pl.pallas_call(
        gather_kernel,
        out_shape=jax.ShapeDtypeStruct((NY * ROWS, NP), BF16),
        in_specs=[pl.BlockSpec(memory_space=pltpu.VMEM)] * 4,
        out_specs=pl.BlockSpec(memory_space=pltpu.VMEM),
        scratch_shapes=[
            pltpu.VMEM((2048, CA), BF16),
            pltpu.VMEM((2048, CB), BF16),
            pltpu.VMEM((NY, ROWS, 2048), BF16),
            pltpu.VMEM((NY * ROWS, 2048), BF16),
            pltpu.SemaphoreType.DMA((2,)),
            pltpu.SemaphoreType.DMA((count + 3,)),
            pltpu.SemaphoreType.DMA((count + 3,)),
        ],
        compiler_params=pltpu.CompilerParams(
            collective_id=0, has_side_effects=True, vmem_limit_bytes=48 * 1024 * 1024),
        name="gather_project",
    )(acts, wa, wb, gain)


def column_slices(w):
    rows = w.shape[0]
    xr = w[:, :2048].reshape(rows, NY, 512).transpose(1, 0, 2)
    bc = jnp.broadcast_to(w[None, :, 2048:2304], (NY, rows, 256))
    zg = w[:, 2304:4352].reshape(rows, NY, 512).transpose(1, 0, 2)
    dr = w[:, 4352:4384].reshape(rows, NY, 8).transpose(1, 0, 2)
    lr = w[:, 4384:4640].reshape(rows, NY, 64).transpose(1, 0, 2)
    pad = jnp.zeros((NY, rows, 56), w.dtype)
    return xr, jnp.concatenate([bc, zg, lr, dr, pad], axis=2)


HI = lax.Precision.HIGHEST


def swapped(block, apart):
    route = []
    for low in range(128):
        high = low | 1 << apart
        if high != low:
            route += [(low, high), (high, low)]
    return lax.ppermute(block, "seq", route)


def turned(block, d):
    return lax.ppermute(block, "seq", [(i, i // 4 * 4 + (i + d) % 4) for i in range(128)])


def inside(c, b, x, cum, dt, lam):
    s = jnp.dot(c, b.T, preferred_element_type=F32)
    t = lax.broadcasted_iota(jnp.int32, s.shape, 0) >= lax.broadcasted_iota(jnp.int32, s.shape, 1)
    t = t[:, :, None]
    e = jnp.where(t, jnp.exp(jnp.where(t, cum[:, None] - cum[None], 0.0)), 0.0)
    w = e * s[:, :, None] * dt[None] * lam[:, None]
    return jnp.einsum("tsh,shp->thp", w, x)


def per_device(acts, in_proj, out_proj, conv_weight, conv_bias, dt_bias, decay_rate, skip_gain, level_bias, norm_gain, gate_gain):
    i = lax.axis_index("seq")
    y = i % NY
    wa, wb = column_slices(in_proj[0])
    p = gather_project(acts[0], wa, wb, norm_gain)
    tail = lax.ppermute(p[-3:, :768], "seq", [(k, k + 4) for k in range(124)])

    def own(a, n):
        return lax.dynamic_slice_in_dim(a, y * n, n, axis=-1)

    cw = jnp.concatenate([own(conv_weight[0, :, :2048], 512), conv_weight[0, :, 2048:]], axis=1)
    cb = jnp.concatenate([own(conv_bias[0, :2048], 512), conv_bias[0, 2048:]])
    dtb, rate, skip, lb = own(dt_bias[0], 8), own(decay_rate[0], 8), own(skip_gain[0], 8), own(level_bias[0], 64)
    ext = jnp.concatenate([tail, p[:, :768]]).astype(F32)
    mixed = cb + sum(cw[k] * ext[k : k + 1024] for k in range(4))
    mixed = jax.nn.silu(mixed)
    x = mixed[:, :512].reshape(4, 256, 8, 64)
    b = mixed[:, 512:640].reshape(4, 256, 128)
    c = mixed[:, 640:].reshape(4, 256, 128)
    zg = p[:, 768:1280].astype(F32)
    dt = jax.nn.softplus(p[:, 1344:1352].astype(F32) + dtb).reshape(4, 256, 8)
    lam = jax.nn.softplus(p[:, 1280:1344].astype(F32) + lb).reshape(4, 256, 8, 8)
    cum = jnp.cumsum(-dt * rate, axis=1)
    yb = [inside(c[n], b[n], x[n], cum[n], dt[n], lam[n, :, :, 0]) for n in range(4)]
    end = cum[:, -1]
    keep = jnp.exp(end)
    st = [jnp.einsum("sn,shp->hnp", b[n], x[n] * (jnp.exp(end[n] - cum[n]) * dt[n])[..., None]) for n in range(4)]
    low = keep[1][:, None, None] * st[0] + st[1]
    high = keep[3][:, None, None] * st[2] + st[3]

    def read(n, state, level, before):
        r = jnp.einsum("tn,hnp->thp", c[n], state)
        return r * (lam[n, :, :, level] * jnp.exp(cum[n] + before))[..., None]

    zero = jnp.zeros((8,), F32)
    yb[1] += read(1, st[0], 1, zero)
    yb[3] += read(3, st[2], 1, zero)
    yb[2] += read(2, low, 2, zero)
    yb[3] += read(3, low, 2, end[2])
    before = [zero, end[0], end[0] + end[1], end[0] + end[1] + end[2]]
    blog = before[3] + end[3]
    bst = jnp.exp(end[2] + end[3])[:, None, None] * low + high
    blow = zero
    g = i // 4
    for bit in range(5):
        olog = swapped(blog, bit + 2)
        ost = swapped(bst.astype(BF16), bit + 2).astype(F32)
        upper = g >> bit & 1 == 1
        bucket = jnp.where(upper, jnp.exp(blow)[:, None, None] * ost, 0.0)
        for n in range(4):
            yb[n] += read(n, bucket, bit + 3, before[n])
        bst = jnp.where(upper, jnp.exp(blog)[:, None, None] * ost + bst, jnp.exp(olog)[:, None, None] * bst + ost)
        blow = jnp.where(upper, blow + olog, blow)
        blog = blog + olog
    yv = jnp.stack(yb).reshape(1024, 8, 64) + skip[None, :, None] * mixed[:, :512].reshape(1024, 8, 64)
    q = (yv.reshape(1024, 512) * jax.nn.silu(zg)).astype(BF16).reshape(4, 256, 512)
    got = jnp.zeros((4, 256, 512), BF16)
    got = lax.dynamic_update_index_in_dim(got, lax.dynamic_index_in_dim(q, y, 0, False), y, 0)
    for d in (1, 2, 3):
        arrived = turned(lax.dynamic_index_in_dim(q, (y + d) % 4, 0, False), d)
        got = lax.dynamic_update_index_in_dim(got, arrived, (y - d) % 4, 0)
    gated = got.transpose(1, 0, 2).reshape(256, 2048).astype(F32)
    n = (gated * lax.rsqrt(jnp.mean(gated * gated, axis=1, keepdims=True) + EPS) * gate_gain[0]).astype(BF16)
    o = (acts[0].astype(F32) + jnp.dot(n, out_proj[0], preferred_element_type=F32)).astype(BF16)
    return lax.ppermute(o, "section", [(0, 1), (1, 0)])[None]


def solution(mesh):
    two = P("section", None)
    three = P("section", None, None)
    return jax.shard_map(
        per_device,
        mesh=mesh,
        in_specs=(P("section", "seq", None), P("section", "seq", None), three, three, two, two, two, two, two, two, two),
        out_specs=P("section", "seq", None),
        check_vma=False,
    )
```

```python
import functools
import jax
import jax.numpy as jnp
from jax import lax
from jax.experimental import pallas as pl
from jax.experimental.pallas import tpu as pltpu
from jax.sharding import PartitionSpec as P

EPS = 1e-05
MESH = pl.DeviceIdType.MESH
NX, NZ, NY = 4, 8, 4
GROUPS = NX * NZ
CA, CB = 512, 896
NP = CA + CB
ROWS = 256
F32, BF16 = jnp.float32, jnp.bfloat16


def seq_of(x, z, y):
    return (lax.rem(x + 4 * NX, NX) * NZ + lax.rem(z + 4 * NZ, NZ)) * NY + lax.rem(y + 4 * NY, NY)


def plan():
    msgs = {}
    ua, ub, un = 64 * CA * 2, 64 * CB * 2, 128 * 2048 * 2
    for d, links in ((1, {"y+": 1}), (3, {"y-": 1}), (2, {"y+": 1, "y-": 1})):
        msgs[("w", d)] = ("w", None, (0, 0, d), None, 16 * NP * 2, links)
    msgs[("P", 0)] = ("h0", 0, (0, 0, 1), None, un, {"y+": 1})
    msgs[("M", 1)] = ("h1", 0, (0, 0, -1), None, un, {"y-": 1})
    msgs[("P", 1)] = ("h1", 0, (0, 0, 1), None, un, {"y+": 1})
    msgs[("M", 0)] = ("h0", 0, (0, 0, -1), None, un, {"y-": 1})
    msgs[("P", 2)] = ("h0", -1, (0, 0, 1), ("P", 0), un, {"y+": 1})
    msgs[("M", 2)] = ("h1", 1, (0, 0, -1), ("M", 1), un, {"y-": 1})
    own = "own"
    for d, links in ((1, {"x+": 1}), (3, {"x-": 1}), (2, {"x+": 2})):
        msgs[("A1", d)] = ("a", (0, 0), (d, 0, 0), own, ua, links)
    for k in range(1, 5):
        if k < 5:
            dep = own if k == 1 else ("B1+", k - 1)
            msgs[("B1+", k)] = ("b", (0, -(k - 1)), (0, 1, 0), dep, ub, {"z+": 1})
        if k < 4:
            dep = own if k == 1 else ("B1-", k - 1)
            msgs[("B1-", k)] = ("b", (0, k - 1), (0, -1, 0), dep, ub, {"z-": 1})
    for k in range(1, 5):
        for d in range(4):
            up, down = (4, 3) if d < 2 else (3, 4)
            if k <= up:
                dep = (own if d == 0 else ("A1", d)) if k == 1 else ("A2+", d, k - 1)
                msgs[("A2+", d, k)] = ("a", (-d, -(k - 1)), (0, 1, 0), dep, ua, {"z+": 1})
            if k <= down:
                dep = (own if d == 0 else ("A1", d)) if k == 1 else ("A2-", d, k - 1)
                msgs[("A2-", d, k)] = ("a", (-d, k - 1), (0, -1, 0), dep, ua, {"z-": 1})
    offs = [0, -1, 1, -2, 2, -3, 3, -4]
    for n, o in enumerate(offs):
        dep = own if o == 0 else (("B1+", -o) if o < 0 else ("B1-", o))
        msgs[("B2+", o)] = ("b", (0, o), (1, 0, 0), dep, ub, {"x+": 1})
        msgs[("B2-", o)] = ("b", (0, o), (-1, 0, 0), dep, ub, {"x-": 1})
        if n in (1, 3, 5):
            msgs[("B2+2", o)] = ("b", (-1, o), (1, 0, 0), ("B2+", o), ub, {"x+": 1})
        else:
            msgs[("B2-2", o)] = ("b", (1, o), (-1, 0, 0), ("B2-", o), ub, {"x-": 1})
    return msgs


def schedule(msgs, rate=46.6e3, latency=1.9):
    free, arrive, order = {}, {}, []
    started = set()
    events = []

    def start(name, now):
        part, chunk, to, dep, size, links = msgs[name]
        begin = max([now] + [free.get(l, 0.0) for l in links])
        end = begin
        for l, n in links.items():
            free[l] = begin + size * n / rate
            end = max(end, free[l])
        arrive[name] = end + latency
        events.append((end + latency, len(started), name))
        started.add(name)

    for name, m in msgs.items():
        if m[3] is None:
            start(name, 0.0)
    got = set()
    while events:
        events.sort()
        now, _, name = events.pop(0)
        order.append(name)
        got.add(name)
        if all(("w", d) in got for d in (1, 2, 3)) and "own" not in got:
            got.add("own")
            order.append("own")
            for other, m in msgs.items():
                if m[3] == "own":
                    start(other, now)
        for other, m in msgs.items():
            if m[3] == name:
                start(other, now)
    return order, arrive


def gather_kernel(acts, wa_in, wb_in, gain, out, wa, wb, ablk, u, local_sems, send_sems, recv_sems):
    i = lax.axis_index("seq")
    y = lax.rem(i, NY)
    z = lax.rem(lax.div(i, NY), NZ)
    x = lax.div(i, NY * NZ)

    def there(dx, dz, dy):
        return {"seq": seq_of(x + dx, z + dz, y + dy)}

    barrier = pltpu.get_barrier_semaphore()
    near = ((1, 0, 0), (-1, 0, 0), (2, 0, 0), (0, 1, 0), (0, -1, 0), (0, 0, 1), (0, 0, -1), (0, 0, 2))
    for to in near:
        pl.semaphore_signal(barrier, inc=1, device_id=there(*to), device_id_type=MESH)

    msgs = plan()
    number = {name: n for n, name in enumerate(msgs)}
    order, _ = schedule(msgs)

    def block(rel):
        return lax.rem(y + rel + 2 * NY, NY)

    def rows_of(cx, cz):
        return pl.ds(pl.multiple_of(seq_of(x + cx, z + cz, 0) * 16, 64), 64)

    mine = pl.ds(pl.multiple_of(i * 16, 16), 16)
    local = [
        pltpu.make_async_copy(wa_in.at[y], wa.at[mine], local_sems.at[0]),
        pltpu.make_async_copy(wb_in.at[y], wb.at[mine], local_sems.at[1]),
    ]
    for copy in local:
        copy.start()
    pl.semaphore_wait(barrier, len(near))

    def remote(src, dst, n, to):
        return pltpu.make_async_remote_copy(
            src_ref=src, dst_ref=dst, send_sem=send_sems.at[n], recv_sem=recv_sems.at[n],
            device_id=there(*to), device_id_type=MESH)

    def copies(name, arriving):
        part, chunk, to, dep, _, _ = msgs[name]
        n = number[name]
        back = to if arriving else (0, 0, 0)
        if part == "w":
            d = to[2]
            if arriving:
                rows = pl.ds(pl.multiple_of(seq_of(x, z, y - d) * 16, 16), 16)
            else:
                rows = mine
            slot = lax.rem(y + d, NY)
            return [remote(wa_in.at[slot], wa.at[rows], n, to),
                    remote(wb_in.at[slot], wb.at[rows], len(msgs) + n, to)]
        if part in ("h0", "h1"):
            half = pl.ds(128 * int(part[1]), 128)
            dst = ablk.at[block(chunk - back[2]), half]
            src = acts.at[half] if chunk == 0 and not arriving else dst
            return [remote(src, dst, n, to)]
        ref = wa if part == "a" else wb
        rows = rows_of(chunk[0] - back[0], chunk[1] - back[1])
        return [remote(ref.at[rows], ref.at[rows], n, to)]

    def start(name):
        for copy in copies(name, False):
            copy.start()

    def normed(src, rel, half):
        def step(n, _):
            at = pl.multiple_of(half * 128 + n * 64, 64)
            h = src[pl.ds(at, 64), :].astype(F32)
            r = lax.rsqrt(jnp.mean(h * h, axis=1, keepdims=True) + EPS)
            to = pl.multiple_of(block(rel) * ROWS + at, 64)
            u[pl.ds(to, 64), :] = (h * r * gain[...]).astype(BF16)
            return 0

        lax.fori_loop(0, 2, step, 0)

    for name, m in msgs.items():
        if m[3] is None:
            start(name)
    normed(acts, 0, 0)
    normed(acts, 0, 1)
    halves = {("P", 0): (-1, 0), ("P", 1): (-1, 1), ("M", 1): (1, 1), ("M", 0): (1, 0), ("P", 2): (-2, 0), ("M", 2): (2, 1)}
    for name in order:
        if name == "own":
            for copy in local:
                copy.wait()
        else:
            for copy in copies(name, True):
                copy.wait_recv()
        for other, m in msgs.items():
            if m[3] == name:
                start(other)
        if name in halves:
            rel, half = halves[name]
            normed(ablk.at[block(rel)], rel, half)

    def product(n, _):
        rows = pl.ds(pl.multiple_of(n * 512, 512), 512)
        out[rows, :CA] = jnp.dot(u[rows, :], wa[...], preferred_element_type=F32).astype(BF16)
        out[rows, CA:] = jnp.dot(u[rows, :], wb[...], preferred_element_type=F32).astype(BF16)
        return 0

    lax.fori_loop(0, 2, product, 0)
    for name in msgs:
        for copy in copies(name, False):
            copy.wait_send()


def gather_project(acts, wa, wb, gain):
    count = len(plan())
    return pl.pallas_call(
        gather_kernel,
        out_shape=jax.ShapeDtypeStruct((NY * ROWS, NP), BF16),
        in_specs=[pl.BlockSpec(memory_space=pltpu.VMEM)] * 4,
        out_specs=pl.BlockSpec(memory_space=pltpu.VMEM),
        scratch_shapes=[
            pltpu.VMEM((2048, CA), BF16),
            pltpu.VMEM((2048, CB), BF16),
            pltpu.VMEM((NY, ROWS, 2048), BF16),
            pltpu.VMEM((NY * ROWS, 2048), BF16),
            pltpu.SemaphoreType.DMA((2,)),
            pltpu.SemaphoreType.DMA((count + 3,)),
            pltpu.SemaphoreType.DMA((count + 3,)),
        ],
        compiler_params=pltpu.CompilerParams(
            collective_id=0, has_side_effects=True, vmem_limit_bytes=48 * 1024 * 1024),
        name="gather_project",
    )(acts, wa, wb, gain)


def column_slices(w):
    rows = w.shape[0]
    xr = w[:, :2048].reshape(rows, NY, 512).transpose(1, 0, 2)
    bc = jnp.broadcast_to(w[None, :, 2048:2304], (NY, rows, 256))
    zg = w[:, 2304:4352].reshape(rows, NY, 512).transpose(1, 0, 2)
    dr = jnp.repeat(w[:, 4352:4384].reshape(rows, NY, 8).transpose(1, 0, 2), 8, axis=2)
    lr = w[:, 4384:4640].reshape(rows, NY, 64).transpose(1, 0, 2)
    return xr, jnp.concatenate([bc, zg, lr, dr], axis=2)


HI = lax.Precision.HIGHEST
MID = CA + 768
LEVELS_OUT = 5
TABLE = (0, 16, 24, 28, 30)


def spread(row, lanes):
    k = lax.broadcasted_iota(jnp.int32, (128, lanes), 0)
    c = lax.broadcasted_iota(jnp.int32, (128, lanes), 1)
    return jnp.dot(row, (k == 64 + 8 * lax.shift_right_logical(c, 6)).astype(F32), precision=HI, preferred_element_type=F32)


def halves_of(a, lane_low, lane_high, first):
    return jnp.where(first, a[:, lane_low : lane_low + 1], a[:, lane_high : lane_high + 1])


def softplus(v):
    return jnp.maximum(v, 0.0) + jnp.log1p(jnp.exp(-jnp.abs(v)))


def mixer_kernel(p, acts_in, wout_in, cw, cb, dtb, rate, skip, lb, gg, out,
                 ext, xf, bcs, td, cu, yacc, near_st, eb, ee, snd1, slog, rcv1, rlog, table, rcv2, tail,
                 qs, qr, wout, acts, acc, os, oin,
                 in_sems, ssem, rsem, lsend, lrecv, tsem, qsend, qrecv, osend, orecv, dsem):
    i = lax.axis_index("seq")
    y = lax.rem(i, NY)
    g = lax.div(i, NY)
    s = lax.axis_index("section")

    def group(n):
        return {"seq": n * NY + y}

    def beside(n):
        return {"seq": g * NY + lax.rem(y + n, NY)}

    def wrap(n):
        return lax.rem(n, GROUPS)

    def remote(src, dst, send, recv, to):
        return pltpu.make_async_remote_copy(
            src_ref=src, dst_ref=dst, send_sem=send, recv_sem=recv, device_id=to, device_id_type=MESH)

    barrier = pltpu.get_barrier_semaphore()

    def greet(d, _):
        pl.semaphore_signal(barrier, inc=1, device_id=group(wrap(g + d)), device_id_type=MESH)
        return 0

    lax.fori_loop(1, GROUPS, greet, 0)
    for d in (1, 2, 3):
        pl.semaphore_signal(barrier, inc=1, device_id=beside(d), device_id_type=MESH)
    pl.semaphore_signal(barrier, inc=1, device_id={"section": 1 - s}, device_id_type=MESH)
    loads = [pltpu.make_async_copy(acts_in, acts, in_sems.at[0]), pltpu.make_async_copy(wout_in, wout, in_sems.at[1])]
    for copy in loads:
        copy.start()

    def picked(v, hit):
        rows = jnp.broadcast_to(v[...], (8, v.shape[1]))
        return jnp.dot(rows, hit.astype(F32), precision=HI, preferred_element_type=F32)[:1]

    def two(rows, lanes):
        return (lax.broadcasted_iota(jnp.int32, (rows, lanes), 0), lax.broadcasted_iota(jnp.int32, (rows, lanes), 1))

    k, c = two(32, 128)
    of_head = (c >= 64) & (k == 8 * y + lax.shift_right_logical(c - 64, 3))
    k2, c2 = two(256, 128)
    bias = picked(dtb, of_head) + picked(lb, (c2 < 64) & (k2 == 64 * y + c2))
    rates = picked(rate, of_head)
    k3, c3 = two(32, 512)
    skips = picked(skip, k3 == 8 * y + lax.shift_right_logical(c3, 6))

    low_tri = (lax.broadcasted_iota(jnp.int32, (ROWS, ROWS), 1) <= lax.broadcasted_iota(jnp.int32, (ROWS, ROWS), 0)).astype(BF16)
    for b in range(4):
        rows = slice(b * ROWS, (b + 1) * ROWS)
        t = softplus(p[rows, MID:].astype(F32) + bias)
        td[rows, :] = t
        left = -t * rates
        total = jnp.zeros((ROWS, 128), F32)
        for _ in range(3):
            piece = left.astype(BF16)
            total = total + jnp.dot(low_tri, piece, preferred_element_type=F32)
            left = left - piece.astype(F32)
        cu[rows, :] = total
        eb[b : b + 1, :] = total[ROWS - 1 :, :]
    eb[4:, :] = jnp.zeros((4, 128), F32)
    ends = eb[...]
    ee[...] = jnp.exp(spread(ends, 512))
    slog[...] = jnp.broadcast_to(jnp.sum(ends, axis=0, keepdims=True), (8, 128))

    pl.semaphore_wait(barrier, GROUPS - 1 + 3 + 1)
    back = remote(p.at[pl.ds(1008, 16), pl.ds(0, 768)], tail, tsem.at[0], tsem.at[1], group(wrap(g + 1)))
    back.start()

    for n in range(4):
        ext[8 + n * ROWS : 8 + (n + 1) * ROWS, :] = p[n * ROWS : (n + 1) * ROWS, :768].astype(F32)
    own = pl.ds(pl.multiple_of(y * 512, 512), 512)
    tx = [cw[k : k + 1, own] for k in range(4)]
    tb = [cw[k : k + 1, 2048:] for k in range(4)]
    bx, bb = cb[:, own], cb[:, 2048:]

    def convolved(n):
        at = n * 128
        v = bx
        for k in range(4):
            v = v + tx[k] * ext[at + 5 + k : at + 133 + k, :512]
        xf[at : at + 128, :] = jax.nn.silu(v)
        v = bb
        for k in range(4):
            v = v + tb[k] * ext[at + 5 + k : at + 133 + k, 512:]
        bcs[at : at + 128, :] = jax.nn.silu(v).astype(BF16)

    for n in range(1, 8):
        convolved(n)
    back.wait_recv()
    before = tail[...].astype(F32)
    ext[0:8, :] = jnp.where(g > 0, before[8:, :], 0.0)
    convolved(0)

    first = lax.broadcasted_iota(jnp.int32, (1, 128), 1) < 64

    def state(b):
        rows = slice(b * ROWS, (b + 1) * ROWS)
        tl = jnp.exp(ends[b : b + 1, :] - cu[rows, :]) * td[rows, :]
        parts = []
        for h in range(4):
            parts.append((xf[rows, 128 * h : 128 * h + 128] * halves_of(tl, 64 + 16 * h, 72 + 16 * h, first)).astype(BF16))
        xt = jnp.concatenate(parts, axis=1)
        return lax.dot_general(bcs[rows, :128], xt, (((0,), (0,)), ((), ())), preferred_element_type=F32)

    st = state(0)
    near_st[0] = st.astype(BF16)
    st = ee[1:2, :] * st + state(1)
    near_st[1] = st.astype(BF16)
    other = state(2)
    near_st[2] = other.astype(BF16)
    st = ee[2:3, :] * ee[3:4, :] * st + ee[3:4, :] * other + state(3)
    st = st.astype(BF16)
    for n in range(GROUPS):
        ct, nt = n // 8, n % 8
        snd1[n] = st[16 * nt : 16 * nt + 16, 128 * ct : 128 * ct + 128]

    def first_send(d, _):
        to = wrap(g + d)
        remote(snd1.at[to], rcv1.at[g], ssem.at[0], rsem.at[0], group(to)).start()
        remote(slog, rlog.at[g], ssem.at[1], rsem.at[1], group(to)).start()
        return 0

    lax.fori_loop(1, GROUPS, first_send, 0)
    rcv1[g] = snd1[g]
    rlog[g] = slog[...]

    def inside(b, _):
        base = pl.multiple_of(b * ROWS, ROWS)
        every = pl.ds(base, ROWS)
        cum_t = jnp.transpose(cu[every, :])
        dt_t = jnp.transpose(td[every, :])
        for r in range(2):
            rows = pl.ds(pl.multiple_of(base + 128 * r, 128), 128)
            wide = 128 * (r + 1)
            seen = pl.ds(base, wide)
            scores = lax.dot_general(bcs[rows, 128:], bcs[seen, :128], (((1,), (1,)), ((), ())), preferred_element_type=F32)
            ti, si = two(128, wide)
            causal = si <= ti + 128 * r
            cum, lam = cu[rows, :], td[rows, :]
            for h in range(4):
                xp = xf[seen, 128 * h : 128 * h + 128].astype(BF16)
                got = []
                for e in (2 * h, 2 * h + 1):
                    lane = 64 + 8 * e
                    differ = jnp.where(causal, cum[:, lane : lane + 1] - cum_t[lane : lane + 1, :wide], -1e30)
                    w = scores * jnp.exp(differ) * dt_t[lane : lane + 1, :wide]
                    got.append(jnp.dot(w.astype(BF16), xp, preferred_element_type=F32))
                val = jnp.where(first, got[0], got[1]) * halves_of(lam, 16 * h, 16 * h + 8, first)
                cols = slice(128 * h, 128 * h + 128)
                yacc[rows, cols] = val + skips[:, cols] * xf[rows, cols]
        return 0

    lax.fori_loop(0, 4, inside, 0)

    remote(rcv1.at[pl.ds(0, GROUPS - 1)], rcv1.at[pl.ds(0, GROUPS - 1)], ssem.at[0], rsem.at[0], group(g)).wait_recv()
    remote(rlog.at[pl.ds(0, GROUPS - 1)], rlog.at[pl.ds(0, GROUPS - 1)], ssem.at[1], rsem.at[1], group(g)).wait_recv()
    logs = rlog[:, 0, :]
    wide_logs = spread(logs, 512)
    ct = lax.div(g, 8)
    mine = jnp.zeros((GROUPS, 128), F32)
    for n in range(4):
        mine = jnp.where(ct == n, wide_logs[:, 128 * n : 128 * n + 128], mine)
    level = [rcv1[n].astype(F32) for n in range(GROUPS)]
    ends_of = [mine[n : n + 1, :] for n in range(GROUPS)]
    for l in range(LEVELS_OUT):
        for n in range(0, len(level), 2):
            table[TABLE[l] + n // 2] = level[n].astype(BF16)
        level = [jnp.exp(ends_of[n + 1]) * level[n] + level[n + 1] for n in range(0, len(level), 2)]
        ends_of = [ends_of[n] + ends_of[n + 1] for n in range(0, len(ends_of), 2)]

    def second_send(d, _):
        to = wrap(g + d)
        for l in range(LEVELS_OUT):
            up = lax.div(to, 2**l)

            @pl.when(lax.rem(up, 2) == 1)
            def _():
                remote(table.at[TABLE[l] + lax.div(up, 2)], rcv2.at[l, g], lsend.at[l], lrecv.at[l], group(to)).start()

        return 0

    lax.fori_loop(1, GROUPS, second_send, 0)
    bits = [lax.rem(lax.div(g, 2**l), 2) for l in range(LEVELS_OUT)]

    lane8 = lax.broadcasted_iota(jnp.int32, (1, 128), 1) & 7

    def read(b, rows, bucket, scale, lev):
        r = jnp.dot(bcs[rows, 128:], bucket, preferred_element_type=F32)
        for h in range(4):
            cols = slice(128 * h, 128 * h + 128)
            yacc[rows, cols] += r[:, cols] * halves_of(scale, 16 * h + lev, 16 * h + 8 + lev, first)

    def scales(rows, add):
        return pltpu.roll(jnp.exp(cu[rows, :] + add), 64, 1) * td[rows, :]

    zero = jnp.zeros((1, 128), F32)
    block = [pl.ds(b * ROWS, ROWS) for b in range(4)]
    read(1, block[1], near_st[0], scales(block[1], zero), 1)
    read(2, block[2], near_st[1], scales(block[2], zero), 2)
    sc = scales(block[3], jnp.where(lane8 == 2, ends[2:3, :], 0.0))
    read(3, block[3], near_st[2], sc, 1)
    read(3, block[3], near_st[1], sc, 2)

    row_of = lax.broadcasted_iota(jnp.int32, (GROUPS, 1), 0)
    outer = zero
    for l in range(LEVELS_OUT):
        start = lax.div(g, 2**l) * 2**l
        summed = jnp.sum(jnp.where((row_of >= start) & (row_of < g), logs, 0.0), axis=0, keepdims=True)
        outer = jnp.where(lane8 == l + 3, summed, outer)
    run = zero
    for b in range(4):
        eb[4 + b : 5 + b, :] = run + outer
        run = run + ends[b : b + 1, :]

    for l in range(LEVELS_OUT):
        @pl.when(bits[l] == 1)
        def _():
            remote(rcv2.at[l, pl.ds(0, GROUPS - 1)], rcv2.at[l, pl.ds(0, GROUPS - 1)], lsend.at[l], lrecv.at[l], group(g)).wait_recv()
            rcv2[l, g] = table[TABLE[l] + lax.div(g, 2 ** (l + 1))]

        @pl.when(bits[l] == 0)
        def _():
            rcv2[l] = jnp.zeros((GROUPS, 16, 128), BF16)

    def finish(n, _):
        b = lax.rem(y + n, NY)
        base = pl.multiple_of(b * ROWS, ROWS)
        for half in range(2):
            rows = pl.ds(pl.multiple_of(base + 128 * half, 128), 128)
            scale = scales(rows, eb[pl.ds(4 + b, 1), :])
            c = bcs[rows, 128:]
            for h in range(0, 4, 2):
                vals = [yacc[rows, 128 * (h + e) : 128 * (h + e) + 128] for e in range(2)]
                for l in range(LEVELS_OUT):
                    pair = [rcv2[l, 8 * (h + e) : 8 * (h + e) + 8].reshape(128, 128) for e in range(2)]
                    r = jnp.dot(c, jnp.concatenate(pair, axis=1), preferred_element_type=F32)
                    for e in range(2):
                        lane = 16 * (h + e) + l + 3
                        vals[e] = vals[e] + r[:, 128 * e : 128 * e + 128] * halves_of(scale, lane, lane + 8, first)
                for e in range(2):
                    cols = slice(128 * (h + e), 128 * (h + e) + 128)
                    zg = p[rows, 768 + 128 * (h + e) : 896 + 128 * (h + e)].astype(F32)
                    qs[b, 128 * half : 128 * half + 128, cols] = (vals[e] * jax.nn.silu(zg)).astype(BF16)

        @pl.when(n < 4)
        def _():
            remote(qs.at[b], qr.at[y], qsend.at[n], qrecv.at[n], beside(n)).start()

        return 0

    lax.fori_loop(1, 5, finish, 0)
    qr[y] = qs[y]
    for copy in loads:
        copy.wait()

    squares = jnp.zeros((ROWS, 1), F32)
    for at, n in enumerate((0, 1, 3, 2)):
        src = lax.rem(y + NY - n, NY)
        if n:
            remote(qs.at[0], qr.at[src], qsend.at[n], qrecv.at[n], beside(n)).wait_recv()
        v = qr[src].astype(F32)
        squares = squares + jnp.sum(v * v, axis=1, keepdims=True)
        lanes = pl.ds(pl.multiple_of(src * 512, 512), 512)
        v = (v * gg[:, lanes]).astype(BF16)
        for t in range(4):
            cols = slice(512 * t, 512 * t + 512)
            part = jnp.dot(v, wout[lanes, cols], preferred_element_type=F32)
            acc[:, cols] = part if at == 0 else acc[:, cols] + part
    r = lax.rsqrt(squares * (1.0 / 2048.0) + EPS)
    sends = []
    for t in range(4):
        cols = slice(512 * t, 512 * t + 512)
        os[t] = (acts[:, cols].astype(F32) + r * acc[:, cols]).astype(BF16)
        sends.append(remote(os.at[t], oin.at[t], osend.at[t], orecv.at[t], {"section": 1 - s}))
        sends[-1].start()
    stores = []
    for t in range(4):
        sends[t].wait_recv()
        stores.append(pltpu.make_async_copy(oin.at[t], out.at[:, pl.ds(512 * t, 512)], dsem.at[t]))
        stores[-1].start()
    back.wait_send()
    remote(rcv1.at[pl.ds(0, GROUPS - 1)], rcv1.at[pl.ds(0, GROUPS - 1)], ssem.at[0], rsem.at[0], group(g)).wait_send()
    remote(rlog.at[pl.ds(0, GROUPS - 1)], rlog.at[pl.ds(0, GROUPS - 1)], ssem.at[1], rsem.at[1], group(g)).wait_send()
    for l in range(LEVELS_OUT):
        for bit in range(2):
            @pl.when(bits[l] == bit)
            def _():
                some = rcv2.at[l, pl.ds(0, 16 - bit)]
                remote(some, some, lsend.at[l], lrecv.at[l], group(g)).wait_send()
    for n in (1, 2, 3):
        remote(qs.at[0], qr.at[y], qsend.at[n], qrecv.at[n], beside(n)).wait_send()
    for copy in sends:
        copy.wait_send()
    for copy in stores:
        copy.wait()


def mix(p, acts, wout, *params):
    vmem = pl.BlockSpec(memory_space=pltpu.VMEM)
    anywhere = pl.BlockSpec(memory_space=pl.ANY)
    n = NY * ROWS
    dma = pltpu.SemaphoreType.DMA
    return pl.pallas_call(
        mixer_kernel,
        out_shape=jax.ShapeDtypeStruct((ROWS, 2048), BF16),
        in_specs=[vmem, anywhere, anywhere] + [vmem] * len(params),
        out_specs=anywhere,
        scratch_shapes=[
            pltpu.VMEM((n + 8, 768), F32),
            pltpu.VMEM((n, 512), F32),
            pltpu.VMEM((n, 256), BF16),
            pltpu.VMEM((n, 128), F32),
            pltpu.VMEM((n, 128), F32),
            pltpu.VMEM((n, 512), F32),
            pltpu.VMEM((3, 128, 512), BF16),
            pltpu.VMEM((8, 128), F32),
            pltpu.VMEM((8, 512), F32),
            pltpu.VMEM((GROUPS, 16, 128), BF16),
            pltpu.VMEM((8, 128), F32),
            pltpu.VMEM((GROUPS, 16, 128), BF16),
            pltpu.VMEM((GROUPS, 8, 128), F32),
            pltpu.VMEM((31, 16, 128), BF16),
            pltpu.VMEM((LEVELS_OUT, GROUPS, 16, 128), BF16),
            pltpu.VMEM((16, 768), BF16),
            pltpu.VMEM((NY, ROWS, 512), BF16),
            pltpu.VMEM((NY, ROWS, 512), BF16),
            pltpu.VMEM((2048, 2048), BF16),
            pltpu.VMEM((ROWS, 2048), BF16),
            pltpu.VMEM((ROWS, 2048), F32),
            pltpu.VMEM((4, ROWS, 512), BF16),
            pltpu.VMEM((4, ROWS, 512), BF16),
            dma((2,)), dma((2,)), dma((2,)), dma((5,)), dma((5,)), dma((2,)), dma((4,)), dma((4,)), dma((4,)), dma((4,)), dma((4,)),
        ],
        compiler_params=pltpu.CompilerParams(
            collective_id=1, has_side_effects=True, vmem_limit_bytes=52 * 1024 * 1024),
        name="mix",
    )(p, acts, wout, *params)


def per_device(acts, in_proj, out_proj, conv_weight, conv_bias, dt_bias, decay_rate, skip_gain, level_bias, norm_gain, gate_gain):
    wa, wb = column_slices(in_proj[0])
    p = gather_project(acts[0], wa, wb, norm_gain)
    o = mix(p, acts[0], out_proj[0], conv_weight[0], conv_bias, dt_bias, decay_rate, skip_gain, level_bias, gate_gain)
    return o[None]


def solution(mesh):
    two = P("section", None)
    three = P("section", None, None)
    return jax.shard_map(
        per_device,
        mesh=mesh,
        in_specs=(P("section", "seq", None), P("section", "seq", None), three, three, two, two, two, two, two, two, two),
        out_specs=P("section", "seq", None),
        check_vma=False,
    )
```

```python
import functools
import jax
import jax.numpy as jnp
from jax import lax
from jax.experimental import pallas as pl
from jax.experimental.pallas import tpu as pltpu
from jax.sharding import PartitionSpec as P

EPS = 1e-05
MESH = pl.DeviceIdType.MESH
NX, NZ, NY = 4, 8, 4
GROUPS = NX * NZ
CA, CB = 512, 896
NP = CA + CB
ROWS = 256
F32, BF16 = jnp.float32, jnp.bfloat16


def seq_of(x, z, y):
    return (lax.rem(x + 4 * NX, NX) * NZ + lax.rem(z + 4 * NZ, NZ)) * NY + lax.rem(y + 4 * NY, NY)


def plan():
    msgs = {}
    ua, ub, un = 64 * CA * 2, 64 * CB * 2, 128 * 2048 * 2
    for d, links in ((1, {"y+": 1}), (3, {"y-": 1}), (2, {"y+": 1, "y-": 1})):
        msgs[("w", d)] = ("w", None, (0, 0, d), None, 16 * NP * 2, links)
    msgs[("P", 0)] = ("h0", 0, (0, 0, 1), None, un, {"y+": 1})
    msgs[("M", 1)] = ("h1", 0, (0, 0, -1), None, un, {"y-": 1})
    msgs[("P", 1)] = ("h1", 0, (0, 0, 1), None, un, {"y+": 1})
    msgs[("M", 0)] = ("h0", 0, (0, 0, -1), None, un, {"y-": 1})
    msgs[("P", 2)] = ("h0", -1, (0, 0, 1), ("P", 0), un, {"y+": 1})
    msgs[("M", 2)] = ("h1", 1, (0, 0, -1), ("M", 1), un, {"y-": 1})
    own = "own"
    for d, links in ((1, {"x+": 1}), (3, {"x-": 1}), (2, {"x+": 2})):
        msgs[("A1", d)] = ("a", (0, 0), (d, 0, 0), own, ua, links)
    for k in range(1, 5):
        if k < 5:
            dep = own if k == 1 else ("B1+", k - 1)
            msgs[("B1+", k)] = ("b", (0, -(k - 1)), (0, 1, 0), dep, ub, {"z+": 1})
        if k < 4:
            dep = own if k == 1 else ("B1-", k - 1)
            msgs[("B1-", k)] = ("b", (0, k - 1), (0, -1, 0), dep, ub, {"z-": 1})
    for k in range(1, 5):
        for d in range(4):
            up, down = (4, 3) if d < 2 else (3, 4)
            if k <= up:
                dep = (own if d == 0 else ("A1", d)) if k == 1 else ("A2+", d, k - 1)
                msgs[("A2+", d, k)] = ("a", (-d, -(k - 1)), (0, 1, 0), dep, ua, {"z+": 1})
            if k <= down:
                dep = (own if d == 0 else ("A1", d)) if k == 1 else ("A2-", d, k - 1)
                msgs[("A2-", d, k)] = ("a", (-d, k - 1), (0, -1, 0), dep, ua, {"z-": 1})
    offs = [0, -1, 1, -2, 2, -3, 3, -4]
    for n, o in enumerate(offs):
        dep = own if o == 0 else (("B1+", -o) if o < 0 else ("B1-", o))
        msgs[("B2+", o)] = ("b", (0, o), (1, 0, 0), dep, ub, {"x+": 1})
        msgs[("B2-", o)] = ("b", (0, o), (-1, 0, 0), dep, ub, {"x-": 1})
        if n in (1, 3, 5):
            msgs[("B2+2", o)] = ("b", (-1, o), (1, 0, 0), ("B2+", o), ub, {"x+": 1})
        else:
            msgs[("B2-2", o)] = ("b", (1, o), (-1, 0, 0), ("B2-", o), ub, {"x-": 1})
    return msgs


def schedule(msgs, rate=46.6e3, latency=1.9):
    free, arrive, order = {}, {}, []
    started = set()
    events = []

    def start(name, now):
        part, chunk, to, dep, size, links = msgs[name]
        begin = max([now] + [free.get(l, 0.0) for l in links])
        end = begin
        for l, n in links.items():
            free[l] = begin + size * n / rate
            end = max(end, free[l])
        arrive[name] = end + latency
        events.append((end + latency, len(started), name))
        started.add(name)

    for name, m in msgs.items():
        if m[3] is None:
            start(name, 0.0)
    got = set()
    while events:
        events.sort()
        now, _, name = events.pop(0)
        order.append(name)
        got.add(name)
        if all(("w", d) in got for d in (1, 2, 3)) and "own" not in got:
            got.add("own")
            order.append("own")
            for other, m in msgs.items():
                if m[3] == "own":
                    start(other, now)
        for other, m in msgs.items():
            if m[3] == name:
                start(other, now)
    return order, arrive


HI = lax.Precision.HIGHEST
MID = CA + 768
LEVELS_OUT = 5
TABLE = (0, 16, 24, 28, 30)


def spread(row, lanes):
    k = lax.broadcasted_iota(jnp.int32, (128, lanes), 0)
    c = lax.broadcasted_iota(jnp.int32, (128, lanes), 1)
    return jnp.dot(row, (k == 64 + 8 * lax.shift_right_logical(c, 6)).astype(F32), precision=HI, preferred_element_type=F32)


def halves_of(a, lane_low, lane_high, first):
    return jnp.where(first, a[:, lane_low : lane_low + 1], a[:, lane_high : lane_high + 1])


def softplus(v):
    return jnp.maximum(v, 0.0) + jnp.log1p(jnp.exp(-jnp.abs(v)))


def layer_kernel(acts_in, proj_in, wout_in, gain_in, cw_in, cb_in, dtb_in, rate_in, skip_in, lb_in, gg_in, out,
                 wa, wb, ablk, u, p, proj, small,
                 gain, cw, cb, dtb, rate, skip, lb, gg,
                 ext, xf, bcs, td, cu, yacc, near_st, eb, ee, snd1, slog, rcv1, rlog, table, rcv2, tail,
                 qs, qr, wout, acc, os, oin,
                 local_sems, send_sems, recv_sems, in_sems,
                 ssem, rsem, lsend, lrecv, tsem, qsend, qrecv, osend, orecv, dsem):
    i = lax.axis_index("seq")
    y = lax.rem(i, NY)
    g = lax.div(i, NY)
    z = lax.rem(g, NZ)
    x = lax.div(g, NZ)
    s = lax.axis_index("section")

    def there(dx, dz, dy):
        return {"seq": seq_of(x + dx, z + dz, y + dy)}

    def group(n):
        return {"seq": n * NY + y}

    def beside(n):
        return {"seq": g * NY + lax.rem(y + n, NY)}

    def wrap(n):
        return lax.rem(n, GROUPS)

    def remote(src, dst, send, recv, to):
        return pltpu.make_async_remote_copy(
            src_ref=src, dst_ref=dst, send_sem=send, recv_sem=recv, device_id=to, device_id_type=MESH)

    with jax.named_scope("enter"):
        barrier = pltpu.get_barrier_semaphore()

        def greet(d, _):
            pl.semaphore_signal(barrier, inc=1, device_id=group(wrap(g + d)), device_id_type=MESH)
            return 0

        lax.fori_loop(1, GROUPS, greet, 0)
        for d in (1, 2, 3):
            pl.semaphore_signal(barrier, inc=1, device_id=beside(d), device_id_type=MESH)
        pl.semaphore_signal(barrier, inc=1, device_id={"section": 1 - s}, device_id_type=MESH)
        pairs = ((proj_in, proj), (acts_in, ablk.at[y]), (gain_in, gain), (cw_in, cw), (cb_in, cb), (dtb_in, dtb),
                 (rate_in, rate), (skip_in, skip), (lb_in, lb), (gg_in, gg), (wout_in, wout))
        loads = [pltpu.make_async_copy(a, b, in_sems.at[n]) for n, (a, b) in enumerate(pairs)]
        for copy in loads[:-1]:
            copy.start()

        loads[0].wait()
        rows_k = lax.broadcasted_iota(jnp.int32, (288, 128), 0)
        lane_k = lax.broadcasted_iota(jnp.int32, (288, 128), 1)
        packed = proj[:, 4352:]
        for n in range(NY):
            from_lr = (lane_k < 64) & (rows_k == 32 + 64 * n + lane_k)
            from_dr = (lane_k >= 64) & (rows_k == 8 * n + lax.shift_right_logical(lane_k - 64, 3))
            hit = (from_lr | from_dr).astype(BF16)
            small[n] = jnp.dot(packed, hit, preferred_element_type=F32).astype(BF16)

        msgs = plan()
        number = {name: n for n, name in enumerate(msgs)}
        order, _ = schedule(msgs)

        def block(rel):
            return lax.rem(y + rel + 2 * NY, NY)

        def rows_of(cx, cz):
            return pl.ds(pl.multiple_of(seq_of(x + cx, z + cz, 0) * 16, 64), 64)

        def pieces(slot, rows):
            cols = pl.multiple_of(slot * 512, 512)
            return [(proj.at[:, pl.ds(cols, 512)], wa.at[rows]),
                    (proj.at[:, pl.ds(2048, 256)], wb.at[rows, pl.ds(0, 256)]),
                    (proj.at[:, pl.ds(pl.multiple_of(2304 + cols, 256), 512)], wb.at[rows, pl.ds(256, 512)]),
                    (small.at[slot], wb.at[rows, pl.ds(768, 128)])]

        mine = pl.ds(pl.multiple_of(i * 16, 16), 16)
        local = [pltpu.make_async_copy(a, b, local_sems.at[n]) for n, (a, b) in enumerate(pieces(y, mine))]
        for copy in local:
            copy.start()
        loads[1].wait()
        pl.semaphore_wait(barrier, GROUPS - 1 + 3 + 1)

    def copies(name, arriving):
        part, chunk, to, dep, _, _ = msgs[name]
        n = number[name]
        back = to if arriving else (0, 0, 0)
        if part == "w":
            d = to[2]
            rows = pl.ds(pl.multiple_of(seq_of(x, z, y - d) * 16, 16), 16) if arriving else mine
            slot = lax.rem(y + d, NY)
            return [remote(a, b, send_sems.at[n if e == 0 else len(msgs) + 3 * n + e], recv_sems.at[n if e == 0 else len(msgs) + 3 * n + e], there(*to))
                    for e, (a, b) in enumerate(pieces(slot, rows))]
        if part in ("h0", "h1"):
            ref = ablk.at[block(chunk - back[2]), pl.ds(128 * int(part[1]), 128)]
        else:
            ref = (wa if part == "a" else wb).at[rows_of(chunk[0] - back[0], chunk[1] - back[1])]
        return [remote(ref, ref, send_sems.at[n], recv_sems.at[n], there(*to))]

    def start(name):
        for copy in copies(name, False):
            copy.start()

    def normed(rel, half):
        def step(n, _):
            at = pl.multiple_of(half * 128 + n * 64, 64)
            b = block(rel)
            h = ablk[b, pl.ds(at, 64), :].astype(F32)
            r = lax.rsqrt(jnp.mean(h * h, axis=1, keepdims=True) + EPS)
            u[pl.ds(pl.multiple_of(b * ROWS + at, 64), 64), :] = (h * r * gain[...]).astype(BF16)
            return 0

        lax.fori_loop(0, 2, step, 0)

    with jax.named_scope("gather"):
        for name, m in msgs.items():
            if m[3] is None:
                start(name)
        for copy in loads[2:-1]:
            copy.wait()
        loads[-1].start()
        normed(0, 0)
        normed(0, 1)
        halves = {("P", 0): (-1, 0), ("P", 1): (-1, 1), ("M", 1): (1, 1), ("M", 0): (1, 0), ("P", 2): (-2, 0), ("M", 2): (2, 1)}
        for name in order:
            if name == "own":
                for copy in local:
                    copy.wait()
            else:
                for copy in copies(name, True):
                    copy.wait_recv()
            for other, m in msgs.items():
                if m[3] == name:
                    start(other)
            if name in halves:
                normed(*halves[name])

    def product(n, _):
        rows = pl.ds(pl.multiple_of(n * 512, 512), 512)
        p[rows, :CA] = jnp.dot(u[rows, :], wa[...], preferred_element_type=F32).astype(BF16)
        p[rows, CA:] = jnp.dot(u[rows, :], wb[...], preferred_element_type=F32).astype(BF16)
        return 0

    with jax.named_scope("project"):
        lax.fori_loop(0, 2, product, 0)

    with jax.named_scope("rows"):
        def picked(v, hit):
            rows = jnp.broadcast_to(v[...], (8, v.shape[1]))
            return jnp.dot(rows, hit.astype(F32), precision=HI, preferred_element_type=F32)[:1]

        def two(rows, lanes):
            return (lax.broadcasted_iota(jnp.int32, (rows, lanes), 0), lax.broadcasted_iota(jnp.int32, (rows, lanes), 1))

        k, c = two(32, 128)
        of_head = (c >= 64) & (k == 8 * y + lax.shift_right_logical(c - 64, 3))
        k2, c2 = two(256, 128)
        bias = picked(dtb, of_head) + picked(lb, (c2 < 64) & (k2 == 64 * y + c2))
        rates = picked(rate, of_head)
        k3, c3 = two(32, 512)
        skips = picked(skip, k3 == 8 * y + lax.shift_right_logical(c3, 6))

        low_tri = (lax.broadcasted_iota(jnp.int32, (ROWS, ROWS), 1) <= lax.broadcasted_iota(jnp.int32, (ROWS, ROWS), 0)).astype(BF16)
        for b in range(4):
            rows = slice(b * ROWS, (b + 1) * ROWS)
            t = softplus(p[rows, MID:].astype(F32) + bias)
            td[rows, :] = t
            left = -t * rates
            total = jnp.zeros((ROWS, 128), F32)
            for _ in range(3):
                piece = left.astype(BF16)
                total = total + jnp.dot(low_tri, piece, preferred_element_type=F32)
                left = left - piece.astype(F32)
            cu[rows, :] = total
            eb[b : b + 1, :] = total[ROWS - 1 :, :]
        eb[4:, :] = jnp.zeros((4, 128), F32)
        ends = eb[...]
        ee[...] = jnp.exp(spread(ends, 512))
        slog[...] = jnp.broadcast_to(jnp.sum(ends, axis=0, keepdims=True), (8, 128))

    with jax.named_scope("conv"):
        back = remote(p.at[pl.ds(1008, 16), pl.ds(0, 768)], tail, tsem.at[0], tsem.at[1], group(wrap(g + 1)))
        back.start()

        for n in range(4):
            ext[8 + n * ROWS : 8 + (n + 1) * ROWS, :] = p[n * ROWS : (n + 1) * ROWS, :768].astype(F32)
        own = pl.ds(pl.multiple_of(y * 512, 512), 512)
        tx = [cw[k : k + 1, own] for k in range(4)]
        tb = [cw[k : k + 1, 2048:] for k in range(4)]
        bx, bb = cb[:, own], cb[:, 2048:]

        def convolved(n):
            at = n * 128
            v = bx
            for k in range(4):
                v = v + tx[k] * ext[at + 5 + k : at + 133 + k, :512]
            xf[at : at + 128, :] = jax.nn.silu(v)
            v = bb
            for k in range(4):
                v = v + tb[k] * ext[at + 5 + k : at + 133 + k, 512:]
            bcs[at : at + 128, :] = jax.nn.silu(v).astype(BF16)

        for n in range(1, 8):
            convolved(n)
        back.wait_recv()
        before = tail[...].astype(F32)
        ext[0:8, :] = jnp.where(g > 0, before[8:, :], 0.0)
        convolved(0)

    with jax.named_scope("states"):
        first = lax.broadcasted_iota(jnp.int32, (1, 128), 1) < 64

        def state(b):
            rows = slice(b * ROWS, (b + 1) * ROWS)
            tl = jnp.exp(ends[b : b + 1, :] - cu[rows, :]) * td[rows, :]
            parts = []
            for h in range(4):
                parts.append((xf[rows, 128 * h : 128 * h + 128] * halves_of(tl, 64 + 16 * h, 72 + 16 * h, first)).astype(BF16))
            xt = jnp.concatenate(parts, axis=1)
            return lax.dot_general(bcs[rows, :128], xt, (((0,), (0,)), ((), ())), preferred_element_type=F32)

        st = state(0)
        near_st[0] = st.astype(BF16)
        st = ee[1:2, :] * st + state(1)
        near_st[1] = st.astype(BF16)
        other = state(2)
        near_st[2] = other.astype(BF16)
        st = ee[2:3, :] * ee[3:4, :] * st + ee[3:4, :] * other + state(3)
        st = st.astype(BF16)
        for n in range(GROUPS):
            ct, nt = n // 8, n % 8
            snd1[n] = st[16 * nt : 16 * nt + 16, 128 * ct : 128 * ct + 128]

        def first_send(d, _):
            to = wrap(g + d)
            remote(snd1.at[to], rcv1.at[g], ssem.at[0], rsem.at[0], group(to)).start()
            remote(slog, rlog.at[g], ssem.at[1], rsem.at[1], group(to)).start()
            return 0

        lax.fori_loop(1, GROUPS, first_send, 0)
        rcv1[g] = snd1[g]
        rlog[g] = slog[...]

    with jax.named_scope("inside"):
        def inside(b, _):
            base = pl.multiple_of(b * ROWS, ROWS)
            every = pl.ds(base, ROWS)
            cum_t = jnp.transpose(cu[every, :])
            dt_t = jnp.transpose(td[every, :])
            for r in range(2):
                rows = pl.ds(pl.multiple_of(base + 128 * r, 128), 128)
                wide = 128 * (r + 1)
                seen = pl.ds(base, wide)
                scores = lax.dot_general(bcs[rows, 128:], bcs[seen, :128], (((1,), (1,)), ((), ())), preferred_element_type=F32)
                ti, si = two(128, wide)
                causal = si <= ti + 128 * r
                cum, lam = cu[rows, :], td[rows, :]
                for h in range(4):
                    xp = xf[seen, 128 * h : 128 * h + 128].astype(BF16)
                    got = []
                    for e in (2 * h, 2 * h + 1):
                        lane = 64 + 8 * e
                        differ = jnp.where(causal, cum[:, lane : lane + 1] - cum_t[lane : lane + 1, :wide], -1e30)
                        w = scores * jnp.exp(differ) * dt_t[lane : lane + 1, :wide]
                        got.append(jnp.dot(w.astype(BF16), xp, preferred_element_type=F32))
                    val = jnp.where(first, got[0], got[1]) * halves_of(lam, 16 * h, 16 * h + 8, first)
                    cols = slice(128 * h, 128 * h + 128)
                    yacc[rows, cols] = val + skips[:, cols] * xf[rows, cols]
            return 0

        lax.fori_loop(0, 4, inside, 0)

    with jax.named_scope("wait1"):
        remote(rcv1.at[pl.ds(0, GROUPS - 1)], rcv1.at[pl.ds(0, GROUPS - 1)], ssem.at[0], rsem.at[0], group(g)).wait_recv()
        remote(rlog.at[pl.ds(0, GROUPS - 1)], rlog.at[pl.ds(0, GROUPS - 1)], ssem.at[1], rsem.at[1], group(g)).wait_recv()
    with jax.named_scope("merge"):
        logs = rlog[:, 0, :]
        wide_logs = spread(logs, 512)
        ct = lax.div(g, 8)
        head_logs = jnp.zeros((GROUPS, 128), F32)
        for n in range(4):
            head_logs = jnp.where(ct == n, wide_logs[:, 128 * n : 128 * n + 128], head_logs)
        level = [rcv1[n].astype(F32) for n in range(GROUPS)]
        ends_of = [head_logs[n : n + 1, :] for n in range(GROUPS)]
        for l in range(LEVELS_OUT):
            for n in range(0, len(level), 2):
                table[TABLE[l] + n // 2] = level[n].astype(BF16)
            level = [jnp.exp(ends_of[n + 1]) * level[n] + level[n + 1] for n in range(0, len(level), 2)]
            ends_of = [ends_of[n] + ends_of[n + 1] for n in range(0, len(ends_of), 2)]

        def second_send(d, _):
            to = wrap(g + d)
            for l in range(LEVELS_OUT):
                up = lax.div(to, 2**l)

                @pl.when(lax.rem(up, 2) == 1)
                def _():
                    remote(table.at[TABLE[l] + lax.div(up, 2)], rcv2.at[l, g], lsend.at[l], lrecv.at[l], group(to)).start()

            return 0

        lax.fori_loop(1, GROUPS, second_send, 0)
    with jax.named_scope("near"):
        bits = [lax.rem(lax.div(g, 2**l), 2) for l in range(LEVELS_OUT)]

        lane8 = lax.broadcasted_iota(jnp.int32, (1, 128), 1) & 7

        def read(b, rows, bucket, scale, lev):
            r = jnp.dot(bcs[rows, 128:], bucket, preferred_element_type=F32)
            for h in range(4):
                cols = slice(128 * h, 128 * h + 128)
                yacc[rows, cols] += r[:, cols] * halves_of(scale, 16 * h + lev, 16 * h + 8 + lev, first)

        def scales(rows, add):
            return pltpu.roll(jnp.exp(cu[rows, :] + add), 64, 1) * td[rows, :]

        zero = jnp.zeros((1, 128), F32)
        at_block = [pl.ds(b * ROWS, ROWS) for b in range(4)]
        read(1, at_block[1], near_st[0], scales(at_block[1], zero), 1)
        read(2, at_block[2], near_st[1], scales(at_block[2], zero), 2)
        sc = scales(at_block[3], jnp.where(lane8 == 2, ends[2:3, :], 0.0))
        read(3, at_block[3], near_st[2], sc, 1)
        read(3, at_block[3], near_st[1], sc, 2)

        row_of = lax.broadcasted_iota(jnp.int32, (GROUPS, 1), 0)
        outer = zero
        for l in range(LEVELS_OUT):
            start = lax.div(g, 2**l) * 2**l
            summed = jnp.sum(jnp.where((row_of >= start) & (row_of < g), logs, 0.0), axis=0, keepdims=True)
            outer = jnp.where(lane8 == l + 3, summed, outer)
        run = zero
        for b in range(4):
            eb[4 + b : 5 + b, :] = run + outer
            run = run + ends[b : b + 1, :]

    with jax.named_scope("wait2"):
        for l in range(LEVELS_OUT):
            @pl.when(bits[l] == 1)
            def _():
                remote(rcv2.at[l, pl.ds(0, GROUPS - 1)], rcv2.at[l, pl.ds(0, GROUPS - 1)], lsend.at[l], lrecv.at[l], group(g)).wait_recv()
                rcv2[l, g] = table[TABLE[l] + lax.div(g, 2 ** (l + 1))]

            @pl.when(bits[l] == 0)
            def _():
                rcv2[l] = jnp.zeros((GROUPS, 16, 128), BF16)

    with jax.named_scope("finish"):
        def finish(n, _):
            b = lax.rem(y + n, NY)
            base = pl.multiple_of(b * ROWS, ROWS)
            for half in range(2):
                rows = pl.ds(pl.multiple_of(base + 128 * half, 128), 128)
                scale = scales(rows, eb[pl.ds(4 + b, 1), :])
                c = bcs[rows, 128:]
                for h in range(0, 4, 2):
                    vals = [yacc[rows, 128 * (h + e) : 128 * (h + e) + 128] for e in range(2)]
                    for l in range(LEVELS_OUT):
                        pair = [rcv2[l, 8 * (h + e) : 8 * (h + e) + 8].reshape(128, 128) for e in range(2)]
                        r = jnp.dot(c, jnp.concatenate(pair, axis=1), preferred_element_type=F32)
                        for e in range(2):
                            lane = 16 * (h + e) + l + 3
                            vals[e] = vals[e] + r[:, 128 * e : 128 * e + 128] * halves_of(scale, lane, lane + 8, first)
                    for e in range(2):
                        cols = slice(128 * (h + e), 128 * (h + e) + 128)
                        zg = p[rows, 768 + 128 * (h + e) : 896 + 128 * (h + e)].astype(F32)
                        qs[b, 128 * half : 128 * half + 128, cols] = (vals[e] * jax.nn.silu(zg)).astype(BF16)

            @pl.when(n < 4)
            def _():
                remote(qs.at[b], qr.at[y], qsend.at[n], qrecv.at[n], beside(n)).start()

            return 0

        lax.fori_loop(1, 5, finish, 0)
    with jax.named_scope("out"):
        qr[y] = qs[y]
        loads[-1].wait()

        squares = jnp.zeros((ROWS, 1), F32)
        for at, n in enumerate((0, 1, 3, 2)):
            src = lax.rem(y + NY - n, NY)
            if n:
                remote(qs.at[0], qr.at[src], qsend.at[n], qrecv.at[n], beside(n)).wait_recv()
            v = qr[src].astype(F32)
            squares = squares + jnp.sum(v * v, axis=1, keepdims=True)
            lanes = pl.ds(pl.multiple_of(src * 512, 512), 512)
            v = (v * gg[:, lanes]).astype(BF16)
            for t in range(4):
                cols = slice(512 * t, 512 * t + 512)
                part = jnp.dot(v, wout[lanes, cols], preferred_element_type=F32)
                acc[:, cols] = part if at == 0 else acc[:, cols] + part
    with jax.named_scope("swap"):
        r = lax.rsqrt(squares * (1.0 / 2048.0) + EPS)
        sends = []
        for t in range(4):
            cols = slice(512 * t, 512 * t + 512)
            os[t] = (ablk[y, :, cols].astype(F32) + r * acc[:, cols]).astype(BF16)
            sends.append(remote(os.at[t], oin.at[t], osend.at[t], orecv.at[t], {"section": 1 - s}))
            sends[-1].start()
        stores = []
        for t in range(4):
            sends[t].wait_recv()
            stores.append(pltpu.make_async_copy(oin.at[t], out.at[:, pl.ds(512 * t, 512)], dsem.at[t]))
            stores[-1].start()
    with jax.named_scope("drain"):
        for name in msgs:
            for copy in copies(name, False):
                copy.wait_send()
        back.wait_send()
        remote(rcv1.at[pl.ds(0, GROUPS - 1)], rcv1.at[pl.ds(0, GROUPS - 1)], ssem.at[0], rsem.at[0], group(g)).wait_send()
        remote(rlog.at[pl.ds(0, GROUPS - 1)], rlog.at[pl.ds(0, GROUPS - 1)], ssem.at[1], rsem.at[1], group(g)).wait_send()
        for l in range(LEVELS_OUT):
            for bit in range(2):
                @pl.when(bits[l] == bit)
                def _():
                    some = rcv2.at[l, pl.ds(0, 16 - bit)]
                    remote(some, some, lsend.at[l], lrecv.at[l], group(g)).wait_send()
        for n in (1, 2, 3):
            remote(qs.at[0], qr.at[y], qsend.at[n], qrecv.at[n], beside(n)).wait_send()
        for copy in sends:
            copy.wait_send()
        for copy in stores:
            copy.wait()


def layer(acts, proj, wout, *params):
    anywhere = pl.BlockSpec(memory_space=pl.ANY)
    n = NY * ROWS
    count = 4 * len(plan())
    dma = pltpu.SemaphoreType.DMA
    return pl.pallas_call(
        layer_kernel,
        out_shape=jax.ShapeDtypeStruct((ROWS, 2048), BF16),
        in_specs=[anywhere] * (3 + len(params)),
        out_specs=anywhere,
        scratch_shapes=[
            pltpu.VMEM((2048, CA), BF16),
            pltpu.VMEM((2048, CB), BF16),
            pltpu.VMEM((NY, ROWS, 2048), BF16),
            pltpu.VMEM((n, 2048), BF16),
            pltpu.VMEM((n, NP), BF16),
            pltpu.VMEM(proj.shape, BF16),
            pltpu.VMEM((NY, 16, 128), BF16),
            *[pltpu.VMEM(a.shape, a.dtype) for a in params],
            pltpu.VMEM((n + 8, 768), F32),
            pltpu.VMEM((n, 512), F32),
            pltpu.VMEM((n, 256), BF16),
            pltpu.VMEM((n, 128), F32),
            pltpu.VMEM((n, 128), F32),
            pltpu.VMEM((n, 512), F32),
            pltpu.VMEM((3, 128, 512), BF16),
            pltpu.VMEM((8, 128), F32),
            pltpu.VMEM((8, 512), F32),
            pltpu.VMEM((GROUPS, 16, 128), BF16),
            pltpu.VMEM((8, 128), F32),
            pltpu.VMEM((GROUPS, 16, 128), BF16),
            pltpu.VMEM((GROUPS, 8, 128), F32),
            pltpu.VMEM((31, 16, 128), BF16),
            pltpu.VMEM((LEVELS_OUT, GROUPS, 16, 128), BF16),
            pltpu.VMEM((16, 768), BF16),
            pltpu.VMEM((NY, ROWS, 512), BF16),
            pltpu.VMEM((NY, ROWS, 512), BF16),
            pltpu.VMEM((2048, 2048), BF16),
            pltpu.VMEM((ROWS, 2048), F32),
            pltpu.VMEM((4, ROWS, 512), BF16),
            pltpu.VMEM((4, ROWS, 512), BF16),
            dma((4,)), dma((count,)), dma((count,)), dma((11,)),
            dma((2,)), dma((2,)), dma((5,)), dma((5,)), dma((2,)), dma((4,)), dma((4,)), dma((4,)), dma((4,)), dma((4,)),
        ],
        compiler_params=pltpu.CompilerParams(
            collective_id=0, has_side_effects=True, vmem_limit_bytes=62 * 1024 * 1024),
        name="layer",
    )(acts, proj, wout, *params)


def per_device(acts, in_proj, out_proj, conv_weight, conv_bias, dt_bias, decay_rate, skip_gain, level_bias, norm_gain, gate_gain):
    o = layer(acts[0], in_proj[0], out_proj[0], norm_gain, conv_weight[0], conv_bias, dt_bias, decay_rate, skip_gain, level_bias, gate_gain)
    return o[None]


def solution(mesh):
    two = P("section", None)
    three = P("section", None, None)
    return jax.shard_map(
        per_device,
        mesh=mesh,
        in_specs=(P("section", "seq", None), P("section", "seq", None), three, three, two, two, two, two, two, two, two),
        out_specs=P("section", "seq", None),
        check_vma=False,
    )
```

```python
import functools
import jax
import jax.numpy as jnp
from jax import lax
from jax.experimental import pallas as pl
from jax.experimental.pallas import tpu as pltpu
from jax.sharding import PartitionSpec as P

EPS = 1e-05
MESH = pl.DeviceIdType.MESH
NX, NZ, NY = 4, 8, 4
GROUPS = NX * NZ
CA, CB = 512, 896
NP = CA + CB
ROWS = 256
F32, BF16 = jnp.float32, jnp.bfloat16


def seq_of(x, z, y):
    return (lax.rem(x + 4 * NX, NX) * NZ + lax.rem(z + 4 * NZ, NZ)) * NY + lax.rem(y + 4 * NY, NY)


def plan():
    msgs = {}
    ua, ub, un = 64 * CA * 2, 64 * CB * 2, 128 * 2048 * 2
    for d, links in ((1, {"y+": 1}), (3, {"y-": 1}), (2, {"y+": 1, "y-": 1})):
        msgs[("w", d)] = ("w", None, (0, 0, d), None, 16 * NP * 2, links)
    msgs[("P", 0)] = ("h0", 0, (0, 0, 1), None, un, {"y+": 1})
    msgs[("M", 1)] = ("h1", 0, (0, 0, -1), None, un, {"y-": 1})
    msgs[("P", 1)] = ("h1", 0, (0, 0, 1), None, un, {"y+": 1})
    msgs[("M", 0)] = ("h0", 0, (0, 0, -1), None, un, {"y-": 1})
    msgs[("P", 2)] = ("h0", -1, (0, 0, 1), ("P", 0), un, {"y+": 1})
    msgs[("M", 2)] = ("h1", 1, (0, 0, -1), ("M", 1), un, {"y-": 1})
    own = "own"
    for d, links in ((1, {"x+": 1}), (3, {"x-": 1}), (2, {"x+": 2})):
        msgs[("A1", d)] = ("a", (0, 0), (d, 0, 0), own, ua, links)
    for k in range(1, 5):
        if k < 5:
            dep = own if k == 1 else ("B1+", k - 1)
            msgs[("B1+", k)] = ("b", (0, -(k - 1)), (0, 1, 0), dep, ub, {"z+": 1})
        if k < 4:
            dep = own if k == 1 else ("B1-", k - 1)
            msgs[("B1-", k)] = ("b", (0, k - 1), (0, -1, 0), dep, ub, {"z-": 1})
    for k in range(1, 5):
        for d in range(4):
            up, down = (4, 3) if d < 2 else (3, 4)
            if k <= up:
                dep = (own if d == 0 else ("A1", d)) if k == 1 else ("A2+", d, k - 1)
                msgs[("A2+", d, k)] = ("a", (-d, -(k - 1)), (0, 1, 0), dep, ua, {"z+": 1})
            if k <= down:
                dep = (own if d == 0 else ("A1", d)) if k == 1 else ("A2-", d, k - 1)
                msgs[("A2-", d, k)] = ("a", (-d, k - 1), (0, -1, 0), dep, ua, {"z-": 1})
    offs = [0, -1, 1, -2, 2, -3, 3, -4]
    for n, o in enumerate(offs):
        dep = own if o == 0 else (("B1+", -o) if o < 0 else ("B1-", o))
        msgs[("B2+", o)] = ("b", (0, o), (1, 0, 0), dep, ub, {"x+": 1})
        msgs[("B2-", o)] = ("b", (0, o), (-1, 0, 0), dep, ub, {"x-": 1})
        if n in (1, 3, 5):
            msgs[("B2+2", o)] = ("b", (-1, o), (1, 0, 0), ("B2+", o), ub, {"x+": 1})
        else:
            msgs[("B2-2", o)] = ("b", (1, o), (-1, 0, 0), ("B2-", o), ub, {"x-": 1})
    return msgs


def schedule(msgs, rate=46.6e3, latency=1.9):
    free, arrive, order = {}, {}, []
    started = set()
    events = []

    def start(name, now):
        part, chunk, to, dep, size, links = msgs[name]
        begin = max([now] + [free.get(l, 0.0) for l in links])
        end = begin
        for l, n in links.items():
            free[l] = begin + size * n / rate
            end = max(end, free[l])
        arrive[name] = end + latency
        events.append((end + latency, len(started), name))
        started.add(name)

    for name, m in msgs.items():
        if m[3] is None:
            start(name, 0.0)
    got = set()
    while events:
        events.sort()
        now, _, name = events.pop(0)
        order.append(name)
        got.add(name)
        if all(("w", d) in got for d in (1, 2, 3)) and "own" not in got:
            got.add("own")
            order.append("own")
            for other, m in msgs.items():
                if m[3] == "own":
                    start(other, now)
        for other, m in msgs.items():
            if m[3] == name:
                start(other, now)
    return order, arrive


HI = lax.Precision.HIGHEST
MID = CA + 768
LEVELS_OUT = 5
TABLE = (0, 16, 24, 28, 30)


def spread(row, lanes):
    k = lax.broadcasted_iota(jnp.int32, (128, lanes), 0)
    c = lax.broadcasted_iota(jnp.int32, (128, lanes), 1)
    return jnp.dot(row, (k == 64 + 8 * lax.shift_right_logical(c, 6)).astype(F32), precision=HI, preferred_element_type=F32)


def halves_of(a, lane_low, lane_high, first):
    return jnp.where(first, a[:, lane_low : lane_low + 1], a[:, lane_high : lane_high + 1])


def softplus(v):
    return jnp.maximum(v, 0.0) + jnp.log1p(jnp.exp(-jnp.abs(v)))


def layer_kernel(acts_in, proj_in, wout_in, gain_in, cw_in, cb_in, dtb_in, rate_in, skip_in, lb_in, gg_in, out,
                 wa, wb, ablk, u, pacc, p, proj, small, ones,
                 gain, cw, cb, dtb, rate, skip, lb, gg,
                 ext, xf, bcs, td, cu, yacc, near_st, eb, ee, snd1, slog, rcv1, rlog, table, rcv2, tail,
                 qs, qr, wout, acc, os,
                 local_sems, send_sems, recv_sems, in_sems,
                 ssem, rsem, lsend, lrecv, tsem, qsend, qrecv, osend, orecv):
    i = lax.axis_index("seq")
    y = lax.rem(i, NY)
    g = lax.div(i, NY)
    z = lax.rem(g, NZ)
    x = lax.div(g, NZ)
    s = lax.axis_index("section")

    def there(dx, dz, dy):
        return {"seq": seq_of(x + dx, z + dz, y + dy)}

    def group(n):
        return {"seq": n * NY + y}

    def beside(n):
        return {"seq": g * NY + lax.rem(y + n, NY)}

    def wrap(n):
        return lax.rem(n, GROUPS)

    def remote(src, dst, send, recv, to):
        return pltpu.make_async_remote_copy(
            src_ref=src, dst_ref=dst, send_sem=send, recv_sem=recv, device_id=to, device_id_type=MESH)

    with jax.named_scope("enter"):
        barrier = pltpu.get_barrier_semaphore()

        def greet(d, _):
            pl.semaphore_signal(barrier, inc=1, device_id=group(wrap(g + d)), device_id_type=MESH)
            return 0

        lax.fori_loop(1, GROUPS, greet, 0)
        for d in (1, 2, 3):
            pl.semaphore_signal(barrier, inc=1, device_id=beside(d), device_id_type=MESH)
        pl.semaphore_signal(barrier, inc=1, device_id={"section": 1 - s}, device_id_type=MESH)
        pairs = ((proj_in, proj), (acts_in, ablk.at[y]), (gain_in, gain), (cw_in, cw), (cb_in, cb), (dtb_in, dtb),
                 (rate_in, rate), (skip_in, skip), (lb_in, lb), (gg_in, gg), (wout_in, wout))
        loads = [pltpu.make_async_copy(a, b, in_sems.at[n]) for n, (a, b) in enumerate(pairs)]
        for copy in loads[:-1]:
            copy.start()

        loads[0].wait()
        rows_k = lax.broadcasted_iota(jnp.int32, (288, 128), 0)
        lane_k = lax.broadcasted_iota(jnp.int32, (288, 128), 1)
        packed = proj[:, 4352:]
        for n in range(NY):
            from_lr = (lane_k < 64) & (rows_k == 32 + 64 * n + lane_k)
            from_dr = (lane_k >= 64) & (rows_k == 8 * n + lax.shift_right_logical(lane_k - 64, 3))
            hit = (from_lr | from_dr).astype(BF16)
            small[n] = jnp.dot(packed, hit, preferred_element_type=F32).astype(BF16)

        msgs = plan()
        number = {name: n for n, name in enumerate(msgs)}
        order, _ = schedule(msgs)

        def block(rel):
            return lax.rem(y + rel + 2 * NY, NY)

        def rows_of(cx, cz):
            return pl.ds(pl.multiple_of(seq_of(x + cx, z + cz, 0) * 16, 64), 64)

        def pieces(slot, rows):
            cols = pl.multiple_of(slot * 512, 512)
            return [(proj.at[:, pl.ds(cols, 512)], wa.at[rows]),
                    (proj.at[:, pl.ds(2048, 256)], wb.at[rows, pl.ds(0, 256)]),
                    (proj.at[:, pl.ds(pl.multiple_of(2304 + cols, 256), 512)], wb.at[rows, pl.ds(256, 512)]),
                    (small.at[slot], wb.at[rows, pl.ds(768, 128)])]

        mine = pl.ds(pl.multiple_of(i * 16, 16), 16)
        local = [pltpu.make_async_copy(a, b, local_sems.at[n]) for n, (a, b) in enumerate(pieces(y, mine))]
        for copy in local:
            copy.start()
        loads[1].wait()
        pl.semaphore_wait(barrier, GROUPS - 1 + 3 + 1)

    def copies(name, arriving):
        part, chunk, to, dep, _, _ = msgs[name]
        n = number[name]
        back = to if arriving else (0, 0, 0)
        if part == "w":
            d = to[2]
            rows = pl.ds(pl.multiple_of(seq_of(x, z, y - d) * 16, 16), 16) if arriving else mine
            slot = lax.rem(y + d, NY)
            return [remote(a, b, send_sems.at[n if e == 0 else len(msgs) + 3 * n + e], recv_sems.at[n if e == 0 else len(msgs) + 3 * n + e], there(*to))
                    for e, (a, b) in enumerate(pieces(slot, rows))]
        if part in ("h0", "h1"):
            ref = ablk.at[block(chunk - back[2]), pl.ds(128 * int(part[1]), 128)]
        else:
            ref = (wa if part == "a" else wb).at[rows_of(chunk[0] - back[0], chunk[1] - back[1])]
        return [remote(ref, ref, send_sems.at[n], recv_sems.at[n], there(*to))]

    def start(name):
        for copy in copies(name, False):
            copy.start()

    def normed(rel, half):
        def step(n, _):
            at = pl.multiple_of(half * 128 + n * 64, 64)
            b = block(rel)
            h = ablk[b, pl.ds(at, 64), :].astype(F32)
            r = lax.rsqrt(jnp.mean(h * h, axis=1, keepdims=True) + EPS)
            u[pl.ds(pl.multiple_of(b * ROWS + at, 64), 64), :] = (h * r * gain[...]).astype(BF16)
            return 0

        lax.fori_loop(0, 2, step, 0)

    with jax.named_scope("gather"):
        for name, m in msgs.items():
            if m[3] is None:
                start(name)
        for copy in loads[2:-1]:
            copy.wait()
        loads[-1].start()
        normed(0, 0)
        normed(0, 1)
        def picked(v, hit):
            rows = jnp.broadcast_to(v[...], (8, v.shape[1]))
            return jnp.dot(rows, hit.astype(F32), precision=HI, preferred_element_type=F32)[:1]

        def two(rows, lanes):
            return (lax.broadcasted_iota(jnp.int32, (rows, lanes), 0), lax.broadcasted_iota(jnp.int32, (rows, lanes), 1))

        k, c = two(32, 128)
        of_head = (c >= 64) & (k == 8 * y + lax.shift_right_logical(c - 64, 3))
        k2, c2 = two(256, 128)
        bias = picked(dtb, of_head) + picked(lb, (c2 < 64) & (k2 == 64 * y + c2))
        rates = picked(rate, of_head)
        k3, c3 = two(32, 512)
        skips = picked(skip, k3 == 8 * y + lax.shift_right_logical(c3, 6))

        low_tri = (lax.broadcasted_iota(jnp.int32, (ROWS, ROWS), 1) <= lax.broadcasted_iota(jnp.int32, (ROWS, ROWS), 0)).astype(BF16)
        lane_in, col_in = two(256, 512)
        for lev in range(9):
            lane = lev + 8 * lax.shift_right_logical(col_in, 6) + (64 - 8 if lev == 8 else 0)
            ones[lev] = ((lane_in & 127) == lane).astype(BF16)

        def widened(v, lev):
            high = v.astype(BF16)
            low = (v - high.astype(F32)).astype(BF16)
            return jnp.concatenate([high, low], axis=1), lev

        def wide(pair, cols=slice(0, 512)):
            return jnp.dot(pair[0], ones[pair[1], :, cols], preferred_element_type=F32)

        halves = {("P", 0): (-1, 0), ("P", 1): (-1, 1), ("M", 1): (1, 1), ("M", 0): (1, 0), ("P", 2): (-2, 0), ("M", 2): (2, 1)}
        missing = {d: set() for d in range(NX)}
        for name, m in msgs.items():
            if m[0] in ("a", "b"):
                missing[(m[2][0] - m[1][0]) % NX].add(name)
        lacking = {-1: {("P", 0), ("P", 1)}, 1: {("M", 1), ("M", 0)}, -2: {("P", 2), ("M", 2)}}
        here, held, ready, counted = [0], [], [], {rel: 0 for rel in (0, -1, 1, -2)}

        def multiply(rel, d):
            counted[rel] += 1
            rows = pl.ds(pl.multiple_of(block(rel) * ROWS, ROWS), ROWS)
            deep = pl.ds(pl.multiple_of(lax.rem(x + NX - d, NX) * 512, 512), 512)
            for w, cols in ((wa, slice(0, CA)), (wb, slice(CA, NP))):
                r = jnp.dot(u[rows, deep], w[deep, :], preferred_element_type=F32)
                if counted[rel] > 1:
                    r = r + pacc[rows, cols]
                if counted[rel] == NX:
                    p[rows, cols] = r.astype(BF16)
                else:
                    pacc[rows, cols] = r

        for name in order:
            if name == "own":
                for copy in local:
                    copy.wait()
            else:
                for copy in copies(name, True):
                    copy.wait_recv()
            for other, m in msgs.items():
                if m[3] == name:
                    start(other)
            if name in halves:
                normed(*halves[name])
            for rel, left in list(lacking.items()):
                left.discard(name)
                if not left:
                    del lacking[rel]
                    here.append(rel)
                    ready += [(rel, d) for d in held]
            for d, left in list(missing.items()):
                left.discard(name)
                if not left:
                    del missing[d]
                    held.append(d)
                    ready += [(rel, d) for rel in here]
            if ready:
                multiply(*ready.pop(0))
        for pair in ready:
            multiply(*pair)

    with jax.named_scope("rows"):
        for b in range(4):
            rows = slice(b * ROWS, (b + 1) * ROWS)
            t = softplus(p[rows, MID:].astype(F32) + bias)
            td[rows, :] = t
            left = -t * rates
            total = jnp.zeros((ROWS, 128), F32)
            for _ in range(3):
                piece = left.astype(BF16)
                total = total + jnp.dot(low_tri, piece, preferred_element_type=F32)
                left = left - piece.astype(F32)
            cu[rows, :] = total
            eb[b : b + 1, :] = total[ROWS - 1 :, :]
        eb[4:, :] = jnp.zeros((4, 128), F32)
        ends = eb[...]
        ee[...] = jnp.exp(spread(ends, 512))
        slog[...] = jnp.broadcast_to(jnp.sum(ends, axis=0, keepdims=True), (8, 128))

    with jax.named_scope("conv"):
        back = remote(p.at[pl.ds(1008, 16), pl.ds(0, 768)], tail, tsem.at[0], tsem.at[1], group(wrap(g + 1)))
        back.start()

        for n in range(4):
            ext[8 + n * ROWS : 8 + (n + 1) * ROWS, :] = p[n * ROWS : (n + 1) * ROWS, :768].astype(F32)
        own = pl.ds(pl.multiple_of(y * 512, 512), 512)
        tx = [cw[k : k + 1, own] for k in range(4)]
        tb = [cw[k : k + 1, 2048:] for k in range(4)]
        bx, bb = cb[:, own], cb[:, 2048:]

        def convolved(n):
            at = n * 128
            v = bx
            for k in range(4):
                v = v + tx[k] * ext[at + 5 + k : at + 133 + k, :512]
            xf[at : at + 128, :] = jax.nn.silu(v)
            v = bb
            for k in range(4):
                v = v + tb[k] * ext[at + 5 + k : at + 133 + k, 512:]
            bcs[at : at + 128, :] = jax.nn.silu(v).astype(BF16)

        for n in range(1, 8):
            convolved(n)
        back.wait_recv()
        before = tail[...].astype(F32)
        ext[0:8, :] = jnp.where(g > 0, before[8:, :], 0.0)
        convolved(0)

    with jax.named_scope("states"):
        first = lax.broadcasted_iota(jnp.int32, (1, 128), 1) < 64

        def state(b):
            rows = slice(b * ROWS, (b + 1) * ROWS)
            tl = jnp.exp(ends[b : b + 1, :] - cu[rows, :]) * td[rows, :]
            xt = (xf[rows, :] * wide(widened(tl, 8))).astype(BF16)
            return lax.dot_general(bcs[rows, :128], xt, (((0,), (0,)), ((), ())), preferred_element_type=F32)

        st = state(0)
        near_st[0] = st.astype(BF16)
        st = ee[1:2, :] * st + state(1)
        near_st[1] = st.astype(BF16)
        other = state(2)
        near_st[2] = other.astype(BF16)
        st = ee[2:3, :] * ee[3:4, :] * st + ee[3:4, :] * other + state(3)
        st = st.astype(BF16)
        for n in range(GROUPS):
            ct, nt = n // 8, n % 8
            snd1[n] = st[16 * nt : 16 * nt + 16, 128 * ct : 128 * ct + 128]

        def first_send(d, _):
            to = wrap(g + d)
            remote(snd1.at[to], rcv1.at[g], ssem.at[0], rsem.at[0], group(to)).start()
            remote(slog, rlog.at[g], ssem.at[1], rsem.at[1], group(to)).start()
            return 0

        lax.fori_loop(1, GROUPS, first_send, 0)
        rcv1[g] = snd1[g]
        rlog[g] = slog[...]

    with jax.named_scope("inside"):
        def inside(b, _):
            base = pl.multiple_of(b * ROWS, ROWS)
            every = pl.ds(base, ROWS)
            cum_t = jnp.transpose(cu[every, :])
            dt_t = jnp.transpose(td[every, :])
            for r in range(2):
                rows = pl.ds(pl.multiple_of(base + 128 * r, 128), 128)
                reach = 128 * (r + 1)
                seen = pl.ds(base, reach)
                scores = lax.dot_general(bcs[rows, 128:], bcs[seen, :128], (((1,), (1,)), ((), ())), preferred_element_type=F32)
                ti, si = two(128, reach)
                causal = si <= ti + 128 * r
                cum, lam = cu[rows, :], wide(widened(td[rows, :], 0))
                for h in range(4):
                    xp = xf[seen, 128 * h : 128 * h + 128].astype(BF16)
                    got = []
                    for e in (2 * h, 2 * h + 1):
                        lane = 64 + 8 * e
                        differ = jnp.where(causal, cum[:, lane : lane + 1] - cum_t[lane : lane + 1, :reach], -1e30)
                        w = scores * jnp.exp(differ) * dt_t[lane : lane + 1, :reach]
                        got.append(jnp.dot(w.astype(BF16), xp, preferred_element_type=F32))
                    cols = slice(128 * h, 128 * h + 128)
                    val = jnp.where(first, got[0], got[1]) * lam[:, cols]
                    yacc[rows, cols] = val + skips[:, cols] * xf[rows, cols]
            return 0

        lax.fori_loop(0, 4, inside, 0)

    with jax.named_scope("wait1"):
        remote(rcv1.at[pl.ds(0, GROUPS - 1)], rcv1.at[pl.ds(0, GROUPS - 1)], ssem.at[0], rsem.at[0], group(g)).wait_recv()
        remote(rlog.at[pl.ds(0, GROUPS - 1)], rlog.at[pl.ds(0, GROUPS - 1)], ssem.at[1], rsem.at[1], group(g)).wait_recv()
    with jax.named_scope("merge"):
        logs = rlog[:, 0, :]
        wide_logs = spread(logs, 512)
        ct = lax.div(g, 8)
        head_logs = jnp.zeros((GROUPS, 128), F32)
        for n in range(4):
            head_logs = jnp.where(ct == n, wide_logs[:, 128 * n : 128 * n + 128], head_logs)
        level = [rcv1[n].astype(F32) for n in range(GROUPS)]
        ends_of = [head_logs[n : n + 1, :] for n in range(GROUPS)]
        for l in range(LEVELS_OUT):
            for n in range(0, len(level), 2):
                table[TABLE[l] + n // 2] = level[n].astype(BF16)
            level = [jnp.exp(ends_of[n + 1]) * level[n] + level[n + 1] for n in range(0, len(level), 2)]
            ends_of = [ends_of[n] + ends_of[n + 1] for n in range(0, len(ends_of), 2)]

        def second_send(d, _):
            to = wrap(g + d)
            for l in range(LEVELS_OUT):
                up = lax.div(to, 2**l)

                @pl.when(lax.rem(up, 2) == 1)
                def _():
                    remote(table.at[TABLE[l] + lax.div(up, 2)], rcv2.at[l, g], lsend.at[l], lrecv.at[l], group(to)).start()

            return 0

        lax.fori_loop(1, GROUPS, second_send, 0)
    with jax.named_scope("near"):
        bits = [lax.rem(lax.div(g, 2**l), 2) for l in range(LEVELS_OUT)]

        lane8 = lax.broadcasted_iota(jnp.int32, (1, 128), 1) & 7

        def read(b, rows, bucket, scale, lev):
            r = jnp.dot(bcs[rows, 128:], bucket, preferred_element_type=F32)
            yacc[rows, :] += r * wide(widened(scale, lev))

        def scales(rows, add):
            return pltpu.roll(jnp.exp(cu[rows, :] + add), 64, 1) * td[rows, :]

        zero = jnp.zeros((1, 128), F32)
        at_block = [pl.ds(b * ROWS, ROWS) for b in range(4)]
        read(1, at_block[1], near_st[0], scales(at_block[1], zero), 1)
        read(2, at_block[2], near_st[1], scales(at_block[2], zero), 2)
        sc = scales(at_block[3], jnp.where(lane8 == 2, ends[2:3, :], 0.0))
        read(3, at_block[3], near_st[2], sc, 1)
        read(3, at_block[3], near_st[1], sc, 2)

        row_of = lax.broadcasted_iota(jnp.int32, (GROUPS, 1), 0)
        outer = zero
        for l in range(LEVELS_OUT):
            start = lax.div(g, 2**l) * 2**l
            summed = jnp.sum(jnp.where((row_of >= start) & (row_of < g), logs, 0.0), axis=0, keepdims=True)
            outer = jnp.where(lane8 == l + 3, summed, outer)
        run = zero
        for b in range(4):
            eb[4 + b : 5 + b, :] = run + outer
            run = run + ends[b : b + 1, :]

    with jax.named_scope("wait2"):
        for l in range(LEVELS_OUT):
            @pl.when(bits[l] == 1)
            def _():
                remote(rcv2.at[l, pl.ds(0, GROUPS - 1)], rcv2.at[l, pl.ds(0, GROUPS - 1)], lsend.at[l], lrecv.at[l], group(g)).wait_recv()
                rcv2[l, g] = table[TABLE[l] + lax.div(g, 2 ** (l + 1))]

            @pl.when(bits[l] == 0)
            def _():
                rcv2[l] = jnp.zeros((GROUPS, 16, 128), BF16)

    with jax.named_scope("finish"):
        def finish(n, _):
            b = lax.rem(y + n, NY)
            base = pl.multiple_of(b * ROWS, ROWS)
            for half in range(2):
                rows = pl.ds(pl.multiple_of(base + 128 * half, 128), 128)
                scale = scales(rows, eb[pl.ds(4 + b, 1), :])
                c = bcs[rows, 128:]
                pair_of = widened(scale, 0)[0]
                for h in range(0, 4, 2):
                    cols = slice(128 * h, 128 * h + 256)
                    vals = yacc[rows, cols]
                    for l in range(LEVELS_OUT):
                        pair = [rcv2[l, 8 * (h + e) : 8 * (h + e) + 8].reshape(128, 128) for e in range(2)]
                        r = jnp.dot(c, jnp.concatenate(pair, axis=1), preferred_element_type=F32)
                        vals = vals + r * wide((pair_of, l + 3), cols)
                    zg = p[rows, 768 + 128 * h : 1024 + 128 * h].astype(F32)
                    qs[b, 128 * half : 128 * half + 128, cols] = (vals * jax.nn.silu(zg)).astype(BF16)

            @pl.when(n < 4)
            def _():
                remote(qs.at[b], qr.at[y], qsend.at[n], qrecv.at[n], beside(n)).start()

            return 0

        lax.fori_loop(1, 5, finish, 0)
    with jax.named_scope("out"):
        qr[y] = qs[y]
        loads[-1].wait()

        squares = jnp.zeros((ROWS, 1), F32)
        for at, n in enumerate((0, 1, 3, 2)):
            src = lax.rem(y + NY - n, NY)
            if n:
                remote(qs.at[0], qr.at[src], qsend.at[n], qrecv.at[n], beside(n)).wait_recv()
            v = qr[src].astype(F32)
            squares = squares + jnp.sum(v * v, axis=1, keepdims=True)
            lanes = pl.ds(pl.multiple_of(src * 512, 512), 512)
            v = (v * gg[:, lanes]).astype(BF16)
            for t in range(4):
                cols = slice(512 * t, 512 * t + 512)
                part = jnp.dot(v, wout[lanes, cols], preferred_element_type=F32)
                acc[:, cols] = part if at == 0 else acc[:, cols] + part
    with jax.named_scope("swap"):
        r = lax.rsqrt(squares * (1.0 / 2048.0) + EPS)
        sends = []
        for t in range(4):
            cols = slice(512 * t, 512 * t + 512)
            os[t] = (ablk[y, :, cols].astype(F32) + r * acc[:, cols]).astype(BF16)
            sends.append(remote(os.at[t], out.at[:, pl.ds(512 * t, 512)], osend.at[t], orecv.at[t], {"section": 1 - s}))
            sends[-1].start()
        for copy in sends:
            copy.wait_recv()
    with jax.named_scope("drain"):
        for name in msgs:
            for copy in copies(name, False):
                copy.wait_send()
        back.wait_send()
        remote(rcv1.at[pl.ds(0, GROUPS - 1)], rcv1.at[pl.ds(0, GROUPS - 1)], ssem.at[0], rsem.at[0], group(g)).wait_send()
        remote(rlog.at[pl.ds(0, GROUPS - 1)], rlog.at[pl.ds(0, GROUPS - 1)], ssem.at[1], rsem.at[1], group(g)).wait_send()
        for l in range(LEVELS_OUT):
            for bit in range(2):
                @pl.when(bits[l] == bit)
                def _():
                    some = rcv2.at[l, pl.ds(0, 16 - bit)]
                    remote(some, some, lsend.at[l], lrecv.at[l], group(g)).wait_send()
        for n in (1, 2, 3):
            remote(qs.at[0], qr.at[y], qsend.at[n], qrecv.at[n], beside(n)).wait_send()
        for copy in sends:
            copy.wait_send()


def layer(acts, proj, wout, *params):
    anywhere = pl.BlockSpec(memory_space=pl.ANY)
    n = NY * ROWS
    count = 4 * len(plan())
    dma = pltpu.SemaphoreType.DMA
    return pl.pallas_call(
        layer_kernel,
        out_shape=jax.ShapeDtypeStruct((ROWS, 2048), BF16),
        in_specs=[anywhere] * (3 + len(params)),
        out_specs=anywhere,
        scratch_shapes=[
            pltpu.VMEM((2048, CA), BF16),
            pltpu.VMEM((2048, CB), BF16),
            pltpu.VMEM((NY, ROWS, 2048), BF16),
            pltpu.VMEM((n, 2048), BF16),
            pltpu.VMEM((n, NP), F32),
            pltpu.VMEM((n, NP), BF16),
            pltpu.VMEM(proj.shape, BF16),
            pltpu.VMEM((NY, 16, 128), BF16),
            pltpu.VMEM((9, 256, 512), BF16),
            *[pltpu.VMEM(a.shape, a.dtype) for a in params],
            pltpu.VMEM((n + 8, 768), F32),
            pltpu.VMEM((n, 512), F32),
            pltpu.VMEM((n, 256), BF16),
            pltpu.VMEM((n, 128), F32),
            pltpu.VMEM((n, 128), F32),
            pltpu.VMEM((n, 512), F32),
            pltpu.VMEM((3, 128, 512), BF16),
            pltpu.VMEM((8, 128), F32),
            pltpu.VMEM((8, 512), F32),
            pltpu.VMEM((GROUPS, 16, 128), BF16),
            pltpu.VMEM((8, 128), F32),
            pltpu.VMEM((GROUPS, 16, 128), BF16),
            pltpu.VMEM((GROUPS, 8, 128), F32),
            pltpu.VMEM((31, 16, 128), BF16),
            pltpu.VMEM((LEVELS_OUT, GROUPS, 16, 128), BF16),
            pltpu.VMEM((16, 768), BF16),
            pltpu.VMEM((NY, ROWS, 512), BF16),
            pltpu.VMEM((NY, ROWS, 512), BF16),
            pltpu.VMEM((2048, 2048), BF16),
            pltpu.VMEM((ROWS, 2048), F32),
            pltpu.VMEM((4, ROWS, 512), BF16),
            dma((4,)), dma((count,)), dma((count,)), dma((11,)),
            dma((2,)), dma((2,)), dma((5,)), dma((5,)), dma((2,)), dma((4,)), dma((4,)), dma((4,)), dma((4,)),
        ],
        compiler_params=pltpu.CompilerParams(
            collective_id=0, has_side_effects=True, vmem_limit_bytes=56 * 1024 * 1024),
        name="layer",
    )(acts, proj, wout, *params)


def per_device(acts, in_proj, out_proj, conv_weight, conv_bias, dt_bias, decay_rate, skip_gain, level_bias, norm_gain, gate_gain):
    o = layer(acts[0], in_proj[0], out_proj[0], norm_gain, conv_weight[0], conv_bias, dt_bias, decay_rate, skip_gain, level_bias, gate_gain)
    return o[None]


def solution(mesh):
    two = P("section", None)
    three = P("section", None, None)
    return jax.shard_map(
        per_device,
        mesh=mesh,
        in_specs=(P("section", "seq", None), P("section", "seq", None), three, three, two, two, two, two, two, two, two),
        out_specs=P("section", "seq", None),
        check_vma=False,
    )
```

```python
import functools
import jax
import jax.numpy as jnp
from jax import lax
from jax.experimental import pallas as pl
from jax.experimental.pallas import tpu as pltpu
from jax.sharding import PartitionSpec as P

EPS = 1e-05
MESH = pl.DeviceIdType.MESH
NX, NZ, NY = 4, 8, 4
GROUPS = NX * NZ
CA, CB = 512, 896
NP = CA + CB
ROWS = 256
F32, BF16 = jnp.float32, jnp.bfloat16


def seq_of(x, z, y):
    return (lax.rem(x + 4 * NX, NX) * NZ + lax.rem(z + 4 * NZ, NZ)) * NY + lax.rem(y + 4 * NY, NY)


def plan():
    msgs = {}
    ua, ub, un = 64 * CA * 2, 64 * CB * 2, 128 * 2048 * 2
    for d, links in ((1, {"y+": 1}), (3, {"y-": 1}), (2, {"y+": 1, "y-": 1})):
        msgs[("w", d)] = ("w", None, (0, 0, d), None, 16 * NP * 2, links)
    msgs[("P", 0)] = ("h0", 0, (0, 0, 1), None, un, {"y+": 1})
    msgs[("M", 1)] = ("h1", 0, (0, 0, -1), None, un, {"y-": 1})
    msgs[("P", 1)] = ("h1", 0, (0, 0, 1), None, un, {"y+": 1})
    msgs[("M", 0)] = ("h0", 0, (0, 0, -1), None, un, {"y-": 1})
    msgs[("P", 2)] = ("h0", -1, (0, 0, 1), ("P", 0), un, {"y+": 1})
    msgs[("M", 2)] = ("h1", 1, (0, 0, -1), ("M", 1), un, {"y-": 1})
    own = "own"
    for d, links in ((1, {"x+": 1}), (3, {"x-": 1}), (2, {"x+": 2})):
        msgs[("A1", d)] = ("a", (0, 0), (d, 0, 0), own, ua, links)
    for k in range(1, 5):
        if k < 5:
            dep = own if k == 1 else ("B1+", k - 1)
            msgs[("B1+", k)] = ("b", (0, -(k - 1)), (0, 1, 0), dep, ub, {"z+": 1})
        if k < 4:
            dep = own if k == 1 else ("B1-", k - 1)
            msgs[("B1-", k)] = ("b", (0, k - 1), (0, -1, 0), dep, ub, {"z-": 1})
    for k in range(1, 5):
        for d in range(4):
            up, down = (4, 3) if d < 2 else (3, 4)
            if k <= up:
                dep = (own if d == 0 else ("A1", d)) if k == 1 else ("A2+", d, k - 1)
                msgs[("A2+", d, k)] = ("a", (-d, -(k - 1)), (0, 1, 0), dep, ua, {"z+": 1})
            if k <= down:
                dep = (own if d == 0 else ("A1", d)) if k == 1 else ("A2-", d, k - 1)
                msgs[("A2-", d, k)] = ("a", (-d, k - 1), (0, -1, 0), dep, ua, {"z-": 1})
    offs = [0, -1, 1, -2, 2, -3, 3, -4]
    for o in offs:
        dep = own if o == 0 else (("B1+", -o) if o < 0 else ("B1-", o))
        msgs[("B2+", o)] = ("b", (0, o), (1, 0, 0), dep, ub, {"x+": 1})
        msgs[("B2-", o)] = ("b", (0, o), (-1, 0, 0), dep, ub, {"x-": 1})
        if o in (0, -1, 3, -4):
            msgs[("B2+2", o)] = ("b", (-1, o), (1, 0, 0), ("B2+", o), ub, {"x+": 1})
        else:
            msgs[("B2-2", o)] = ("b", (1, o), (-1, 0, 0), ("B2-", o), ub, {"x-": 1})
    return msgs


BOOST = {(way, d): b for way in ("A2+", "A2-") for d, b in enumerate((0.0, 0.0, -6.0, 0.0))}


def schedule(msgs, rate=46.6e3, latency=2.2, early=1.5, window=4.0):
    kids = {}
    for name, m in msgs.items():
        kids.setdefault(m[3], []).append(name)

    def path(name):
        _, _, _, _, size, links = msgs[name]
        step = size * max(links.values()) / rate + latency
        return step + max([path(k) for k in kids.get(name, [])], default=0.0)

    def boost(name):
        return 100.0 if msgs[name][0] == "w" else BOOST.get(name[:2], 0.0) if name[0][:2] == "A2" else 0.0

    rank = {name: -path(name) - boost(name) for name in msgs}
    free, arrive, events, waiting, plan_of, got = {}, {}, [], [], [], set()

    def issue(now):
        sent = []
        for name in sorted(waiting, key=lambda n: (rank[n], str(n))):
            part, _, _, _, size, links = msgs[name]
            if part != "w" and any(free.get(l, 0.0) > now + window for l in links):
                continue
            begin = max([now] + [free.get(l, 0.0) for l in links])
            for l, n in links.items():
                free[l] = begin + size * n / rate
            arrive[name] = max(free[l] for l in links) + latency + (early if part == "w" else 0.0)
            events.append((arrive[name], len(arrive), name))
            sent.append(name)
        for name in sent:
            waiting.remove(name)
        return sent

    waiting += kids[None]
    first = issue(0.0)
    while events:
        events.sort()
        now, _, name = events.pop(0)
        waiting += kids.get(name, [])
        got.add(name)
        plan_of.append((name, issue(now)))
        if "own" not in got and all(("w", d) in got for d in (1, 2, 3)):
            got.add("own")
            waiting += kids["own"]
            plan_of.append(("own", issue(now)))
    assert not waiting
    return first, plan_of, arrive


HI = lax.Precision.HIGHEST
MID = CA + 768
LEVELS_OUT = 5
TABLE = (0, 16, 24, 28, 30)


def spread(row, lanes):
    k = lax.broadcasted_iota(jnp.int32, (128, lanes), 0)
    c = lax.broadcasted_iota(jnp.int32, (128, lanes), 1)
    return jnp.dot(row, (k == 64 + 8 * lax.shift_right_logical(c, 6)).astype(F32), precision=HI, preferred_element_type=F32)


def halves_of(a, lane_low, lane_high, first):
    return jnp.where(first, a[:, lane_low : lane_low + 1], a[:, lane_high : lane_high + 1])


def softplus(v):
    return jnp.maximum(v, 0.0) + jnp.log1p(jnp.exp(-jnp.abs(v)))


def layer_kernel(acts_in, proj_in, wout_in, gain_in, cw_in, cb_in, dtb_in, rate_in, skip_in, lb_in, gg_in, out_low, out_high,
                 wa, wb, ablk, u, pacc, p, proj, small, ones,
                 gain, cw, cb, dtb, rate, skip, lb, gg,
                 ext, xf, bcs, td, cu, yacc, near_st, eb, ee, snd1, slog, rcv1, rlog, table, rcv2, tail,
                 qs, qr, relay, wout, acc, os,
                 local_sems, send_sems, recv_sems, in_sems,
                 ssem, rsem, lsend, lrecv, tsem, qsend, qrecv, osend, orecv):
    i = lax.axis_index("seq")
    y = lax.rem(i, NY)
    g = lax.div(i, NY)
    z = lax.rem(g, NZ)
    x = lax.div(g, NZ)
    s = lax.axis_index("section")

    def there(dx, dz, dy):
        return {"seq": seq_of(x + dx, z + dz, y + dy)}

    def group(n):
        return {"seq": n * NY + y}

    def beside(n):
        return {"seq": g * NY + lax.rem(y + n, NY)}

    def wrap(n):
        return lax.rem(n, GROUPS)

    def remote(src, dst, send, recv, to):
        return pltpu.make_async_remote_copy(
            src_ref=src, dst_ref=dst, send_sem=send, recv_sem=recv, device_id=to, device_id_type=MESH)

    with jax.named_scope("enter"):
        barrier = pltpu.get_barrier_semaphore()

        def greet(d, _):
            pl.semaphore_signal(barrier, inc=1, device_id=group(wrap(g + d)), device_id_type=MESH)
            return 0

        lax.fori_loop(1, GROUPS, greet, 0)
        for d in (1, 2, 3):
            pl.semaphore_signal(barrier, inc=1, device_id=beside(d), device_id_type=MESH)
        pl.semaphore_signal(barrier, inc=1, device_id={"section": 1 - s}, device_id_type=MESH)
        pairs = ((proj_in, proj), (acts_in, ablk.at[y]), (gain_in, gain), (cw_in, cw), (cb_in, cb), (dtb_in, dtb),
                 (rate_in, rate), (skip_in, skip), (lb_in, lb), (gg_in, gg), (wout_in, wout))
        loads = [pltpu.make_async_copy(a, b, in_sems.at[n]) for n, (a, b) in enumerate(pairs)]
        for copy in loads[:-1]:
            copy.start()

        loads[0].wait()
        rows_k = lax.broadcasted_iota(jnp.int32, (288, 128), 0)
        lane_k = lax.broadcasted_iota(jnp.int32, (288, 128), 1)
        packed = proj[:, 4352:]
        for n in range(NY):
            from_lr = (lane_k < 64) & (rows_k == 32 + 64 * n + lane_k)
            from_dr = (lane_k >= 64) & (rows_k == 8 * n + lax.shift_right_logical(lane_k - 64, 3))
            hit = (from_lr | from_dr).astype(BF16)
            small[n] = jnp.dot(packed, hit, preferred_element_type=F32).astype(BF16)

        msgs = plan()
        number = {name: n for n, name in enumerate(msgs)}
        first_sends, steps, _ = schedule(msgs)

        def block(rel):
            return lax.rem(y + rel + 2 * NY, NY)

        def rows_of(cx, cz):
            return pl.ds(pl.multiple_of(seq_of(x + cx, z + cz, 0) * 16, 64), 64)

        def pieces(slot, rows):
            cols = pl.multiple_of(slot * 512, 512)
            return [(proj.at[:, pl.ds(cols, 512)], wa.at[rows]),
                    (proj.at[:, pl.ds(2048, 256)], wb.at[rows, pl.ds(0, 256)]),
                    (proj.at[:, pl.ds(pl.multiple_of(2304 + cols, 256), 512)], wb.at[rows, pl.ds(256, 512)]),
                    (small.at[slot], wb.at[rows, pl.ds(768, 128)])]

        mine = pl.ds(pl.multiple_of(i * 16, 16), 16)
        local = [pltpu.make_async_copy(a, b, local_sems.at[n]) for n, (a, b) in enumerate(pieces(y, mine))]
        for copy in local:
            copy.start()
        loads[1].wait()
        pl.semaphore_wait(barrier, GROUPS - 1 + 3 + 1)

    def copies(name, arriving):
        part, chunk, to, dep, _, _ = msgs[name]
        n = number[name]
        back = to if arriving else (0, 0, 0)
        if part == "w":
            d = to[2]
            rows = pl.ds(pl.multiple_of(seq_of(x, z, y - d) * 16, 16), 16) if arriving else mine
            slot = lax.rem(y + d, NY)
            return [remote(a, b, send_sems.at[n if e == 0 else len(msgs) + 4 * n + e], recv_sems.at[n if e == 0 else len(msgs) + 4 * n + e], there(*to))
                    for e, (a, b) in enumerate(pieces(slot, rows))]
        if part in ("h0", "h1"):
            ref = ablk.at[block(chunk - back[2]), pl.ds(128 * int(part[1]), 128)]
        else:
            ref = (wa if part == "a" else wb).at[rows_of(chunk[0] - back[0], chunk[1] - back[1])]
        return [remote(ref, ref, send_sems.at[n], recv_sems.at[n], there(*to))]

    def start(name):
        for copy in copies(name, False):
            copy.start()

    def normed(rel, half):
        def step(n, _):
            at = pl.multiple_of(half * 128 + n * 64, 64)
            b = block(rel)
            h = ablk[b, pl.ds(at, 64), :].astype(F32)
            r = lax.rsqrt(jnp.mean(h * h, axis=1, keepdims=True) + EPS)
            u[pl.ds(pl.multiple_of(b * ROWS + at, 64), 64), :] = (h * r * gain[...]).astype(BF16)
            return 0

        lax.fori_loop(0, 2, step, 0)

    with jax.named_scope("gather"):
        for name in first_sends:
            start(name)
        for copy in loads[2:-1]:
            copy.wait()
        loads[-1].start()
        normed(0, 0)
        normed(0, 1)
        def picked(v, hit):
            rows = jnp.broadcast_to(v[...], (8, v.shape[1]))
            return jnp.dot(rows, hit.astype(F32), precision=HI, preferred_element_type=F32)[:1]

        def two(rows, lanes):
            return (lax.broadcasted_iota(jnp.int32, (rows, lanes), 0), lax.broadcasted_iota(jnp.int32, (rows, lanes), 1))

        k, c = two(32, 128)
        of_head = (c >= 64) & (k == 8 * y + lax.shift_right_logical(c - 64, 3))
        k2, c2 = two(256, 128)
        bias = picked(dtb, of_head) + picked(lb, (c2 < 64) & (k2 == 64 * y + c2))
        rates = picked(rate, of_head)
        k3, c3 = two(32, 512)
        skips = picked(skip, k3 == 8 * y + lax.shift_right_logical(c3, 6))

        low_tri = (lax.broadcasted_iota(jnp.int32, (ROWS, ROWS), 1) <= lax.broadcasted_iota(jnp.int32, (ROWS, ROWS), 0)).astype(BF16)
        lane_in, col_in = two(256, 512)
        for lev in range(9):
            lane = lev + 8 * lax.shift_right_logical(col_in, 6) + (64 - 8 if lev == 8 else 0)
            ones[lev] = ((lane_in & 127) == lane).astype(BF16)

        def widened(v, lev):
            high = v.astype(BF16)
            low = (v - high.astype(F32)).astype(BF16)
            return jnp.concatenate([high, low], axis=1), lev

        def wide(pair, cols=slice(0, 512)):
            return jnp.dot(pair[0], ones[pair[1], :, cols], preferred_element_type=F32)

        halves = {("P", 0): (-1, 0), ("P", 1): (-1, 1), ("M", 1): (1, 1), ("M", 0): (1, 0), ("P", 2): (-2, 0), ("M", 2): (2, 1)}
        missing = {(part, d): set() for d in range(NX) for part in "ab"}
        for name, m in msgs.items():
            if m[0] in ("a", "b"):
                missing[(m[0], (m[2][0] - m[1][0]) % NX)].add(name)
        lacking = {-1: {("P", 0), ("P", 1)}, 1: {("M", 1), ("M", 0)}, -2: {("P", 2), ("M", 2)}}
        here, held, ready, counted = [0], [], [], {}

        def multiply():
            which = ready[0][1]
            rels = [rel for rel, other in ready if other == which]
            ready[:] = [e for e in ready if e[1] != which]
            part, d = which
            rows = [pl.ds(pl.multiple_of(block(rel) * ROWS, ROWS), ROWS) for rel in rels]
            deep = pl.ds(pl.multiple_of(lax.rem(x + NX - d, NX) * 512, 512), 512)
            w, cols = (wa, slice(0, CA)) if part == "a" else (wb, slice(CA, NP))
            left = jnp.concatenate([u[r, deep] for r in rows], axis=0)
            full = jnp.dot(left, w[deep, :], preferred_element_type=F32)
            for e, (rel, at) in enumerate(zip(rels, rows)):
                done = counted[rel, part] = counted.get((rel, part), 0) + 1
                r = full[e * ROWS : (e + 1) * ROWS]
                if done > 1:
                    r = r + pacc[at, cols]
                if done == NX:
                    p[at, cols] = r.astype(BF16)
                else:
                    pacc[at, cols] = r

        for name, then in steps:
            if name == "own":
                for copy in local:
                    copy.wait()
            else:
                for copy in copies(name, True):
                    copy.wait_recv()
            for other in then:
                start(other)
            if name in halves:
                normed(*halves[name])
            for rel, left in list(lacking.items()):
                left.discard(name)
                if not left:
                    del lacking[rel]
                    here.append(rel)
                    ready += [(rel, d) for d in held]
            for d, left in list(missing.items()):
                left.discard(name)
                if not left:
                    del missing[d]
                    held.append(d)
                    ready += [(rel, d) for rel in here]
            if ready:
                multiply()
        while ready:
            multiply()

    with jax.named_scope("rows"):
        for b in range(4):
            rows = slice(b * ROWS, (b + 1) * ROWS)
            t = softplus(p[rows, MID:].astype(F32) + bias)
            td[rows, :] = t
            left = -t * rates
            total = jnp.zeros((ROWS, 128), F32)
            for _ in range(3):
                piece = left.astype(BF16)
                total = total + jnp.dot(low_tri, piece, preferred_element_type=F32)
                left = left - piece.astype(F32)
            cu[rows, :] = total
            eb[b : b + 1, :] = total[ROWS - 1 :, :]
        eb[4:, :] = jnp.zeros((4, 128), F32)
        ends = eb[...]
        ee[...] = jnp.exp(spread(ends, 512))
        slog[...] = jnp.sum(ends, axis=0, keepdims=True)

    with jax.named_scope("conv"):
        back = remote(p.at[pl.ds(1008, 16), pl.ds(0, 768)], tail, tsem.at[0], tsem.at[1], group(wrap(g + 1)))
        back.start()

        for n in range(4):
            ext[8 + n * ROWS : 8 + (n + 1) * ROWS, :] = p[n * ROWS : (n + 1) * ROWS, :768].astype(F32)
        own = pl.ds(pl.multiple_of(y * 512, 512), 512)
        tx = [cw[k : k + 1, own] for k in range(4)]
        tb = [cw[k : k + 1, 2048:] for k in range(4)]
        bx, bb = cb[:, own], cb[:, 2048:]

        def convolved(n):
            at = n * 128
            v = bx
            for k in range(4):
                v = v + tx[k] * ext[at + 5 + k : at + 133 + k, :512]
            xf[at : at + 128, :] = jax.nn.silu(v)
            v = bb
            for k in range(4):
                v = v + tb[k] * ext[at + 5 + k : at + 133 + k, 512:]
            bcs[at : at + 128, :] = jax.nn.silu(v).astype(BF16)

        for n in range(1, 8):
            convolved(n)
        back.wait_recv()
        before = tail[...].astype(F32)
        ext[0:8, :] = jnp.where(g > 0, before[8:, :], 0.0)
        convolved(0)

    with jax.named_scope("states"):
        first = lax.broadcasted_iota(jnp.int32, (1, 128), 1) < 64

        def state(b):
            rows = slice(b * ROWS, (b + 1) * ROWS)
            tl = jnp.exp(ends[b : b + 1, :] - cu[rows, :]) * td[rows, :]
            xt = (xf[rows, :] * wide(widened(tl, 8))).astype(BF16)
            return lax.dot_general(bcs[rows, :128], xt, (((0,), (0,)), ((), ())), preferred_element_type=F32)

        st = state(0)
        near_st[0] = st.astype(BF16)
        st = ee[1:2, :] * st + state(1)
        near_st[1] = st.astype(BF16)
        other = state(2)
        near_st[2] = other.astype(BF16)
        st = ee[2:3, :] * ee[3:4, :] * st + ee[3:4, :] * other + state(3)
        st = st.astype(BF16)
        for n in range(GROUPS):
            ct, nt = n // 8, n % 8
            snd1[n] = st[16 * nt : 16 * nt + 16, 128 * ct : 128 * ct + 128]

        def first_send(d, _):
            to = wrap(g + d)
            remote(snd1.at[to], rcv1.at[g], ssem.at[0], rsem.at[0], group(to)).start()
            remote(slog, rlog.at[g], ssem.at[1], rsem.at[1], group(to)).start()
            return 0

        lax.fori_loop(1, GROUPS, first_send, 0)
        rcv1[g] = snd1[g]
        rlog[g] = slog[...]

    with jax.named_scope("inside"):
        def inside(b, _):
            base = pl.multiple_of(b * ROWS, ROWS)
            every = pl.ds(base, ROWS)
            cum_t = jnp.transpose(cu[every, :])
            dt_t = jnp.transpose(td[every, :])
            for r in range(2):
                rows = pl.ds(pl.multiple_of(base + 128 * r, 128), 128)
                reach = 128 * (r + 1)
                seen = pl.ds(base, reach)
                scores = lax.dot_general(bcs[rows, 128:], bcs[seen, :128], (((1,), (1,)), ((), ())), preferred_element_type=F32)
                ti, si = two(128, reach)
                causal = si <= ti + 128 * r
                cum, lam = cu[rows, :], wide(widened(td[rows, :], 0))
                for h in range(4):
                    xp = xf[seen, 128 * h : 128 * h + 128].astype(BF16)
                    got = []
                    for e in (2 * h, 2 * h + 1):
                        lane = 64 + 8 * e
                        differ = jnp.where(causal, cum[:, lane : lane + 1] - cum_t[lane : lane + 1, :reach], -1e30)
                        w = scores * jnp.exp(differ) * dt_t[lane : lane + 1, :reach]
                        got.append(jnp.dot(w.astype(BF16), xp, preferred_element_type=F32))
                    cols = slice(128 * h, 128 * h + 128)
                    val = jnp.where(first, got[0], got[1]) * lam[:, cols]
                    yacc[rows, cols] = val + skips[:, cols] * xf[rows, cols]
            return 0

        lax.fori_loop(0, 4, inside, 0)

    with jax.named_scope("near"):
        lane8 = lax.broadcasted_iota(jnp.int32, (1, 128), 1) & 7

        def read(b, rows, bucket, scale, lev):
            r = jnp.dot(bcs[rows, 128:], bucket, preferred_element_type=F32)
            yacc[rows, :] += r * wide(widened(scale, lev))

        def scales(rows, add):
            return pltpu.roll(jnp.exp(cu[rows, :] + add), 64, 1) * td[rows, :]

        zero = jnp.zeros((1, 128), F32)
        at_block = [pl.ds(b * ROWS, ROWS) for b in range(4)]
        read(1, at_block[1], near_st[0], scales(at_block[1], zero), 1)
        read(2, at_block[2], near_st[1], scales(at_block[2], zero), 2)
        sc = scales(at_block[3], jnp.where(lane8 == 2, ends[2:3, :], 0.0))
        read(3, at_block[3], near_st[2], sc, 1)
        read(3, at_block[3], near_st[1], sc, 2)

        def gates(n, _):
            rows = pl.ds(pl.multiple_of(n * 128, 128), 128)
            v = p[rows, 768:1280].astype(F32)
            xf[rows, :] = jax.nn.silu(v)
            return 0

        lax.fori_loop(0, 8, gates, 0)

    with jax.named_scope("wait1"):
        remote(rcv1.at[pl.ds(0, GROUPS - 1)], rcv1.at[pl.ds(0, GROUPS - 1)], ssem.at[0], rsem.at[0], group(g)).wait_recv()
        remote(rlog.at[pl.ds(0, GROUPS - 1)], rlog.at[pl.ds(0, GROUPS - 1)], ssem.at[1], rsem.at[1], group(g)).wait_recv()
    with jax.named_scope("merge"):
        logs = rlog[:, 0, :]
        wide_logs = spread(logs, 512)
        ct = lax.div(g, 8)
        head_logs = jnp.zeros((GROUPS, 128), F32)
        for n in range(4):
            head_logs = jnp.where(ct == n, wide_logs[:, 128 * n : 128 * n + 128], head_logs)
        bits = [lax.rem(lax.div(g, 2**l), 2) for l in range(LEVELS_OUT)]

        def give(l):
            own = lax.div(g, 2 ** (l + 1)) * 2**l + lax.rem(g, 2**l)

            def to_one(k, _):
                at = lax.rem(own + k, 16)
                half = lax.div(at, 2**l)
                to = (2 * half + 1) * 2**l + lax.rem(at, 2**l)
                src = rcv1.at[2 * half] if l == 0 else table.at[TABLE[l] + half]
                remote(src, rcv2.at[l, g], lsend.at[l], lrecv.at[l], group(to)).start()
                return 0

            lax.fori_loop(1, 16, to_one, 0)

            @pl.when(bits[l] == 0)
            def _():
                to_one(0, 0)

        give(0)
        level = [rcv1[n].astype(F32) for n in range(GROUPS)]
        ends_of = [head_logs[n : n + 1, :] for n in range(GROUPS)]
        for l in range(1, LEVELS_OUT):
            level = [jnp.exp(ends_of[n + 1]) * level[n] + level[n + 1] for n in range(0, len(level), 2)]
            ends_of = [ends_of[n] + ends_of[n + 1] for n in range(0, len(ends_of), 2)]
            for n in range(0, len(level), 2):
                table[TABLE[l] + n // 2] = level[n].astype(BF16)
            give(l)

    with jax.named_scope("outer"):
        row_of = lax.broadcasted_iota(jnp.int32, (GROUPS, 1), 0)
        outer = zero
        for l in range(LEVELS_OUT):
            start = lax.div(g, 2**l) * 2**l
            summed = jnp.sum(jnp.where((row_of >= start) & (row_of < g), logs, 0.0), axis=0, keepdims=True)
            outer = jnp.where(lane8 == l + 3, summed, outer)
        run = zero
        for b in range(4):
            eb[4 + b : 5 + b, :] = run + outer
            run = run + ends[b : b + 1, :]

    with jax.named_scope("wait2"):
        def bucket(l, h):
            return jnp.concatenate([rcv2[l, 8 * e : 8 * e + 8].reshape(128, 128) for e in (h, h + 1)], axis=1)

        def scaled(n):
            rows = pl.ds(pl.multiple_of(n * 128, 128), 128)
            return rows, widened(scales(rows, eb[pl.ds(4 + lax.div(n, 2), 1), :]), 0)[0], bcs[rows, 128:]

        for l in range(LEVELS_OUT):
            @pl.when(bits[l] == 1)
            def _():
                remote(rcv2.at[l, pl.ds(0, GROUPS - 1)], rcv2.at[l, pl.ds(0, GROUPS - 1)], lsend.at[l], lrecv.at[l], group(g)).wait_recv()
                rcv2[l, g] = rcv1[2 * lax.div(g, 2)] if l == 0 else table[TABLE[l] + lax.div(g, 2 ** (l + 1))]

            if l < LEVELS_OUT - 1:
                @pl.when(bits[l] == 1)
                def _():
                    def add(n, _):
                        rows, pair_of, c = scaled(n)
                        for h in (0, 2):
                            cols = slice(128 * h, 128 * h + 256)
                            r = jnp.dot(c, bucket(l, h), preferred_element_type=F32)
                            yacc[rows, cols] += r * wide((pair_of, l + 3), cols)
                        return 0

                    lax.fori_loop(0, 8, add, 0)

    with jax.named_scope("finish"):
        last = LEVELS_OUT - 1

        @pl.when(bits[last] == 0)
        def _():
            rcv2[last] = jnp.zeros((GROUPS, 16, 128), BF16)

        def finish(b):
            for half in range(2):
                rows, pair_of, c = scaled(2 * b + half)
                for h in (0, 2):
                    cols = slice(128 * h, 128 * h + 256)
                    r = jnp.dot(c, bucket(last, h), preferred_element_type=F32)
                    vals = yacc[rows, cols] + r * wide((pair_of, last + 3), cols)
                    qs[b, 128 * half : 128 * half + 128, cols] = (vals * xf[rows, cols]).astype(BF16)

        def side(n):
            return lax.rem(y + n, NY)

        lower, upper = pl.ds(0, 128), pl.ds(128, 128)
        first_hop = [remote(qs.at[side(2), lower], relay.at[0], qsend.at[0], qrecv.at[0], beside(1)),
                     remote(qs.at[side(2), upper], relay.at[1], qsend.at[1], qrecv.at[1], beside(3))]
        next_hop = [remote(relay.at[0], qr.at[side(3), lower], qsend.at[2], qrecv.at[2], beside(1)),
                    remote(relay.at[1], qr.at[side(1), upper], qsend.at[3], qrecv.at[3], beside(3))]
        direct = [remote(qs.at[side(1)], qr.at[y], qsend.at[4], qrecv.at[4], beside(1)),
                  remote(qs.at[side(3)], qr.at[y], qsend.at[5], qrecv.at[5], beside(3))]
        finish(side(2))
        for copy in first_hop:
            copy.start()
        finish(side(1))
        direct[0].start()
        finish(side(3))
        direct[1].start()
        finish(y)
        for a, b in zip(first_hop, next_hop):
            a.wait_recv()
            b.start()
    with jax.named_scope("out"):
        qr[y] = qs[y]
        loads[-1].wait()

        squares = jnp.zeros((ROWS, 1), F32)
        sends = []
        for at, n in enumerate((0, 1, 3, 2)):
            src = lax.rem(y + NY - n, NY)
            if n == 1:
                direct[0].wait_recv()
            elif n == 3:
                direct[1].wait_recv()
            elif n == 2:
                for copy in next_hop:
                    copy.wait_recv()
            v = qr[src].astype(F32)
            squares = squares + jnp.sum(v * v, axis=1, keepdims=True)
            lanes = pl.ds(pl.multiple_of(src * 512, 512), 512)
            v = (v * gg[:, lanes]).astype(BF16)
            for t in range(4):
                cols = slice(512 * t, 512 * t + 512)
                part = jnp.dot(v, wout[lanes, cols], preferred_element_type=F32)
                if at < 3:
                    acc[:, cols] = part if at == 0 else acc[:, cols] + part
                    continue
                r = lax.rsqrt(squares * (1.0 / 2048.0) + EPS)
                os[t] = (ablk[y, :, cols].astype(F32) + r * (acc[:, cols] + part)).astype(BF16)
                sends.append(remote(os.at[t], (out_low, out_high)[t // 2].at[:, pl.ds(512 * (t % 2), 512)], osend.at[t], orecv.at[t], {"section": 1 - s}))
                sends[-1].start()
    with jax.named_scope("swap"):
        for copy in sends:
            copy.wait_recv()
    with jax.named_scope("drain"):
        for name in msgs:
            for copy in copies(name, False):
                copy.wait_send()
        back.wait_send()
        remote(rcv1.at[pl.ds(0, GROUPS - 1)], rcv1.at[pl.ds(0, GROUPS - 1)], ssem.at[0], rsem.at[0], group(g)).wait_send()
        remote(rlog.at[pl.ds(0, GROUPS - 1)], rlog.at[pl.ds(0, GROUPS - 1)], ssem.at[1], rsem.at[1], group(g)).wait_send()
        for l in range(LEVELS_OUT):
            for bit in range(2):
                @pl.when(bits[l] == bit)
                def _():
                    some = rcv2.at[l, pl.ds(0, 16 - bit)]
                    remote(some, some, lsend.at[l], lrecv.at[l], group(g)).wait_send()
        for copy in first_hop + next_hop + direct:
            copy.wait_send()
        for copy in sends:
            copy.wait_send()


def layer(acts, proj, wout, *params):
    anywhere = pl.BlockSpec(memory_space=pl.ANY)
    n = NY * ROWS
    count = 2 * len(plan())
    dma = pltpu.SemaphoreType.DMA
    return pl.pallas_call(
        layer_kernel,
        out_shape=[jax.ShapeDtypeStruct((ROWS, 1024), BF16)] * 2,
        in_specs=[anywhere] * (3 + len(params)),
        out_specs=[anywhere] * 2,
        scratch_shapes=[
            pltpu.VMEM((2048, CA), BF16),
            pltpu.VMEM((2048, CB), BF16),
            pltpu.VMEM((NY, ROWS, 2048), BF16),
            pltpu.VMEM((n, 2048), BF16),
            pltpu.VMEM((n, NP), F32),
            pltpu.VMEM((n, NP), BF16),
            pltpu.VMEM(proj.shape, BF16),
            pltpu.VMEM((NY, 16, 128), BF16),
            pltpu.VMEM((9, 256, 512), BF16),
            *[pltpu.VMEM(a.shape, a.dtype) for a in params],
            pltpu.VMEM((n + 8, 768), F32),
            pltpu.VMEM((n, 512), F32),
            pltpu.VMEM((n, 256), BF16),
            pltpu.VMEM((n, 128), F32),
            pltpu.VMEM((n, 128), F32),
            pltpu.VMEM((n, 512), F32),
            pltpu.VMEM((3, 128, 512), BF16),
            pltpu.VMEM((8, 128), F32),
            pltpu.VMEM((8, 512), F32),
            pltpu.VMEM((GROUPS, 16, 128), BF16),
            pltpu.VMEM((1, 128), F32),
            pltpu.VMEM((GROUPS, 16, 128), BF16),
            pltpu.VMEM((GROUPS, 1, 128), F32),
            pltpu.VMEM((31, 16, 128), BF16),
            pltpu.VMEM((LEVELS_OUT, GROUPS, 16, 128), BF16),
            pltpu.VMEM((16, 768), BF16),
            pltpu.VMEM((NY, ROWS, 512), BF16),
            pltpu.VMEM((NY, ROWS, 512), BF16),
            pltpu.VMEM((2, 128, 512), BF16),
            pltpu.VMEM((2048, 2048), BF16),
            pltpu.VMEM((ROWS, 2048), F32),
            pltpu.VMEM((4, ROWS, 512), BF16),
            dma((5,)), dma((count,)), dma((count,)), dma((11,)),
            dma((2,)), dma((2,)), dma((5,)), dma((5,)), dma((2,)), dma((6,)), dma((6,)), dma((4,)), dma((4,)),
        ],
        compiler_params=pltpu.CompilerParams(
            collective_id=0, has_side_effects=True, vmem_limit_bytes=58 * 1024 * 1024),
        name="layer",
    )(acts, proj, wout, *params)


def per_device(acts, in_proj, out_proj, conv_weight, conv_bias, dt_bias, decay_rate, skip_gain, level_bias, norm_gain, gate_gain):
    low, high = layer(acts[0], in_proj[0], out_proj[0], norm_gain, conv_weight[0], conv_bias, dt_bias, decay_rate, skip_gain, level_bias, gate_gain)
    return jnp.concatenate([low, high], axis=1)[None]


def solution(mesh):
    two = P("section", None)
    three = P("section", None, None)
    return jax.shard_map(
        per_device,
        mesh=mesh,
        in_specs=(P("section", "seq", None), P("section", "seq", None), three, three, two, two, two, two, two, two, two),
        out_specs=P("section", "seq", None),
        check_vma=False,
    )
```

```python
import functools
import jax
import jax.numpy as jnp
from jax import lax
from jax.experimental import pallas as pl
from jax.experimental.pallas import tpu as pltpu
from jax.sharding import PartitionSpec as P

EPS = 1e-05
MESH = pl.DeviceIdType.MESH
NX, NZ, NY = 4, 8, 4
GROUPS = NX * NZ
CA, CB = 512, 896
NP = CA + CB
ROWS = 256
F32, BF16 = jnp.float32, jnp.bfloat16


def seq_of(x, z, y):
    return (lax.rem(x + 4 * NX, NX) * NZ + lax.rem(z + 4 * NZ, NZ)) * NY + lax.rem(y + 4 * NY, NY)


def plan():
    msgs = {}
    ua, ub, un = 64 * CA * 2, 64 * CB * 2, 128 * 2048 * 2
    for d, links in ((1, {"y+": 1}), (3, {"y-": 1}), (2, {"y+": 1, "y-": 1})):
        msgs[("w", d)] = ("w", None, (0, 0, d), None, 16 * NP * 2, links)
    msgs[("P", 0)] = ("h0", 0, (0, 0, 1), None, un, {"y+": 1})
    msgs[("M", 1)] = ("h1", 0, (0, 0, -1), None, un, {"y-": 1})
    msgs[("P", 1)] = ("h1", 0, (0, 0, 1), None, un, {"y+": 1})
    msgs[("M", 0)] = ("h0", 0, (0, 0, -1), None, un, {"y-": 1})
    msgs[("P", 2)] = ("h0", -1, (0, 0, 1), ("P", 0), un, {"y+": 1})
    msgs[("M", 2)] = ("h1", 1, (0, 0, -1), ("M", 1), un, {"y-": 1})
    own = "own"
    for d, links in ((1, {"x+": 1}), (3, {"x-": 1}), (2, {"x+": 2})):
        msgs[("A1", d)] = ("a", (0, 0), (d, 0, 0), own, ua, links)
    for k in range(1, 5):
        if k < 5:
            dep = own if k == 1 else ("B1+", k - 1)
            msgs[("B1+", k)] = ("b", (0, -(k - 1)), (0, 1, 0), dep, ub, {"z+": 1})
        if k < 4:
            dep = own if k == 1 else ("B1-", k - 1)
            msgs[("B1-", k)] = ("b", (0, k - 1), (0, -1, 0), dep, ub, {"z-": 1})
    for k in range(1, 5):
        for d in range(4):
            up, down = (4, 3) if d < 2 else (3, 4)
            if k <= up:
                dep = (own if d == 0 else ("A1", d)) if k == 1 else ("A2+", d, k - 1)
                msgs[("A2+", d, k)] = ("a", (-d, -(k - 1)), (0, 1, 0), dep, ua, {"z+": 1})
            if k <= down:
                dep = (own if d == 0 else ("A1", d)) if k == 1 else ("A2-", d, k - 1)
                msgs[("A2-", d, k)] = ("a", (-d, k - 1), (0, -1, 0), dep, ua, {"z-": 1})
    offs = [0, -1, 1, -2, 2, -3, 3, -4]
    for o in offs:
        dep = own if o == 0 else (("B1+", -o) if o < 0 else ("B1-", o))
        msgs[("B2+", o)] = ("b", (0, o), (1, 0, 0), dep, ub, {"x+": 1})
        msgs[("B2-", o)] = ("b", (0, o), (-1, 0, 0), dep, ub, {"x-": 1})
        if o in (0, -1, 3, -4):
            msgs[("B2+2", o)] = ("b", (-1, o), (1, 0, 0), ("B2+", o), ub, {"x+": 1})
        else:
            msgs[("B2-2", o)] = ("b", (1, o), (-1, 0, 0), ("B2-", o), ub, {"x-": 1})
    return msgs


BOOST = {(way, d): b for way in ("A2+", "A2-") for d, b in enumerate((0.0, 0.0, -6.0, 0.0))}


def schedule(msgs, rate=46.6e3, latency=2.2, early=1.5, window=4.0):
    kids = {}
    for name, m in msgs.items():
        kids.setdefault(m[3], []).append(name)

    def path(name):
        _, _, _, _, size, links = msgs[name]
        step = size * max(links.values()) / rate + latency
        return step + max([path(k) for k in kids.get(name, [])], default=0.0)

    def boost(name):
        return 100.0 if msgs[name][0] == "w" else BOOST.get(name[:2], 0.0) if name[0][:2] == "A2" else 0.0

    rank = {name: -path(name) - boost(name) for name in msgs}
    free, arrive, events, waiting, plan_of, got = {}, {}, [], [], [], set()

    def issue(now):
        sent = []
        for name in sorted(waiting, key=lambda n: (rank[n], str(n))):
            part, _, _, _, size, links = msgs[name]
            if part != "w" and any(free.get(l, 0.0) > now + window for l in links):
                continue
            begin = max([now] + [free.get(l, 0.0) for l in links])
            for l, n in links.items():
                free[l] = begin + size * n / rate
            arrive[name] = max(free[l] for l in links) + latency + (early if part == "w" else 0.0)
            events.append((arrive[name], len(arrive), name))
            sent.append(name)
        for name in sent:
            waiting.remove(name)
        return sent

    waiting += kids[None]
    first = issue(0.0)
    while events:
        events.sort()
        now, _, name = events.pop(0)
        waiting += kids.get(name, [])
        got.add(name)
        plan_of.append((name, issue(now)))
        if "own" not in got and all(("w", d) in got for d in (1, 2, 3)):
            got.add("own")
            waiting += kids["own"]
            plan_of.append(("own", issue(now)))
    assert not waiting
    return first, plan_of, arrive


HI = lax.Precision.HIGHEST
MID = CA + 768
LEVELS_OUT = 5
TABLE = (0, 16, 24, 28, 30)


def spread(row, lanes):
    k = lax.broadcasted_iota(jnp.int32, (128, lanes), 0)
    c = lax.broadcasted_iota(jnp.int32, (128, lanes), 1)
    return jnp.dot(row, (k == 64 + 8 * lax.shift_right_logical(c, 6)).astype(F32), precision=HI, preferred_element_type=F32)


def halves_of(a, lane_low, lane_high, first):
    return jnp.where(first, a[:, lane_low : lane_low + 1], a[:, lane_high : lane_high + 1])


def softplus(v):
    return jnp.maximum(v, 0.0) + jnp.log1p(jnp.exp(-jnp.abs(v)))


def layer_kernel(acts_in, proj_in, wout_in, gain_in, cw_in, cb_in, dtb_in, rate_in, skip_in, lb_in, gg_in, out_low, out_high,
                 wa, wb, ablk, u, pacc, p, proj, small, ones,
                 gain, cw, cb, dtb, rate, skip, lb, gg,
                 ext, xf, bcs, td, cu, yacc, near_st, eb, ee, snd1, slog, rcv1, rlog, table, rcv2, tail,
                 qs, qr, relay, wout, acc, os,
                 local_sems, send_sems, recv_sems, in_sems,
                 ssem, rsem, lsend, lrecv, tsem, qsend, qrecv, osend, orecv):
    i = lax.axis_index("seq")
    y = lax.rem(i, NY)
    g = lax.div(i, NY)
    z = lax.rem(g, NZ)
    x = lax.div(g, NZ)
    s = lax.axis_index("section")

    def there(dx, dz, dy):
        return {"seq": seq_of(x + dx, z + dz, y + dy)}

    def group(n):
        return {"seq": n * NY + y}

    def beside(n):
        return {"seq": g * NY + lax.rem(y + n, NY)}

    def wrap(n):
        return lax.rem(n, GROUPS)

    def remote(src, dst, send, recv, to):
        return pltpu.make_async_remote_copy(
            src_ref=src, dst_ref=dst, send_sem=send, recv_sem=recv, device_id=to, device_id_type=MESH)

    with jax.named_scope("enter"):
        barrier = pltpu.get_barrier_semaphore()

        near = ((1, 0, 0), (-1, 0, 0), (2, 0, 0), (0, 1, 0), (0, -1, 0), (0, 0, 1), (0, 0, -1), (0, 0, 2))
        for to in near:
            pl.semaphore_signal(barrier, inc=1, device_id=there(*to), device_id_type=MESH)
        pl.semaphore_signal(barrier, inc=1, device_id={"section": 1 - s}, device_id_type=MESH)
        pairs = ((proj_in, proj), (acts_in, ablk.at[y]), (gain_in, gain), (cw_in, cw), (cb_in, cb), (dtb_in, dtb),
                 (rate_in, rate), (skip_in, skip), (lb_in, lb), (gg_in, gg), (wout_in, wout))
        loads = [pltpu.make_async_copy(a, b, in_sems.at[n]) for n, (a, b) in enumerate(pairs)]
        for copy in loads[:-1]:
            copy.start()

        loads[0].wait()
        rows_k = lax.broadcasted_iota(jnp.int32, (288, 128), 0)
        lane_k = lax.broadcasted_iota(jnp.int32, (288, 128), 1)
        packed = proj[:, 4352:]
        for n in range(NY):
            from_lr = (lane_k < 64) & (rows_k == 32 + 64 * n + lane_k)
            from_dr = (lane_k >= 64) & (rows_k == 8 * n + lax.shift_right_logical(lane_k - 64, 3))
            hit = (from_lr | from_dr).astype(BF16)
            small[n] = jnp.dot(packed, hit, preferred_element_type=F32).astype(BF16)

        msgs = plan()
        number = {name: n for n, name in enumerate(msgs)}
        first_sends, steps, _ = schedule(msgs)

        def block(rel):
            return lax.rem(y + rel + 2 * NY, NY)

        def rows_of(cx, cz):
            return pl.ds(pl.multiple_of(seq_of(x + cx, z + cz, 0) * 16, 64), 64)

        def pieces(slot, rows):
            cols = pl.multiple_of(slot * 512, 512)
            return [(proj.at[:, pl.ds(cols, 512)], wa.at[rows]),
                    (proj.at[:, pl.ds(2048, 256)], wb.at[rows, pl.ds(0, 256)]),
                    (proj.at[:, pl.ds(pl.multiple_of(2304 + cols, 256), 512)], wb.at[rows, pl.ds(256, 512)]),
                    (small.at[slot], wb.at[rows, pl.ds(768, 128)])]

        mine = pl.ds(pl.multiple_of(i * 16, 16), 16)
        local = [pltpu.make_async_copy(a, b, local_sems.at[n]) for n, (a, b) in enumerate(pieces(y, mine))]
        for copy in local:
            copy.start()
        loads[1].wait()
        pl.semaphore_wait(barrier, len(near) + 1)

    def copies(name, arriving):
        part, chunk, to, dep, _, _ = msgs[name]
        n = number[name]
        back = to if arriving else (0, 0, 0)
        if part == "w":
            d = to[2]
            rows = pl.ds(pl.multiple_of(seq_of(x, z, y - d) * 16, 16), 16) if arriving else mine
            slot = lax.rem(y + d, NY)
            return [remote(a, b, send_sems.at[n if e == 0 else len(msgs) + 4 * n + e], recv_sems.at[n if e == 0 else len(msgs) + 4 * n + e], there(*to))
                    for e, (a, b) in enumerate(pieces(slot, rows))]
        if part in ("h0", "h1"):
            ref = ablk.at[block(chunk - back[2]), pl.ds(128 * int(part[1]), 128)]
        else:
            ref = (wa if part == "a" else wb).at[rows_of(chunk[0] - back[0], chunk[1] - back[1])]
        return [remote(ref, ref, send_sems.at[n], recv_sems.at[n], there(*to))]

    def start(name):
        for copy in copies(name, False):
            copy.start()

    def normed(rel, half):
        def step(n, _):
            at = pl.multiple_of(half * 128 + n * 64, 64)
            b = block(rel)
            h = ablk[b, pl.ds(at, 64), :].astype(F32)
            r = lax.rsqrt(jnp.mean(h * h, axis=1, keepdims=True) + EPS)
            u[pl.ds(pl.multiple_of(b * ROWS + at, 64), 64), :] = (h * r * gain[...]).astype(BF16)
            return 0

        lax.fori_loop(0, 2, step, 0)

    with jax.named_scope("gather"):
        for name in first_sends:
            start(name)
        for copy in loads[2:-1]:
            copy.wait()
        loads[-1].start()
        normed(0, 0)
        normed(0, 1)
        def picked(v, hit):
            rows = jnp.broadcast_to(v[...], (8, v.shape[1]))
            return jnp.dot(rows, hit.astype(F32), precision=HI, preferred_element_type=F32)[:1]

        def two(rows, lanes):
            return (lax.broadcasted_iota(jnp.int32, (rows, lanes), 0), lax.broadcasted_iota(jnp.int32, (rows, lanes), 1))

        k, c = two(32, 128)
        of_head = (c >= 64) & (k == 8 * y + lax.shift_right_logical(c - 64, 3))
        k2, c2 = two(256, 128)
        bias = picked(dtb, of_head) + picked(lb, (c2 < 64) & (k2 == 64 * y + c2))
        rates = picked(rate, of_head)
        k3, c3 = two(32, 512)
        skips = picked(skip, k3 == 8 * y + lax.shift_right_logical(c3, 6))

        low_tri = (lax.broadcasted_iota(jnp.int32, (ROWS, ROWS), 1) <= lax.broadcasted_iota(jnp.int32, (ROWS, ROWS), 0)).astype(BF16)
        lane_in, col_in = two(256, 512)
        for lev in range(9):
            lane = lev + 8 * lax.shift_right_logical(col_in, 6) + (64 - 8 if lev == 8 else 0)
            ones[lev] = ((lane_in & 127) == lane).astype(BF16)

        def widened(v, lev):
            high = v.astype(BF16)
            low = (v - high.astype(F32)).astype(BF16)
            return jnp.concatenate([high, low], axis=1), lev

        def wide(pair, cols=slice(0, 512)):
            return jnp.dot(pair[0], ones[pair[1], :, cols], preferred_element_type=F32)

        halves = {("P", 0): (-1, 0), ("P", 1): (-1, 1), ("M", 1): (1, 1), ("M", 0): (1, 0), ("P", 2): (-2, 0), ("M", 2): (2, 1)}
        missing = {(part, d): set() for d in range(NX) for part in "ab"}
        for name, m in msgs.items():
            if m[0] in ("a", "b"):
                missing[(m[0], (m[2][0] - m[1][0]) % NX)].add(name)
        lacking = {-1: {("P", 0), ("P", 1)}, 1: {("M", 1), ("M", 0)}, -2: {("P", 2), ("M", 2)}}
        here, held, ready, counted = [0], [], [], {}

        def multiply():
            which = ready[0][1]
            rels = [rel for rel, other in ready if other == which]
            ready[:] = [e for e in ready if e[1] != which]
            part, d = which
            rows = [pl.ds(pl.multiple_of(block(rel) * ROWS, ROWS), ROWS) for rel in rels]
            deep = pl.ds(pl.multiple_of(lax.rem(x + NX - d, NX) * 512, 512), 512)
            w, cols = (wa, slice(0, CA)) if part == "a" else (wb, slice(CA, NP))
            left = jnp.concatenate([u[r, deep] for r in rows], axis=0)
            full = jnp.dot(left, w[deep, :], preferred_element_type=F32)
            for e, (rel, at) in enumerate(zip(rels, rows)):
                done = counted[rel, part] = counted.get((rel, part), 0) + 1
                r = full[e * ROWS : (e + 1) * ROWS]
                if done > 1:
                    r = r + pacc[at, cols]
                if done == NX:
                    p[at, cols] = r.astype(BF16)
                else:
                    pacc[at, cols] = r

        for name, then in steps:
            if name == "own":
                for copy in local:
                    copy.wait()
            else:
                for copy in copies(name, True):
                    copy.wait_recv()
            for other in then:
                start(other)
            if name in halves:
                normed(*halves[name])
            for rel, left in list(lacking.items()):
                left.discard(name)
                if not left:
                    del lacking[rel]
                    here.append(rel)
                    ready += [(rel, d) for d in held]
            for d, left in list(missing.items()):
                left.discard(name)
                if not left:
                    del missing[d]
                    held.append(d)
                    ready += [(rel, d) for rel in here]
            if ready:
                multiply()
        while ready:
            multiply()

    with jax.named_scope("rows"):
        for b in range(4):
            rows = slice(b * ROWS, (b + 1) * ROWS)
            t = softplus(p[rows, MID:].astype(F32) + bias)
            td[rows, :] = t
            left = -t * rates
            total = jnp.zeros((ROWS, 128), F32)
            for _ in range(3):
                piece = left.astype(BF16)
                total = total + jnp.dot(low_tri, piece, preferred_element_type=F32)
                left = left - piece.astype(F32)
            cu[rows, :] = total
            eb[b : b + 1, :] = total[ROWS - 1 :, :]
        eb[4:, :] = jnp.zeros((4, 128), F32)
        ends = eb[...]
        ee[...] = jnp.exp(spread(ends, 512))
        slog[...] = jnp.sum(ends, axis=0, keepdims=True)

    with jax.named_scope("conv"):
        back = remote(p.at[pl.ds(1008, 16), pl.ds(0, 768)], tail, tsem.at[0], tsem.at[1], group(wrap(g + 1)))
        back.start()

        for n in range(4):
            ext[8 + n * ROWS : 8 + (n + 1) * ROWS, :] = p[n * ROWS : (n + 1) * ROWS, :768].astype(F32)
        own = pl.ds(pl.multiple_of(y * 512, 512), 512)
        tx = [cw[k : k + 1, own] for k in range(4)]
        tb = [cw[k : k + 1, 2048:] for k in range(4)]
        bx, bb = cb[:, own], cb[:, 2048:]

        def convolved(n):
            at = n * 128
            v = bx
            for k in range(4):
                v = v + tx[k] * ext[at + 5 + k : at + 133 + k, :512]
            xf[at : at + 128, :] = jax.nn.silu(v)
            v = bb
            for k in range(4):
                v = v + tb[k] * ext[at + 5 + k : at + 133 + k, 512:]
            bcs[at : at + 128, :] = jax.nn.silu(v).astype(BF16)

        for n in range(1, 8):
            convolved(n)
        back.wait_recv()
        before = tail[...].astype(F32)
        ext[0:8, :] = jnp.where(g > 0, before[8:, :], 0.0)
        convolved(0)

    with jax.named_scope("states"):
        first = lax.broadcasted_iota(jnp.int32, (1, 128), 1) < 64

        def state(b):
            rows = slice(b * ROWS, (b + 1) * ROWS)
            tl = jnp.exp(ends[b : b + 1, :] - cu[rows, :]) * td[rows, :]
            xt = (xf[rows, :] * wide(widened(tl, 8))).astype(BF16)
            return lax.dot_general(bcs[rows, :128], xt, (((0,), (0,)), ((), ())), preferred_element_type=F32)

        st = state(0)
        near_st[0] = st.astype(BF16)
        st = ee[1:2, :] * st + state(1)
        near_st[1] = st.astype(BF16)
        other = state(2)
        near_st[2] = other.astype(BF16)
        st = ee[2:3, :] * ee[3:4, :] * st + ee[3:4, :] * other + state(3)
        st = st.astype(BF16)
        for n in range(GROUPS):
            ct, nt = n // 8, n % 8
            snd1[n] = st[16 * nt : 16 * nt + 16, 128 * ct : 128 * ct + 128]

        def first_send(d, _):
            to = wrap(g + d)
            remote(snd1.at[to], rcv1.at[g], ssem.at[0], rsem.at[0], group(to)).start()
            remote(slog, rlog.at[g], ssem.at[1], rsem.at[1], group(to)).start()
            return 0

        lax.fori_loop(1, GROUPS, first_send, 0)
        rcv1[g] = snd1[g]
        rlog[g] = slog[...]

    with jax.named_scope("inside"):
        def inside(b, _):
            base = pl.multiple_of(b * ROWS, ROWS)
            every = pl.ds(base, ROWS)
            cum_t = jnp.transpose(cu[every, :])
            dt_t = jnp.transpose(td[every, :])
            for r in range(2):
                rows = pl.ds(pl.multiple_of(base + 128 * r, 128), 128)
                reach = 128 * (r + 1)
                seen = pl.ds(base, reach)
                scores = lax.dot_general(bcs[rows, 128:], bcs[seen, :128], (((1,), (1,)), ((), ())), preferred_element_type=F32)
                ti, si = two(128, reach)
                causal = si <= ti + 128 * r
                cum, lam = cu[rows, :], wide(widened(td[rows, :], 0))
                for h in range(4):
                    xp = xf[seen, 128 * h : 128 * h + 128].astype(BF16)
                    got = []
                    for e in (2 * h, 2 * h + 1):
                        lane = 64 + 8 * e
                        differ = jnp.where(causal, cum[:, lane : lane + 1] - cum_t[lane : lane + 1, :reach], -1e30)
                        w = scores * jnp.exp(differ) * dt_t[lane : lane + 1, :reach]
                        got.append(jnp.dot(w.astype(BF16), xp, preferred_element_type=F32))
                    cols = slice(128 * h, 128 * h + 128)
                    val = jnp.where(first, got[0], got[1]) * lam[:, cols]
                    yacc[rows, cols] = val + skips[:, cols] * xf[rows, cols]
            return 0

        lax.fori_loop(0, 4, inside, 0)

    with jax.named_scope("near"):
        lane8 = lax.broadcasted_iota(jnp.int32, (1, 128), 1) & 7

        def read(b, rows, bucket, scale, lev):
            r = jnp.dot(bcs[rows, 128:], bucket, preferred_element_type=F32)
            yacc[rows, :] += r * wide(widened(scale, lev))

        def scales(rows, add):
            return pltpu.roll(jnp.exp(cu[rows, :] + add), 64, 1) * td[rows, :]

        zero = jnp.zeros((1, 128), F32)
        at_block = [pl.ds(b * ROWS, ROWS) for b in range(4)]
        read(1, at_block[1], near_st[0], scales(at_block[1], zero), 1)
        read(2, at_block[2], near_st[1], scales(at_block[2], zero), 2)
        sc = scales(at_block[3], jnp.where(lane8 == 2, ends[2:3, :], 0.0))
        read(3, at_block[3], near_st[2], sc, 1)
        read(3, at_block[3], near_st[1], sc, 2)

        def gates(n, _):
            rows = pl.ds(pl.multiple_of(n * 128, 128), 128)
            v = p[rows, 768:1280].astype(F32)
            xf[rows, :] = jax.nn.silu(v)
            return 0

        lax.fori_loop(0, 8, gates, 0)

    with jax.named_scope("wait1"):
        remote(rcv1.at[pl.ds(0, GROUPS - 1)], rcv1.at[pl.ds(0, GROUPS - 1)], ssem.at[0], rsem.at[0], group(g)).wait_recv()
        remote(rlog.at[pl.ds(0, GROUPS - 1)], rlog.at[pl.ds(0, GROUPS - 1)], ssem.at[1], rsem.at[1], group(g)).wait_recv()
    with jax.named_scope("merge"):
        logs = rlog[:, 0, :]
        wide_logs = spread(logs, 512)
        ct = lax.div(g, 8)
        head_logs = jnp.zeros((GROUPS, 128), F32)
        for n in range(4):
            head_logs = jnp.where(ct == n, wide_logs[:, 128 * n : 128 * n + 128], head_logs)
        bits = [lax.rem(lax.div(g, 2**l), 2) for l in range(LEVELS_OUT)]

        def give(l):
            own = lax.div(g, 2 ** (l + 1)) * 2**l + lax.rem(g, 2**l)

            def to_one(k, _):
                at = lax.rem(own + k, 16)
                half = lax.div(at, 2**l)
                to = (2 * half + 1) * 2**l + lax.rem(at, 2**l)
                src = rcv1.at[2 * half] if l == 0 else table.at[TABLE[l] + half]
                remote(src, rcv2.at[l, g], lsend.at[l], lrecv.at[l], group(to)).start()
                return 0

            lax.fori_loop(1, 16, to_one, 0)

            @pl.when(bits[l] == 0)
            def _():
                to_one(0, 0)

        give(0)
        level = [rcv1[n].astype(F32) for n in range(GROUPS)]
        ends_of = [head_logs[n : n + 1, :] for n in range(GROUPS)]
        for l in range(1, LEVELS_OUT):
            level = [jnp.exp(ends_of[n + 1]) * level[n] + level[n + 1] for n in range(0, len(level), 2)]
            ends_of = [ends_of[n] + ends_of[n + 1] for n in range(0, len(ends_of), 2)]
            for n in range(0, len(level), 2):
                table[TABLE[l] + n // 2] = level[n].astype(BF16)
            give(l)

    with jax.named_scope("outer"):
        row_of = lax.broadcasted_iota(jnp.int32, (GROUPS, 1), 0)
        outer = zero
        for l in range(LEVELS_OUT):
            start = lax.div(g, 2**l) * 2**l
            summed = jnp.sum(jnp.where((row_of >= start) & (row_of < g), logs, 0.0), axis=0, keepdims=True)
            outer = jnp.where(lane8 == l + 3, summed, outer)
        run = zero
        for b in range(4):
            eb[4 + b : 5 + b, :] = run + outer
            run = run + ends[b : b + 1, :]

    with jax.named_scope("wait2"):
        def bucket(l, h):
            return jnp.concatenate([rcv2[l, 8 * e : 8 * e + 8].reshape(128, 128) for e in (h, h + 1)], axis=1)

        def scaled(n):
            rows = pl.ds(pl.multiple_of(n * 128, 128), 128)
            return rows, widened(scales(rows, eb[pl.ds(4 + lax.div(n, 2), 1), :]), 0)[0], bcs[rows, 128:]

        for l in range(LEVELS_OUT):
            @pl.when(bits[l] == 1)
            def _():
                remote(rcv2.at[l, pl.ds(0, GROUPS - 1)], rcv2.at[l, pl.ds(0, GROUPS - 1)], lsend.at[l], lrecv.at[l], group(g)).wait_recv()
                rcv2[l, g] = rcv1[2 * lax.div(g, 2)] if l == 0 else table[TABLE[l] + lax.div(g, 2 ** (l + 1))]

            if l < LEVELS_OUT - 1:
                @pl.when(bits[l] == 1)
                def _():
                    def add(n, _):
                        rows, pair_of, c = scaled(n)
                        for h in (0, 2):
                            cols = slice(128 * h, 128 * h + 256)
                            r = jnp.dot(c, bucket(l, h), preferred_element_type=F32)
                            yacc[rows, cols] += r * wide((pair_of, l + 3), cols)
                        return 0

                    lax.fori_loop(0, 8, add, 0)

    with jax.named_scope("finish"):
        last = LEVELS_OUT - 1

        @pl.when(bits[last] == 0)
        def _():
            rcv2[last] = jnp.zeros((GROUPS, 16, 128), BF16)

        def finish(b):
            for half in range(2):
                rows, pair_of, c = scaled(2 * b + half)
                for h in (0, 2):
                    cols = slice(128 * h, 128 * h + 256)
                    r = jnp.dot(c, bucket(last, h), preferred_element_type=F32)
                    vals = yacc[rows, cols] + r * wide((pair_of, last + 3), cols)
                    qs[b, 128 * half : 128 * half + 128, cols] = (vals * xf[rows, cols]).astype(BF16)

        def side(n):
            return lax.rem(y + n, NY)

        lower, upper = pl.ds(0, 128), pl.ds(128, 128)
        first_hop = [remote(qs.at[side(2), lower], relay.at[0], qsend.at[0], qrecv.at[0], beside(1)),
                     remote(qs.at[side(2), upper], relay.at[1], qsend.at[1], qrecv.at[1], beside(3))]
        next_hop = [remote(relay.at[0], qr.at[side(3), lower], qsend.at[2], qrecv.at[2], beside(1)),
                    remote(relay.at[1], qr.at[side(1), upper], qsend.at[3], qrecv.at[3], beside(3))]
        direct = [remote(qs.at[side(1)], qr.at[y], qsend.at[4], qrecv.at[4], beside(1)),
                  remote(qs.at[side(3)], qr.at[y], qsend.at[5], qrecv.at[5], beside(3))]
        finish(side(2))
        for copy in first_hop:
            copy.start()
        finish(side(1))
        direct[0].start()
        finish(side(3))
        direct[1].start()
        finish(y)
        for a, b in zip(first_hop, next_hop):
            a.wait_recv()
            b.start()
    with jax.named_scope("out"):
        qr[y] = qs[y]
        loads[-1].wait()

        squares = jnp.zeros((ROWS, 1), F32)
        sends = []
        for at, n in enumerate((0, 1, 3, 2)):
            src = lax.rem(y + NY - n, NY)
            if n == 1:
                direct[0].wait_recv()
            elif n == 3:
                direct[1].wait_recv()
            elif n == 2:
                for copy in next_hop:
                    copy.wait_recv()
            v = qr[src].astype(F32)
            squares = squares + jnp.sum(v * v, axis=1, keepdims=True)
            lanes = pl.ds(pl.multiple_of(src * 512, 512), 512)
            v = (v * gg[:, lanes]).astype(BF16)
            for t in range(4):
                cols = slice(512 * t, 512 * t + 512)
                part = jnp.dot(v, wout[lanes, cols], preferred_element_type=F32)
                if at < 3:
                    acc[:, cols] = part if at == 0 else acc[:, cols] + part
                    continue
                r = lax.rsqrt(squares * (1.0 / 2048.0) + EPS)
                os[t] = (ablk[y, :, cols].astype(F32) + r * (acc[:, cols] + part)).astype(BF16)
                sends.append(remote(os.at[t], (out_low, out_high)[t // 2].at[:, pl.ds(512 * (t % 2), 512)], osend.at[t], orecv.at[t], {"section": 1 - s}))
                sends[-1].start()
    with jax.named_scope("swap"):
        for copy in sends:
            copy.wait_recv()
    with jax.named_scope("drain"):
        for name in msgs:
            for copy in copies(name, False):
                copy.wait_send()
        back.wait_send()
        remote(rcv1.at[pl.ds(0, GROUPS - 1)], rcv1.at[pl.ds(0, GROUPS - 1)], ssem.at[0], rsem.at[0], group(g)).wait_send()
        remote(rlog.at[pl.ds(0, GROUPS - 1)], rlog.at[pl.ds(0, GROUPS - 1)], ssem.at[1], rsem.at[1], group(g)).wait_send()
        for l in range(LEVELS_OUT):
            for bit in range(2):
                @pl.when(bits[l] == bit)
                def _():
                    some = rcv2.at[l, pl.ds(0, 16 - bit)]
                    remote(some, some, lsend.at[l], lrecv.at[l], group(g)).wait_send()
        for copy in first_hop + next_hop + direct:
            copy.wait_send()
        for copy in sends:
            copy.wait_send()


def layer(acts, proj, wout, *params):
    anywhere = pl.BlockSpec(memory_space=pl.ANY)
    n = NY * ROWS
    count = 2 * len(plan())
    dma = pltpu.SemaphoreType.DMA
    return pl.pallas_call(
        layer_kernel,
        out_shape=[jax.ShapeDtypeStruct((ROWS, 1024), BF16)] * 2,
        in_specs=[anywhere] * (3 + len(params)),
        out_specs=[anywhere] * 2,
        scratch_shapes=[
            pltpu.VMEM((2048, CA), BF16),
            pltpu.VMEM((2048, CB), BF16),
            pltpu.VMEM((NY, ROWS, 2048), BF16),
            pltpu.VMEM((n, 2048), BF16),
            pltpu.VMEM((n, NP), F32),
            pltpu.VMEM((n, NP), BF16),
            pltpu.VMEM(proj.shape, BF16),
            pltpu.VMEM((NY, 16, 128), BF16),
            pltpu.VMEM((9, 256, 512), BF16),
            *[pltpu.VMEM(a.shape, a.dtype) for a in params],
            pltpu.VMEM((n + 8, 768), F32),
            pltpu.VMEM((n, 512), F32),
            pltpu.VMEM((n, 256), BF16),
            pltpu.VMEM((n, 128), F32),
            pltpu.VMEM((n, 128), F32),
            pltpu.VMEM((n, 512), F32),
            pltpu.VMEM((3, 128, 512), BF16),
            pltpu.VMEM((8, 128), F32),
            pltpu.VMEM((8, 512), F32),
            pltpu.VMEM((GROUPS, 16, 128), BF16),
            pltpu.VMEM((1, 128), F32),
            pltpu.VMEM((GROUPS, 16, 128), BF16),
            pltpu.VMEM((GROUPS, 1, 128), F32),
            pltpu.VMEM((31, 16, 128), BF16),
            pltpu.VMEM((LEVELS_OUT, GROUPS, 16, 128), BF16),
            pltpu.VMEM((16, 768), BF16),
            pltpu.VMEM((NY, ROWS, 512), BF16),
            pltpu.VMEM((NY, ROWS, 512), BF16),
            pltpu.VMEM((2, 128, 512), BF16),
            pltpu.VMEM((2048, 2048), BF16),
            pltpu.VMEM((ROWS, 2048), F32),
            pltpu.VMEM((4, ROWS, 512), BF16),
            dma((5,)), dma((count,)), dma((count,)), dma((11,)),
            dma((2,)), dma((2,)), dma((5,)), dma((5,)), dma((2,)), dma((6,)), dma((6,)), dma((4,)), dma((4,)),
        ],
        compiler_params=pltpu.CompilerParams(
            collective_id=0, has_side_effects=True, vmem_limit_bytes=58 * 1024 * 1024),
        name="layer",
    )(acts, proj, wout, *params)


def per_device(acts, in_proj, out_proj, conv_weight, conv_bias, dt_bias, decay_rate, skip_gain, level_bias, norm_gain, gate_gain):
    low, high = layer(acts[0], in_proj[0], out_proj[0], norm_gain, conv_weight[0], conv_bias, dt_bias, decay_rate, skip_gain, level_bias, gate_gain)
    return jnp.concatenate([low, high], axis=1)[None]


def solution(mesh):
    two = P("section", None)
    three = P("section", None, None)
    return jax.shard_map(
        per_device,
        mesh=mesh,
        in_specs=(P("section", "seq", None), P("section", "seq", None), three, three, two, two, two, two, two, two, two),
        out_specs=P("section", "seq", None),
        check_vma=False,
    )
```

```python
import functools
import jax
import jax.numpy as jnp
from jax import lax
from jax.experimental import pallas as pl
from jax.experimental.pallas import tpu as pltpu
from jax.sharding import PartitionSpec as P

EPS = 1e-05
MESH = pl.DeviceIdType.MESH
NX, NZ, NY = 4, 8, 4
GROUPS = NX * NZ
CA, CB = 512, 896
NP = CA + CB
ROWS = 256
F32, BF16 = jnp.float32, jnp.bfloat16


def seq_of(x, z, y):
    return (lax.rem(x + 4 * NX, NX) * NZ + lax.rem(z + 4 * NZ, NZ)) * NY + lax.rem(y + 4 * NY, NY)


def plan():
    msgs = {}
    ua, ub, un = 64 * CA * 2, 64 * CB * 2, 128 * 2048 * 2
    for d, links in ((1, {"y+": 1}), (3, {"y-": 1}), (2, {"y+": 1, "y-": 1})):
        msgs[("w", d)] = ("w", None, (0, 0, d), None, 16 * NP * 2, links)
    msgs[("P", 0)] = ("h0", 0, (0, 0, 1), None, un, {"y+": 1})
    msgs[("M", 1)] = ("h1", 0, (0, 0, -1), None, un, {"y-": 1})
    msgs[("P", 1)] = ("h1", 0, (0, 0, 1), None, un, {"y+": 1})
    msgs[("M", 0)] = ("h0", 0, (0, 0, -1), None, un, {"y-": 1})
    msgs[("P", 2)] = ("h0", -1, (0, 0, 1), ("P", 0), un, {"y+": 1})
    msgs[("M", 2)] = ("h1", 1, (0, 0, -1), ("M", 1), un, {"y-": 1})
    own = "own"
    for d, links in ((1, {"x+": 1}), (3, {"x-": 1}), (2, {"x+": 2})):
        msgs[("A1", d)] = ("a", (0, 0), (d, 0, 0), own, ua, links)
    for k in range(1, 5):
        if k < 5:
            dep = own if k == 1 else ("B1+", k - 1)
            msgs[("B1+", k)] = ("b", (0, -(k - 1)), (0, 1, 0), dep, ub, {"z+": 1})
        if k < 4:
            dep = own if k == 1 else ("B1-", k - 1)
            msgs[("B1-", k)] = ("b", (0, k - 1), (0, -1, 0), dep, ub, {"z-": 1})
    for k in range(1, 5):
        for d in range(4):
            up, down = (4, 3) if d < 2 else (3, 4)
            if k <= up:
                dep = (own if d == 0 else ("A1", d)) if k == 1 else ("A2+", d, k - 1)
                msgs[("A2+", d, k)] = ("a", (-d, -(k - 1)), (0, 1, 0), dep, ua, {"z+": 1})
            if k <= down:
                dep = (own if d == 0 else ("A1", d)) if k == 1 else ("A2-", d, k - 1)
                msgs[("A2-", d, k)] = ("a", (-d, k - 1), (0, -1, 0), dep, ua, {"z-": 1})
    offs = [0, -1, 1, -2, 2, -3, 3, -4]
    for o in offs:
        dep = own if o == 0 else (("B1+", -o) if o < 0 else ("B1-", o))
        msgs[("B2+", o)] = ("b", (0, o), (1, 0, 0), dep, ub, {"x+": 1})
        msgs[("B2-", o)] = ("b", (0, o), (-1, 0, 0), dep, ub, {"x-": 1})
        if o in (0, -1, 3, -4):
            msgs[("B2+2", o)] = ("b", (-1, o), (1, 0, 0), ("B2+", o), ub, {"x+": 1})
        else:
            msgs[("B2-2", o)] = ("b", (1, o), (-1, 0, 0), ("B2-", o), ub, {"x-": 1})
    return msgs


BOOST = {(way, d): b for way in ("A2+", "A2-") for d, b in enumerate((0.0, 0.0, -6.0, 0.0))}


def schedule(msgs, rate=46.6e3, latency=2.2, early=1.5, window=4.0):
    kids = {}
    for name, m in msgs.items():
        kids.setdefault(m[3], []).append(name)

    def path(name):
        _, _, _, _, size, links = msgs[name]
        step = size * max(links.values()) / rate + latency
        return step + max([path(k) for k in kids.get(name, [])], default=0.0)

    def boost(name):
        return 100.0 if msgs[name][0] == "w" else BOOST.get(name[:2], 0.0) if name[0][:2] == "A2" else 0.0

    rank = {name: -path(name) - boost(name) for name in msgs}
    free, arrive, events, waiting, plan_of, got = {}, {}, [], [], [], set()

    def issue(now):
        sent = []
        for name in sorted(waiting, key=lambda n: (rank[n], str(n))):
            part, _, _, _, size, links = msgs[name]
            if part != "w" and any(free.get(l, 0.0) > now + window for l in links):
                continue
            begin = max([now] + [free.get(l, 0.0) for l in links])
            for l, n in links.items():
                free[l] = begin + size * n / rate
            arrive[name] = max(free[l] for l in links) + latency + (early if part == "w" else 0.0)
            events.append((arrive[name], len(arrive), name))
            sent.append(name)
        for name in sent:
            waiting.remove(name)
        return sent

    waiting += kids[None]
    first = issue(0.0)
    while events:
        events.sort()
        now, _, name = events.pop(0)
        waiting += kids.get(name, [])
        got.add(name)
        plan_of.append((name, issue(now)))
        if "own" not in got and all(("w", d) in got for d in (1, 2, 3)):
            got.add("own")
            waiting += kids["own"]
            plan_of.append(("own", issue(now)))
    assert not waiting
    return first, plan_of, arrive


HI = lax.Precision.HIGHEST
MID = CA + 768
LEVELS_OUT = 5
TABLE = (0, 16, 24, 28, 30)


def spread(row, lanes):
    k = lax.broadcasted_iota(jnp.int32, (128, lanes), 0)
    c = lax.broadcasted_iota(jnp.int32, (128, lanes), 1)
    return jnp.dot(row, (k == 64 + 8 * lax.shift_right_logical(c, 6)).astype(F32), precision=HI, preferred_element_type=F32)


def halves_of(a, lane_low, lane_high, first):
    return jnp.where(first, a[:, lane_low : lane_low + 1], a[:, lane_high : lane_high + 1])


def softplus(v):
    return jnp.maximum(v, 0.0) + jnp.log1p(jnp.exp(-jnp.abs(v)))


def layer_kernel(acts_in, proj_in, wout_in, gain_in, cw_in, cb_in, dtb_in, rate_in, skip_in, lb_in, gg_in, out_low, out_high,
                 wa, wb, ablk, u, pacc, p, proj, small, ones,
                 gain, cw, cb, dtb, rate, skip, lb, gg,
                 ext, xf, bcs, td, cu, yacc, near_st, eb, ee, snd1, slog, rcv1, rlog, table, rcv2, tail,
                 qs, qr, relay, wout, acc, os,
                 local_sems, send_sems, recv_sems, in_sems,
                 ssem, rsem, lsend, lrecv, tsem, qsend, qrecv, osend, orecv):
    i = lax.axis_index("seq")
    y = lax.rem(i, NY)
    g = lax.div(i, NY)
    z = lax.rem(g, NZ)
    x = lax.div(g, NZ)
    s = lax.axis_index("section")

    def there(dx, dz, dy):
        return {"seq": seq_of(x + dx, z + dz, y + dy)}

    def group(n):
        return {"seq": n * NY + y}

    def beside(n):
        return {"seq": g * NY + lax.rem(y + n, NY)}

    def wrap(n):
        return lax.rem(n, GROUPS)

    def remote(src, dst, send, recv, to):
        return pltpu.make_async_remote_copy(
            src_ref=src, dst_ref=dst, send_sem=send, recv_sem=recv, device_id=to, device_id_type=MESH)

    with jax.named_scope("enter"):
        barrier = pltpu.get_barrier_semaphore()

        near = ((1, 0, 0), (-1, 0, 0), (2, 0, 0), (0, 1, 0), (0, -1, 0), (0, 0, 1), (0, 0, -1), (0, 0, 2))
        for to in near:
            pl.semaphore_signal(barrier, inc=1, device_id=there(*to), device_id_type=MESH)
        pl.semaphore_signal(barrier, inc=1, device_id={"section": 1 - s}, device_id_type=MESH)
        pairs = ((proj_in, proj), (acts_in, ablk.at[y]), (gain_in, gain), (cw_in, cw), (cb_in, cb), (dtb_in, dtb),
                 (rate_in, rate), (skip_in, skip), (lb_in, lb), (gg_in, gg), (wout_in, wout))
        loads = [pltpu.make_async_copy(a, b, in_sems.at[n]) for n, (a, b) in enumerate(pairs)]
        for copy in loads[:-1]:
            copy.start()

        loads[0].wait()
        rows_k = lax.broadcasted_iota(jnp.int32, (288, 128), 0)
        lane_k = lax.broadcasted_iota(jnp.int32, (288, 128), 1)
        packed = proj[:, 4352:]
        for n in range(NY):
            from_lr = (lane_k < 64) & (rows_k == 32 + 64 * n + lane_k)
            from_dr = (lane_k >= 64) & (rows_k == 8 * n + lax.shift_right_logical(lane_k - 64, 3))
            hit = (from_lr | from_dr).astype(BF16)
            small[n] = jnp.dot(packed, hit, preferred_element_type=F32).astype(BF16)

        msgs = plan()
        number = {name: n for n, name in enumerate(msgs)}
        first_sends, steps, _ = schedule(msgs)

        def block(rel):
            return lax.rem(y + rel + 2 * NY, NY)

        def rows_of(cx, cz):
            return pl.ds(pl.multiple_of(seq_of(x + cx, z + cz, 0) * 16, 64), 64)

        def pieces(slot, rows):
            cols = pl.multiple_of(slot * 512, 512)
            return [(proj.at[:, pl.ds(cols, 512)], wa.at[rows]),
                    (proj.at[:, pl.ds(2048, 256)], wb.at[rows, pl.ds(0, 256)]),
                    (proj.at[:, pl.ds(pl.multiple_of(2304 + cols, 256), 512)], wb.at[rows, pl.ds(256, 512)]),
                    (small.at[slot], wb.at[rows, pl.ds(768, 128)])]

        mine = pl.ds(pl.multiple_of(i * 16, 16), 16)
        local = [pltpu.make_async_copy(a, b, local_sems.at[n]) for n, (a, b) in enumerate(pieces(y, mine))]
        for copy in local:
            copy.start()
        loads[1].wait()
        pl.semaphore_wait(barrier, len(near) + 1)

    def copies(name, arriving):
        part, chunk, to, dep, _, _ = msgs[name]
        n = number[name]
        back = to if arriving else (0, 0, 0)
        if part == "w":
            d = to[2]
            rows = pl.ds(pl.multiple_of(seq_of(x, z, y - d) * 16, 16), 16) if arriving else mine
            slot = lax.rem(y + d, NY)
            return [remote(a, b, send_sems.at[n if e == 0 else len(msgs) + 4 * n + e], recv_sems.at[n if e == 0 else len(msgs) + 4 * n + e], there(*to))
                    for e, (a, b) in enumerate(pieces(slot, rows))]
        if part in ("h0", "h1"):
            ref = ablk.at[block(chunk - back[2]), pl.ds(128 * int(part[1]), 128)]
        else:
            ref = (wa if part == "a" else wb).at[rows_of(chunk[0] - back[0], chunk[1] - back[1])]
        return [remote(ref, ref, send_sems.at[n], recv_sems.at[n], there(*to))]

    def start(name):
        for copy in copies(name, False):
            copy.start()

    def normed(rel, half):
        def step(n, _):
            at = pl.multiple_of(half * 128 + n * 64, 64)
            b = block(rel)
            h = ablk[b, pl.ds(at, 64), :].astype(F32)
            r = lax.rsqrt(jnp.mean(h * h, axis=1, keepdims=True) + EPS)
            u[pl.ds(pl.multiple_of(b * ROWS + at, 64), 64), :] = (h * r * gain[...]).astype(BF16)
            return 0

        lax.fori_loop(0, 2, step, 0)

    with jax.named_scope("gather"):
        for name in first_sends:
            start(name)
        for copy in loads[2:-1]:
            copy.wait()
        loads[-1].start()
        normed(0, 0)
        normed(0, 1)
        def picked(v, hit):
            rows = jnp.broadcast_to(v[...], (8, v.shape[1]))
            return jnp.dot(rows, hit.astype(F32), precision=HI, preferred_element_type=F32)[:1]

        def two(rows, lanes):
            return (lax.broadcasted_iota(jnp.int32, (rows, lanes), 0), lax.broadcasted_iota(jnp.int32, (rows, lanes), 1))

        k, c = two(32, 128)
        of_head = (c >= 64) & (k == 8 * y + lax.shift_right_logical(c - 64, 3))
        k2, c2 = two(256, 128)
        bias = picked(dtb, of_head) + picked(lb, (c2 < 64) & (k2 == 64 * y + c2))
        rates = picked(rate, of_head)
        k3, c3 = two(32, 512)
        skips = picked(skip, k3 == 8 * y + lax.shift_right_logical(c3, 6))

        low_tri = (lax.broadcasted_iota(jnp.int32, (ROWS, ROWS), 1) <= lax.broadcasted_iota(jnp.int32, (ROWS, ROWS), 0)).astype(BF16)
        lane_in, col_in = two(256, 512)
        for lev in range(9):
            lane = lev + 8 * lax.shift_right_logical(col_in, 6) + (64 - 8 if lev == 8 else 0)
            ones[lev] = ((lane_in & 127) == lane).astype(BF16)

        def widened(v, lev):
            high = v.astype(BF16)
            low = (v - high.astype(F32)).astype(BF16)
            return jnp.concatenate([high, low], axis=1), lev

        def wide(pair, cols=slice(0, 512)):
            return jnp.dot(pair[0], ones[pair[1], :, cols], preferred_element_type=F32)

        halves = {("P", 0): (-1, 0), ("P", 1): (-1, 1), ("M", 1): (1, 1), ("M", 0): (1, 0), ("P", 2): (-2, 0), ("M", 2): (2, 1)}
        missing = {(part, d): set() for d in range(NX) for part in "ab"}
        for name, m in msgs.items():
            if m[0] in ("a", "b"):
                missing[(m[0], (m[2][0] - m[1][0]) % NX)].add(name)
        lacking = {-1: {("P", 0), ("P", 1)}, 1: {("M", 1), ("M", 0)}, -2: {("P", 2), ("M", 2)}}
        here, held, ready, counted = [0], [], [], {}

        def multiply():
            which = ready[0][1]
            rels = [rel for rel, other in ready if other == which]
            ready[:] = [e for e in ready if e[1] != which]
            part, d = which
            rows = [pl.ds(pl.multiple_of(block(rel) * ROWS, ROWS), ROWS) for rel in rels]
            deep = pl.ds(pl.multiple_of(lax.rem(x + NX - d, NX) * 512, 512), 512)
            w, cols = (wa, slice(0, CA)) if part == "a" else (wb, slice(CA, NP))
            left = jnp.concatenate([u[r, deep] for r in rows], axis=0)
            full = jnp.dot(left, w[deep, :], preferred_element_type=F32)
            for e, (rel, at) in enumerate(zip(rels, rows)):
                done = counted[rel, part] = counted.get((rel, part), 0) + 1
                r = full[e * ROWS : (e + 1) * ROWS]
                if done > 1:
                    r = r + pacc[at, cols]
                if done == NX:
                    p[at, cols] = r.astype(BF16)
                else:
                    pacc[at, cols] = r

        for name, then in steps:
            if name == "own":
                for copy in local:
                    copy.wait()
            else:
                for copy in copies(name, True):
                    copy.wait_recv()
            for other in then:
                start(other)
            if name in halves:
                normed(*halves[name])
            for rel, left in list(lacking.items()):
                left.discard(name)
                if not left:
                    del lacking[rel]
                    here.append(rel)
                    ready += [(rel, d) for d in held]
            for d, left in list(missing.items()):
                left.discard(name)
                if not left:
                    del missing[d]
                    held.append(d)
                    ready += [(rel, d) for rel in here]
            if ready:
                multiply()
        while ready:
            multiply()

    with jax.named_scope("rows"):
        for b in range(4):
            rows = slice(b * ROWS, (b + 1) * ROWS)
            t = softplus(p[rows, MID:].astype(F32) + bias)
            td[rows, :] = t
            left = -t * rates
            total = jnp.zeros((ROWS, 128), F32)
            for _ in range(3):
                piece = left.astype(BF16)
                total = total + jnp.dot(low_tri, piece, preferred_element_type=F32)
                left = left - piece.astype(F32)
            cu[rows, :] = total
            eb[b : b + 1, :] = total[ROWS - 1 :, :]
        eb[4:, :] = jnp.zeros((4, 128), F32)
        ends = eb[...]
        ee[...] = jnp.exp(spread(ends, 512))
        slog[...] = jnp.sum(ends, axis=0, keepdims=True)

    with jax.named_scope("conv"):
        back = remote(p.at[pl.ds(1008, 16), pl.ds(0, 768)], tail, tsem.at[0], tsem.at[1], group(wrap(g + 1)))
        back.start()

        for n in range(4):
            ext[8 + n * ROWS : 8 + (n + 1) * ROWS, :] = p[n * ROWS : (n + 1) * ROWS, :768].astype(F32)
        own = pl.ds(pl.multiple_of(y * 512, 512), 512)
        tx = [cw[k : k + 1, own] for k in range(4)]
        tb = [cw[k : k + 1, 2048:] for k in range(4)]
        bx, bb = cb[:, own], cb[:, 2048:]

        def convolved(n):
            at = n * 128
            v = bx
            for k in range(4):
                v = v + tx[k] * ext[at + 5 + k : at + 133 + k, :512]
            xf[at : at + 128, :] = jax.nn.silu(v)
            v = bb
            for k in range(4):
                v = v + tb[k] * ext[at + 5 + k : at + 133 + k, 512:]
            bcs[at : at + 128, :] = jax.nn.silu(v).astype(BF16)

        for n in range(1, 8):
            convolved(n)
        back.wait_recv()
        before = tail[...].astype(F32)
        ext[0:8, :] = jnp.where(g > 0, before[8:, :], 0.0)
        convolved(0)

    with jax.named_scope("states"):
        first = lax.broadcasted_iota(jnp.int32, (1, 128), 1) < 64

        def state(b):
            rows = slice(b * ROWS, (b + 1) * ROWS)
            tl = jnp.exp(ends[b : b + 1, :] - cu[rows, :]) * td[rows, :]
            xt = (xf[rows, :] * wide(widened(tl, 8))).astype(BF16)
            return lax.dot_general(bcs[rows, :128], xt, (((0,), (0,)), ((), ())), preferred_element_type=F32)

        st = state(0)
        near_st[0] = st.astype(BF16)
        st = ee[1:2, :] * st + state(1)
        near_st[1] = st.astype(BF16)
        other = state(2)
        near_st[2] = other.astype(BF16)
        st = ee[2:3, :] * ee[3:4, :] * st + ee[3:4, :] * other + state(3)
        st = st.astype(BF16)
        for n in range(GROUPS):
            ct, nt = n // 8, n % 8
            snd1[n] = st[16 * nt : 16 * nt + 16, 128 * ct : 128 * ct + 128]

        def first_send(d, _):
            to = wrap(g + d)
            remote(snd1.at[to], rcv1.at[g], ssem.at[0], rsem.at[0], group(to)).start()
            remote(slog, rlog.at[g], ssem.at[1], rsem.at[1], group(to)).start()
            return 0

        lax.fori_loop(1, GROUPS, first_send, 0)
        rcv1[g] = snd1[g]
        rlog[g] = slog[...]

    with jax.named_scope("inside"):
        def inside(b, _):
            base = pl.multiple_of(b * ROWS, ROWS)
            every = pl.ds(base, ROWS)
            cum_t = jnp.transpose(cu[every, :])
            dt_t = jnp.transpose(td[every, :])
            for r in range(2):
                rows = pl.ds(pl.multiple_of(base + 128 * r, 128), 128)
                reach = 128 * (r + 1)
                seen = pl.ds(base, reach)
                scores = lax.dot_general(bcs[rows, 128:], bcs[seen, :128], (((1,), (1,)), ((), ())), preferred_element_type=F32)
                ti, si = two(128, reach)
                causal = si <= ti + 128 * r
                cum, lam = cu[rows, :], wide(widened(td[rows, :], 0))
                for h in range(4):
                    xp = xf[seen, 128 * h : 128 * h + 128].astype(BF16)
                    got = []
                    for e in (2 * h, 2 * h + 1):
                        lane = 64 + 8 * e
                        differ = jnp.where(causal, cum[:, lane : lane + 1] - cum_t[lane : lane + 1, :reach], -1e30)
                        w = scores * jnp.exp(differ) * dt_t[lane : lane + 1, :reach]
                        got.append(jnp.dot(w.astype(BF16), xp, preferred_element_type=F32))
                    cols = slice(128 * h, 128 * h + 128)
                    val = jnp.where(first, got[0], got[1]) * lam[:, cols]
                    yacc[rows, cols] = val + skips[:, cols] * xf[rows, cols]
            return 0

        lax.fori_loop(0, 4, inside, 0)

    with jax.named_scope("near"):
        lane8 = lax.broadcasted_iota(jnp.int32, (1, 128), 1) & 7

        def read(b, rows, bucket, scale, lev):
            r = jnp.dot(bcs[rows, 128:], bucket, preferred_element_type=F32)
            yacc[rows, :] += r * wide(widened(scale, lev))

        def scales(rows, add):
            return pltpu.roll(jnp.exp(cu[rows, :] + add), 64, 1) * td[rows, :]

        zero = jnp.zeros((1, 128), F32)
        at_block = [pl.ds(b * ROWS, ROWS) for b in range(4)]
        read(1, at_block[1], near_st[0], scales(at_block[1], zero), 1)
        read(2, at_block[2], near_st[1], scales(at_block[2], zero), 2)
        sc = scales(at_block[3], jnp.where(lane8 == 2, ends[2:3, :], 0.0))
        read(3, at_block[3], near_st[2], sc, 1)
        read(3, at_block[3], near_st[1], sc, 2)

        def gates(n, _):
            rows = pl.ds(pl.multiple_of(n * 128, 128), 128)
            v = p[rows, 768:1280].astype(F32)
            xf[rows, :] = jax.nn.silu(v)
            return 0

        lax.fori_loop(0, 8, gates, 0)

    with jax.named_scope("wait1"):
        remote(rcv1.at[pl.ds(0, GROUPS - 1)], rcv1.at[pl.ds(0, GROUPS - 1)], ssem.at[0], rsem.at[0], group(g)).wait_recv()
        remote(rlog.at[pl.ds(0, GROUPS - 1)], rlog.at[pl.ds(0, GROUPS - 1)], ssem.at[1], rsem.at[1], group(g)).wait_recv()
    with jax.named_scope("merge"):
        logs = rlog[:, 0, :]
        wide_logs = spread(logs, 512)
        ct = lax.div(g, 8)
        head_logs = jnp.zeros((GROUPS, 128), F32)
        for n in range(4):
            head_logs = jnp.where(ct == n, wide_logs[:, 128 * n : 128 * n + 128], head_logs)
        bits = [lax.rem(lax.div(g, 2**l), 2) for l in range(LEVELS_OUT)]

        def give(l):
            own = lax.div(g, 2 ** (l + 1)) * 2**l + lax.rem(g, 2**l)

            def to_one(k, _):
                at = lax.rem(own + k, 16)
                half = lax.div(at, 2**l)
                to = (2 * half + 1) * 2**l + lax.rem(at, 2**l)
                src = rcv1.at[2 * half] if l == 0 else table.at[TABLE[l] + half]
                remote(src, rcv2.at[l, g], lsend.at[l], lrecv.at[l], group(to)).start()
                return 0

            lax.fori_loop(1, 16, to_one, 0)

            @pl.when(bits[l] == 0)
            def _():
                to_one(0, 0)

        give(0)
        level = [rcv1[n].astype(F32) for n in range(GROUPS)]
        ends_of = [head_logs[n : n + 1, :] for n in range(GROUPS)]
        for l in range(1, LEVELS_OUT):
            level = [jnp.exp(ends_of[n + 1]) * level[n] + level[n + 1] for n in range(0, len(level), 2)]
            ends_of = [ends_of[n] + ends_of[n + 1] for n in range(0, len(ends_of), 2)]
            for n in range(0, len(level), 2):
                table[TABLE[l] + n // 2] = level[n].astype(BF16)
            give(l)

    with jax.named_scope("outer"):
        row_of = lax.broadcasted_iota(jnp.int32, (GROUPS, 1), 0)
        outer = zero
        for l in range(LEVELS_OUT):
            start = lax.div(g, 2**l) * 2**l
            summed = jnp.sum(jnp.where((row_of >= start) & (row_of < g), logs, 0.0), axis=0, keepdims=True)
            outer = jnp.where(lane8 == l + 3, summed, outer)
        run = zero
        for b in range(4):
            eb[4 + b : 5 + b, :] = run + outer
            run = run + ends[b : b + 1, :]

    with jax.named_scope("wait2"):
        def bucket(l, h):
            return jnp.concatenate([rcv2[l, 8 * e : 8 * e + 8].reshape(128, 128) for e in (h, h + 1)], axis=1)

        def scaled(n):
            rows = pl.ds(pl.multiple_of(n * 128, 128), 128)
            return rows, widened(scales(rows, eb[pl.ds(4 + lax.div(n, 2), 1), :]), 0)[0], bcs[rows, 128:]

        for l in range(LEVELS_OUT):
            @pl.when(bits[l] == 1)
            def _():
                remote(rcv2.at[l, pl.ds(0, GROUPS - 1)], rcv2.at[l, pl.ds(0, GROUPS - 1)], lsend.at[l], lrecv.at[l], group(g)).wait_recv()
                rcv2[l, g] = rcv1[2 * lax.div(g, 2)] if l == 0 else table[TABLE[l] + lax.div(g, 2 ** (l + 1))]

            if l < LEVELS_OUT - 1:
                @pl.when(bits[l] == 1)
                def _():
                    def add(n, _):
                        rows, pair_of, c = scaled(n)
                        for h in (0, 2):
                            cols = slice(128 * h, 128 * h + 256)
                            r = jnp.dot(c, bucket(l, h), preferred_element_type=F32)
                            yacc[rows, cols] += r * wide((pair_of, l + 3), cols)
                        return 0

                    lax.fori_loop(0, 8, add, 0)

    with jax.named_scope("finish"):
        last = LEVELS_OUT - 1

        @pl.when(bits[last] == 0)
        def _():
            rcv2[last] = jnp.zeros((GROUPS, 16, 128), BF16)

        def finish(b):
            for half in range(2):
                rows, pair_of, c = scaled(2 * b + half)
                for h in (0, 2):
                    cols = slice(128 * h, 128 * h + 256)
                    r = jnp.dot(c, bucket(last, h), preferred_element_type=F32)
                    vals = yacc[rows, cols] + r * wide((pair_of, last + 3), cols)
                    qs[b, 128 * half : 128 * half + 128, cols] = (vals * xf[rows, cols]).astype(BF16)

        def side(n):
            return lax.rem(y + n, NY)

        lower, upper = pl.ds(0, 128), pl.ds(128, 128)
        first_hop = [remote(qs.at[side(2), lower], relay.at[0], qsend.at[0], qrecv.at[0], beside(1)),
                     remote(qs.at[side(2), upper], relay.at[1], qsend.at[1], qrecv.at[1], beside(3))]
        next_hop = [remote(relay.at[0], qr.at[side(3), lower], qsend.at[2], qrecv.at[2], beside(1)),
                    remote(relay.at[1], qr.at[side(1), upper], qsend.at[3], qrecv.at[3], beside(3))]
        direct = [remote(qs.at[side(1)], qr.at[y], qsend.at[4], qrecv.at[4], beside(1)),
                  remote(qs.at[side(3)], qr.at[y], qsend.at[5], qrecv.at[5], beside(3))]
        finish(side(2))
        for copy in first_hop:
            copy.start()
        finish(side(1))
        direct[0].start()
        finish(side(3))
        direct[1].start()
        finish(y)
        for a, b in zip(first_hop, next_hop):
            a.wait_recv()
            b.start()
    with jax.named_scope("out"):
        qr[y] = qs[y]
        loads[-1].wait()

        squares = jnp.zeros((ROWS, 1), F32)
        sends = []
        for at, n in enumerate((0, 1, 3, 2)):
            src = lax.rem(y + NY - n, NY)
            if n == 1:
                direct[0].wait_recv()
            elif n == 3:
                direct[1].wait_recv()
            elif n == 2:
                for copy in next_hop:
                    copy.wait_recv()
            v = qr[src].astype(F32)
            squares = squares + jnp.sum(v * v, axis=1, keepdims=True)
            lanes = pl.ds(pl.multiple_of(src * 512, 512), 512)
            v = (v * gg[:, lanes]).astype(BF16)
            for t in range(4):
                cols = slice(512 * t, 512 * t + 512)
                part = jnp.dot(v, wout[lanes, cols], preferred_element_type=F32)
                if at < 3:
                    acc[:, cols] = part if at == 0 else acc[:, cols] + part
                    continue
                r = lax.rsqrt(squares * (1.0 / 2048.0) + EPS)
                os[t] = (ablk[y, :, cols].astype(F32) + r * (acc[:, cols] + part)).astype(BF16)
                for half, to in enumerate((out_low, out_high)):
                    n_send = 2 * t + half
                    sends.append(remote(os.at[t, pl.ds(128 * half, 128)], to.at[:, pl.ds(512 * t, 512)], osend.at[n_send], orecv.at[n_send], {"section": 1 - s}))
                    sends[-1].start()
    with jax.named_scope("swap"):
        for copy in sends:
            copy.wait_recv()
    with jax.named_scope("drain"):
        for name in msgs:
            for copy in copies(name, False):
                copy.wait_send()
        back.wait_send()
        remote(rcv1.at[pl.ds(0, GROUPS - 1)], rcv1.at[pl.ds(0, GROUPS - 1)], ssem.at[0], rsem.at[0], group(g)).wait_send()
        remote(rlog.at[pl.ds(0, GROUPS - 1)], rlog.at[pl.ds(0, GROUPS - 1)], ssem.at[1], rsem.at[1], group(g)).wait_send()
        for l in range(LEVELS_OUT):
            for bit in range(2):
                @pl.when(bits[l] == bit)
                def _():
                    some = rcv2.at[l, pl.ds(0, 16 - bit)]
                    remote(some, some, lsend.at[l], lrecv.at[l], group(g)).wait_send()
        for copy in first_hop + next_hop + direct:
            copy.wait_send()
        for copy in sends:
            copy.wait_send()


def layer(acts, proj, wout, *params):
    anywhere = pl.BlockSpec(memory_space=pl.ANY)
    n = NY * ROWS
    count = 2 * len(plan())
    dma = pltpu.SemaphoreType.DMA
    return pl.pallas_call(
        layer_kernel,
        out_shape=[jax.ShapeDtypeStruct((ROWS // 2, 2048), BF16)] * 2,
        in_specs=[anywhere] * (3 + len(params)),
        out_specs=[anywhere] * 2,
        scratch_shapes=[
            pltpu.VMEM((2048, CA), BF16),
            pltpu.VMEM((2048, CB), BF16),
            pltpu.VMEM((NY, ROWS, 2048), BF16),
            pltpu.VMEM((n, 2048), BF16),
            pltpu.VMEM((n, NP), F32),
            pltpu.VMEM((n, NP), BF16),
            pltpu.VMEM(proj.shape, BF16),
            pltpu.VMEM((NY, 16, 128), BF16),
            pltpu.VMEM((9, 256, 512), BF16),
            *[pltpu.VMEM(a.shape, a.dtype) for a in params],
            pltpu.VMEM((n + 8, 768), F32),
            pltpu.VMEM((n, 512), F32),
            pltpu.VMEM((n, 256), BF16),
            pltpu.VMEM((n, 128), F32),
            pltpu.VMEM((n, 128), F32),
            pltpu.VMEM((n, 512), F32),
            pltpu.VMEM((3, 128, 512), BF16),
            pltpu.VMEM((8, 128), F32),
            pltpu.VMEM((8, 512), F32),
            pltpu.VMEM((GROUPS, 16, 128), BF16),
            pltpu.VMEM((1, 128), F32),
            pltpu.VMEM((GROUPS, 16, 128), BF16),
            pltpu.VMEM((GROUPS, 1, 128), F32),
            pltpu.VMEM((31, 16, 128), BF16),
            pltpu.VMEM((LEVELS_OUT, GROUPS, 16, 128), BF16),
            pltpu.VMEM((16, 768), BF16),
            pltpu.VMEM((NY, ROWS, 512), BF16),
            pltpu.VMEM((NY, ROWS, 512), BF16),
            pltpu.VMEM((2, 128, 512), BF16),
            pltpu.VMEM((2048, 2048), BF16),
            pltpu.VMEM((ROWS, 2048), F32),
            pltpu.VMEM((4, ROWS, 512), BF16),
            dma((5,)), dma((count,)), dma((count,)), dma((11,)),
            dma((2,)), dma((2,)), dma((5,)), dma((5,)), dma((2,)), dma((6,)), dma((6,)), dma((8,)), dma((8,)),
        ],
        compiler_params=pltpu.CompilerParams(
            collective_id=0, has_side_effects=True, vmem_limit_bytes=58 * 1024 * 1024),
        name="layer",
    )(acts, proj, wout, *params)


def per_device(acts, in_proj, out_proj, conv_weight, conv_bias, dt_bias, decay_rate, skip_gain, level_bias, norm_gain, gate_gain):
    low, high = layer(acts[0], in_proj[0], out_proj[0], norm_gain, conv_weight[0], conv_bias, dt_bias, decay_rate, skip_gain, level_bias, gate_gain)
    return jnp.concatenate([low, high], axis=0)[None]


def solution(mesh):
    two = P("section", None)
    three = P("section", None, None)
    return jax.shard_map(
        per_device,
        mesh=mesh,
        in_specs=(P("section", "seq", None), P("section", "seq", None), three, three, two, two, two, two, two, two, two),
        out_specs=P("section", "seq", None),
        check_vma=False,
    )
```
